1024 devices in a mesh: plate: 32 (over y_hi, z), tower: 8 (over y_lo, core), gz: 4 (over x).
Axes of the slice: x: 4, y: 8 (y_hi: 2, y_lo: 4; y = y_hi * 4 + y_lo), z: 16, core: 2. Of those that a mesh axis runs over, the one named last changes fastest.
Arguments:
- positions: float32 [32, 8, 4, 3, 128], P('plate', 'tower', 'gz'), may hold values from 0 to 1
- features: bfloat16 [32, 8, 4, 576, 128], P('plate', 'tower', 'gz'), may hold values from -6 to 6
- species: int32 [32, 8, 4, 128], P('plate', 'tower', 'gz'), may hold values from 0 to 5
- emb_table: bfloat16 [6, 64], replicated, may hold values from -4 to 4
- edges: int32 [32, 8, 4, 2, 512], P('plate', 'tower', 'gz'), may hold values from 0 to 1151, as said below
- edge_count: int32 [32, 8, 4], P('plate', 'tower', 'gz'), may hold values from 1 to 512, as said below
- w_first: bfloat16 [128, 328], replicated, may hold values from -0.3125 to 0.3125
- w_second: bfloat16 [64, 128], replicated, may hold values from -0.5 to 0.5
- w_out: bfloat16 [64], replicated, may hold values from -0.75 to 0.75
Outputs:
- forces: float32 [32, 8, 4, 3, 128], P('plate', 'tower', 'gz')
- edge_energy: float32 [32, 8, 4, 512], P('plate', 'tower', 'gz')
The draws below stay inside these ranges and needn't reach their ends.
Inputs may be any that keep to these rules, and one draw needn't show every extreme that they name: `edges`: row 0 holds plate-set indices below 384; row 1 holds column-set indices below 1152. Slots at or beyond a box's edge_count are padding with arbitrary valid indices. `edge_count`: some box holds exactly 512 live edges in every draw.
All inputs are finite; a program needn't handle non-finite values.
Results may differ from the reference program's by a relative error of at most 0.011.
Values may be sent and summed in bfloat16 or wider, within the bound.
A program may use at most 32 MiB of HBM per device.

```python
import math
import jax
import jax.numpy as jnp
from jax import lax

A = 128
E = 512
CH = 64
LAT = 128
RB = 8
S = 6
N_PLATE = 32
N_TOWER = 8
N_GZ = 4


def draw_edges(key, part):
    key_left, key_right = jax.random.split(jax.random.fold_in(key, 11))
    shape = (N_PLATE, N_TOWER, N_GZ, 1, E)
    left_index = jax.random.randint(key_left, shape, 0, 3 * A, dtype=jnp.int32)
    right_index = jax.random.randint(key_right, shape, 0, 9 * A, dtype=jnp.int32)
    return jnp.concatenate([left_index, right_index], axis=3)


def draw_edge_count(key, part):
    key_one, key_two, key_pick = jax.random.split(jax.random.fold_in(key, 23), 3)
    shape = (N_PLATE * N_TOWER * N_GZ,)
    factor_one = jax.random.randint(key_one, shape, 1, E + 1, dtype=jnp.int32)
    factor_two = jax.random.randint(key_two, shape, 1, E + 1, dtype=jnp.int32)
    counts = jnp.maximum(factor_one * factor_two // E, 1)
    chosen = jax.random.randint(key_pick, (), 0, N_PLATE * N_TOWER * N_GZ, dtype=jnp.int32)
    counts = jnp.where(jnp.arange(N_PLATE * N_TOWER * N_GZ, dtype=jnp.int32) == chosen, E, counts)
    return counts.reshape(N_PLATE, N_TOWER, N_GZ).astype(jnp.int32)


def with_ends(drawn, rng, least, largest):
    shape = drawn.shape
    place = [jax.random.randint(jax.random.fold_in(rng, axis), (), 0, shape[axis]) for axis in range(len(shape))]
    drawn = drawn.at[tuple(place)].set(least)
    longest = shape.index(max(shape))
    place[longest] = (place[longest] + 1) % shape[longest]
    return drawn.at[tuple(place)].set(largest)


def block_scale(rng, shape, cuts, least, top_value):
    def one(position, shards_of):
        draws = jax.random.uniform(jax.random.fold_in(jax.random.fold_in(rng, 6), position), (shards_of,), jnp.float32, least / len(cuts), top_value / len(cuts))
        return jnp.repeat(jnp.exp(draws), shape[position] // shards_of).reshape((-1,) + (1,) * (len(shape) - position - 1))

    level = one(*cuts[0])
    for cut in cuts[1:]:
        level = level * one(*cut)
    return level


def centred(key, shape, deviation, limit, cuts=(), kind=jnp.bfloat16):
    loudness = block_scale(key, shape, cuts, -0.22, 0.18) if cuts else 1.0
    array = jax.random.normal(key, shape, jnp.float32) * deviation * loudness
    return jnp.minimum(jnp.maximum(array, -limit), limit).astype(kind)


def setup_inputs(seed: int = 0) -> dict:
    key_list = jax.random.split(jax.random.key(seed), 10)
    positions = jnp.clip(1.0 * jax.random.uniform(key_list[0], (N_PLATE, N_TOWER, N_GZ, 3, A), jnp.float32) ** block_scale(key_list[0], (N_PLATE, N_TOWER, N_GZ, 3, A), ((0, 32), (1, 8), (2, 4)), -0.2, 0.2), 0.0, 1.0)
    features = centred(key_list[1], (N_PLATE, N_TOWER, N_GZ, 9 * CH, A), 1.0, 6.0, ((0, 32), (1, 8), (2, 4)))
    species = with_ends(jax.random.randint(key_list[2], (N_PLATE, N_TOWER, N_GZ, A), 0, S), jax.random.fold_in(key_list[2], 1), 0, S - 1).astype(jnp.int32)
    emb_table = centred(key_list[3], (S, CH), 1.0, 4.0)
    edges = draw_edges(jax.random.fold_in(key_list[9], 71), 0)
    edge_count = draw_edge_count(jax.random.fold_in(key_list[9], 71), 0)
    w_first = centred(key_list[6], (LAT, RB + 5 * CH), (RB + 5 * CH) ** -0.5, 0.3125)
    w_second = centred(key_list[7], (CH, LAT), LAT ** -0.5, 0.5)
    w_out = centred(key_list[8], (CH,), CH ** -0.5, 0.75)
    return dict(positions=positions, features=features, species=species, emb_table=emb_table, edges=edges, edge_count=edge_count, w_first=w_first, w_second=w_second, w_out=w_out)


RADIUS = 3.0
SOFTEN = 0.04

def harmonics(unit_vec):
    cx, cy, cz = (unit_vec[0], unit_vec[1], unit_vec[2])
    root3 = math.sqrt(3.0)
    root15 = math.sqrt(15.0)
    root5 = math.sqrt(5.0)
    return jnp.stack([jnp.ones_like(cx), root3 * cx, root3 * cy, root3 * cz, root15 * cx * cy, root15 * cy * cz, 0.5 * root5 * (3.0 * cz * cz - 1.0), root15 * cx * cz, 0.5 * root15 * (cx * cx - cy * cy)])

def pack_block(positions, features, species, emb_table):
    pos_hi = positions.astype(jnp.bfloat16)
    back = lax.optimization_barrier(pos_hi).astype(jnp.float32)
    pos_lo = (positions - back).astype(jnp.bfloat16)
    kinds = jnp.arange(emb_table.shape[0], dtype=jnp.int32)
    onehot = (species[..., None, :] == kinds[:, None]).astype(jnp.float32)
    emb = jnp.einsum('sc,...sa->...ca', emb_table.astype(jnp.float32), onehot).astype(jnp.bfloat16)
    return jnp.concatenate([features, emb, pos_hi, pos_lo], axis=-2)

def make_offsets(atoms):
    shifts = jnp.arange(3, dtype=jnp.float32) - 1.0
    plate_x = jnp.repeat(shifts, atoms)
    zeros_plate = jnp.zeros_like(plate_x)
    plate_off = jnp.stack([plate_x, zeros_plate, zeros_plate])
    column_y = jnp.repeat(jnp.repeat(shifts, 3), atoms)
    column_z = jnp.repeat(jnp.tile(shifts, 3), atoms)
    column_off = jnp.stack([jnp.zeros_like(column_y), column_y, column_z])
    return (plate_off, column_off)

def degree_sums(terms):
    return jnp.concatenate([terms[0], lax.optimization_barrier(jnp.sum(terms[1:4], 0)), lax.optimization_barrier(jnp.sum(terms[4:9], 0))], 0)

def edge_model(coord_i, coord_j, feat_i, feat_j, emb_i, emb_j, w_first, w_second, w_out):
    width = emb_i.shape[0]
    delta = coord_j - coord_i
    dist2 = lax.optimization_barrier(jnp.sum(delta * delta, 0)) + SOFTEN
    dist = jnp.sqrt(dist2)
    harmonic = harmonics(delta / dist)
    orders = jnp.arange(1, RB + 1, dtype=jnp.float32)
    radial = jnp.sin(orders[:, None] * (math.pi / RADIUS) * dist[None, :]) / dist[None, :]
    envelope = jnp.square(jnp.maximum(1.0 - dist2 / (RADIUS * RADIUS), 0.0))
    proj_i = degree_sums(feat_i.astype(jnp.float32).reshape(9, width, -1) * harmonic[:, None, :])
    proj_j = degree_sums(feat_j.astype(jnp.float32).reshape(9, width, -1) * harmonic[:, None, :])
    inputs = jnp.concatenate([radial, emb_i.astype(jnp.float32), emb_j.astype(jnp.float32), proj_i * proj_j], 0).astype(jnp.bfloat16)
    hidden = jax.nn.silu(jnp.dot(w_first, inputs, preferred_element_type=jnp.float32)).astype(jnp.bfloat16)
    second_layer = jax.nn.silu(jnp.dot(w_second, hidden, preferred_element_type=jnp.float32))
    return envelope * lax.optimization_barrier(jnp.sum(w_out.astype(jnp.float32)[:, None] * second_layer, 0))

def split_rows(picked, offsets, width):
    coord = picked[10 * width:10 * width + 3].astype(jnp.float32) + picked[10 * width + 3:10 * width + 6].astype(jnp.float32) + offsets
    return (coord, picked[:9 * width], picked[9 * width:10 * width])

def device_pass(plate_rows, column_rows, edge_list, live_count, w_first, w_second, w_out, live_only):
    width = (plate_rows.shape[0] - 6) // 10
    atoms = plate_rows.shape[1] // 3
    plate_off, column_off = make_offsets(atoms)
    total = edge_list.shape[-1]
    block = min(1024, total)

    def step(index, carry):
        plate_part, column_part, energy = carry
        start = index * block
        left_index = lax.dynamic_slice_in_dim(edge_list[0], start, block)
        right_index = lax.dynamic_slice_in_dim(edge_list[1], start, block)
        slots = start + jnp.arange(block, dtype=jnp.int32)
        live_mask = (slots < live_count).astype(jnp.float32)
        coord_i, feat_i, emb_i = split_rows(jnp.take(plate_rows, left_index, axis=1), jnp.take(plate_off, left_index, axis=1), width)
        coord_j, feat_j, emb_j = split_rows(jnp.take(column_rows, right_index, axis=1), jnp.take(column_off, right_index, axis=1), width)

        def energy_of(left_coord, right_coord):
            return live_mask * edge_model(left_coord, right_coord, feat_i, feat_j, emb_i, emb_j, w_first, w_second, w_out)
        values, pullback = jax.vjp(energy_of, coord_i, coord_j)
        grad_i, grad_j = pullback(jnp.ones_like(values))
        plate_part = plate_part.at[:, left_index].add(grad_i)
        column_part = column_part.at[:, right_index].add(grad_j)
        energy = lax.dynamic_update_slice_in_dim(energy, values, start, 0)
        return (plate_part, column_part, energy)
    start_carry = (jnp.zeros((3, 3 * atoms), jnp.float32), jnp.zeros((3, 9 * atoms), jnp.float32), jnp.zeros((total,), jnp.float32))
    if live_only:
        upper = (live_count + block - 1) // block
    else:
        upper = total // block
    return lax.fori_loop(0, upper, step, start_carry)

def reference(positions, features, species, emb_table, edges, edge_count, w_first, w_second, w_out):
    packed = pack_block(positions, features, species, emb_table)
    atoms = positions.shape[-1]

    def one_box(forces, device):
        plate = device // (N_TOWER * N_GZ)
        tower = device // N_GZ % N_TOWER
        depth = device % N_GZ
        plate_rows = jnp.concatenate([packed[(plate + shift - 1) % N_PLATE, tower, depth] for shift in range(3)], axis=1)
        column_rows = jnp.concatenate([packed[plate, (tower + row - 1) % N_TOWER, (depth + col - 1) % N_GZ] for row in range(3) for col in range(3)], axis=1)
        plate_part, column_part, energy = device_pass(plate_rows, column_rows, edges[plate, tower, depth], edge_count[plate, tower, depth], w_first, w_second, w_out, False)
        for shift in range(3):
            forces = forces.at[(plate + shift - 1) % N_PLATE, tower, depth].add(-plate_part[:, shift * atoms:(shift + 1) * atoms])
        for row in range(3):
            for col in range(3):
                slot = 3 * row + col
                forces = forces.at[plate, (tower + row - 1) % N_TOWER, (depth + col - 1) % N_GZ].add(-column_part[:, slot * atoms:(slot + 1) * atoms])
        return (forces, energy)
    start_forces = jnp.zeros(positions.shape, jnp.float32)
    forces, energies = lax.scan(one_box, start_forces, jnp.arange(N_PLATE * N_TOWER * N_GZ, dtype=jnp.int32))
    return (forces, energies.reshape(N_PLATE, N_TOWER, N_GZ, edges.shape[-1]))
```

```python
import math

import jax
import jax.numpy as jnp
from jax import lax
from jax.experimental import pallas as pl
from jax.experimental.pallas import tpu as pltpu
from jax.sharding import PartitionSpec as P

ATOMS = 128
EDGES = 512
CH = 64
LAT = 128
RB = 8
ROWS = 9 * CH
HALF = ROWS // 2
RADIUS = 3.0
SOFTEN = 0.04
F32 = jnp.float32
BF16 = jnp.bfloat16

NSLOT = 10


def dot(a, b):
    return lax.dot_general(a, b, (((1,), (0,)), ((), ())), preferred_element_type=F32)


def dot_nt(a, b):
    return lax.dot_general(a, b, (((1,), (1,)), ((), ())), preferred_element_type=F32)


def sin_cos_pi(t):
    turns = jnp.floor(t + 0.5)
    x = (t - turns) * math.pi
    parity = turns - 2.0 * jnp.floor(turns * 0.5)
    sign = 1.0 - 2.0 * parity
    y = x * x
    s = -1.0 / 39916800.0
    for c in (1.0 / 362880.0, -1.0 / 5040.0, 1.0 / 120.0, -1.0 / 6.0, 1.0):
        s = s * y + c
    c_ = 1.0 / 479001600.0
    for c in (-1.0 / 3628800.0, 1.0 / 40320.0, -1.0 / 720.0, 1.0 / 24.0, -0.5, 1.0):
        c_ = c_ * y + c
    return sign * s * x, sign * c_


def kernel(
    pos_ref,
    feat_ref,
    spec_ref,
    edges_ref,
    count_ref,
    table_ref,
    w1_ref,
    w2_ref,
    wout_ref,
    force_ref,
    energy_ref,
    fslot,
    mown,
    mslot,
    ohp,
    ohc,
    gi,
    gj,
    si,
    sj,
    yb,
    xbuf,
    wtmp,
    wp,
    wpt,
    w2t,
    tmat,
    gbuf,
    rad,
    pout,
    pslot,
    msend,
    mrecv,
    fsend,
    frecv,
    psend,
    precv,
):
    n_plate, n_tower, n_gz = (lax.axis_size(a) for a in ("plate", "tower", "gz"))
    p, t, g = (lax.axis_index(a) for a in ("plate", "tower", "gz"))
    odd = lax.rem(t, 2)
    partner = t + 1 - 2 * odd
    outward = lax.rem(t + 2 * odd - 1 + n_tower, n_tower)
    g_up, g_dn = lax.rem(g + 1, n_gz), lax.rem(g + n_gz - 1, n_gz)
    p_up, p_dn = lax.rem(p + 1, n_plate), lax.rem(p + n_plate - 1, n_plate)

    def dev(pp, tt, gg):
        return {"plate": pp, "tower": tt, "gz": gg}

    dest = [
        dev(p, t, g_up), dev(p, t, g_dn), dev(p, partner, g), dev(p, outward, g),
        dev(p, partner, g_up), dev(p, partner, g_dn), dev(p, outward, g_up), dev(p, outward, g_dn),
        dev(p_up, t, g), dev(p_dn, t, g),
    ]
    home = [dest[k] for k in (1, 0, 2, 3, 5, 4, 7, 6, 9, 8)]

    barrier = pltpu.get_barrier_semaphore()
    for d in dest:
        pl.semaphore_signal(barrier, inc=1, device_id=d, device_id_type=pl.DeviceIdType.MESH)

    pos = pos_ref[...]
    hi = pos.astype(BF16).astype(F32)
    lo = (pos - hi).astype(BF16).astype(F32)
    rad[...] = jnp.zeros_like(rad)
    rad[0:3, 0:ATOMS] = hi
    rad[3:6, 0:ATOMS] = lo
    rad[6:7, 0:ATOMS] = spec_ref[...].astype(F32)
    mown[...] = rad[:, 0:ATOMS].astype(BF16)

    def remote(src, dst, ssem, rsem, to):
        return pltpu.make_async_remote_copy(
            src_ref=src,
            dst_ref=dst,
            send_sem=ssem,
            recv_sem=rsem,
            device_id=to,
            device_id_type=pl.DeviceIdType.MESH,
        )

    meta = [remote(mown, mslot.at[k], msend.at[k], mrecv.at[k], dest[k]) for k in range(NSLOT)]
    top, low = pl.ds(0, HALF), pl.ds(HALF, HALF)

    def feature(n, src, slot, to, part=None):
        dst = fslot.at[slot]
        if part is not None:
            src, dst = src.at[part], dst.at[part]
        return remote(src, dst, fsend.at[n], frecv.at[n], to)

    f_g_up = feature(0, feat_ref, 0, dest[0])
    f_g_dn = feature(1, feat_ref, 1, dest[1])
    f_part = feature(2, feat_ref, 2, dest[2])
    f_out = [feature(3, feat_ref, 3, dest[3], top), feature(4, feat_ref, 3, dest[3], low)]
    f_p_up = feature(5, feat_ref, 8, dest[8])
    f_p_dn = feature(6, feat_ref, 9, dest[9])
    r_part = [feature(7, fslot.at[0], 4, dest[2]), feature(8, fslot.at[1], 5, dest[2])]
    r_up = [feature(9, fslot.at[3], 6, dest[0], top), feature(10, fslot.at[3], 6, dest[0], low)]
    r_dn = [feature(11, fslot.at[3], 7, dest[1], top), feature(12, fslot.at[3], 7, dest[1], low)]

    pl.semaphore_wait(barrier, NSLOT)
    for c in meta:
        c.start()
    for c in (f_out[0], f_out[1], f_g_up, f_g_dn, f_p_up, f_p_dn, f_part):
        c.start()

    left, right = edges_ref[0:1, :], edges_ref[1:2, :]
    row = lax.broadcasted_iota(jnp.int32, (3 * ATOMS, EDGES), 0)
    ohp[...] = jnp.where(row == left, 1.0, 0.0).astype(BF16)
    for k, u in enumerate((1, 2 - 2 * odd, 2 * odd)):
        shifted = right - 3 * ATOMS * u
        ohc[3 * ATOMS * k : 3 * ATOMS * (k + 1), :] = jnp.where(row == shifted, 1.0, 0.0).astype(BF16)

    tmat[...] = jnp.zeros_like(tmat)
    tmat[0:6, 0:CH] = table_ref[...].astype(F32)
    tmat[6:7, 0:CH] = wout_ref[...].astype(F32)
    turned = jnp.transpose(tmat[...])
    embt = turned[0:CH, :].astype(BF16)
    wout = turned[0:CH, 6:7]
    wtmp[...] = jnp.zeros_like(wtmp)
    wtmp[:, 0 : RB + 5 * CH] = w1_ref[...].astype(F32)
    wfull = pltpu.roll(wtmp[...], 6 * CH - RB, 1)
    wp[...] = wfull.astype(BF16)
    wpt[...] = jnp.transpose(wfull).astype(BF16)
    w2t[...] = jnp.transpose(w2_ref[...].astype(F32)).astype(BF16)

    f_out[0].wait_recv()
    r_up[0].start()
    r_dn[0].start()
    f_out[1].wait_recv()
    r_up[1].start()
    r_dn[1].start()
    f_g_up.wait_recv()
    r_part[0].start()
    f_g_dn.wait_recv()
    r_part[1].start()

    for c in meta:
        c.wait_recv()
    mi = dot(jnp.concatenate([mslot[8], mown[...], mslot[9]], 1), ohp[...])
    order = [mslot[0], mown[...], mslot[1], mslot[4], mslot[2], mslot[5], mslot[6], mslot[3], mslot[7]]
    mj = dot(jnp.concatenate(order, 1), ohc[...])
    off_i = jnp.where(left < ATOMS, -1.0, jnp.where(left < 2 * ATOMS, 0.0, 1.0))
    off_u = jnp.where(right < 3 * ATOMS, 0, jnp.where(right < 6 * ATOMS, 1, 2))
    rest = right - 3 * ATOMS * off_u
    off_v = jnp.where(rest < ATOMS, -1.0, jnp.where(rest < 2 * ATOMS, 0.0, 1.0))
    dx = (mj[0:1] + mj[3:4]) - (mi[0:1] + mi[3:4] + off_i)
    dy = (mj[1:2] + mj[4:5] + (off_u.astype(F32) - 1.0)) - (mi[1:2] + mi[4:5])
    dz = (mj[2:3] + mj[5:6] + off_v) - (mi[2:3] + mi[5:6])
    r2 = dx * dx + dy * dy + dz * dz + SOFTEN
    r = jnp.sqrt(r2)
    inv = 1.0 / r
    nx, ny, nz = dx * inv, dy * inv, dz * inv
    root3, root5, root15 = math.sqrt(3.0), math.sqrt(5.0), math.sqrt(15.0)
    harm = (
        root3 * nx, root3 * ny, root3 * nz, root15 * nx * ny, root15 * ny * nz,
        0.5 * root5 * (3.0 * nz * nz - 1.0), root15 * nx * nz, 0.5 * root15 * (nx * nx - ny * ny),
    )
    for m in range(8):
        yb[m] = jnp.broadcast_to(harm[m], (8, EDGES))
    orders = (lax.broadcasted_iota(jnp.int32, (RB, EDGES), 0) + 1).astype(F32)
    sin_b, cos_b = sin_cos_pi(orders * (1.0 / RADIUS) * r)
    radial = sin_b * inv
    slope = (orders * (math.pi / RADIUS) * cos_b - radial) * inv
    live = jnp.where(lax.broadcasted_iota(jnp.int32, (1, EDGES), 1) < count_ref[0, 0], 1.0, 0.0)
    gap = jnp.maximum(1.0 - r2 * (1.0 / (RADIUS * RADIUS)), 0.0)
    env = live * gap * gap
    kinds = lax.broadcasted_iota(jnp.int32, (LAT, EDGES), 0)
    for k, m in enumerate((mi, mj)):
        pick = jnp.where(kinds == m[6:7].astype(jnp.int32), 1.0, 0.0).astype(BF16)
        xbuf[CH * k : CH * (k + 1), :] = dot(embt, pick).astype(BF16)
    xbuf[5 * CH : 6 * CH - 16, :] = jnp.zeros((CH - 16, EDGES), BF16)
    xbuf[6 * CH - 16 : 6 * CH, :] = jnp.concatenate([jnp.zeros_like(radial), radial], 0).astype(BF16)

    f_part.wait_recv()
    for c in (*r_part, *r_up, *r_dn):
        c.wait_recv()
    order = [fslot[0], feat_ref[...], fslot[1], fslot[4], fslot[2], fslot[5], fslot[6], fslot[3], fslot[7]]
    gj[...] = dot(jnp.concatenate(order, 1), ohc[...])
    f_p_up.wait_recv()
    f_p_dn.wait_recv()
    gi[...] = dot(jnp.concatenate([fslot[8], feat_ref[...], fslot[9]], 1), ohp[...])

    def rows_of(ref, m, k):
        return ref[m * CH + 8 * k : m * CH + 8 * k + 8, :]

    for k2 in range(CH // 16):
        prods = [[], [], []]
        for k in (2 * k2, 2 * k2 + 1):
            sums = []
            for ref in (gi, gj):
                one = [rows_of(ref, m, k) * yb[m - 1] for m in range(1, 9)]
                sums.append((
                    rows_of(ref, 0, k),
                    one[0] + one[1] + one[2],
                    one[3] + one[4] + one[5] + one[6] + one[7],
                ))
            for l in range(3):
                si[l * CH + 8 * k : l * CH + 8 * k + 8, :] = sums[0][l]
                sj[l * CH + 8 * k : l * CH + 8 * k + 8, :] = sums[1][l]
                prods[l].append(sums[0][l] * sums[1][l])
        for l in range(3):
            start = (2 + l) * CH + 16 * k2
            xbuf[start : start + 16, :] = jnp.concatenate(prods[l], 0).astype(BF16)
    z1 = dot(wp[...], xbuf[...])
    sig1 = 1.0 / (1.0 + jnp.exp(-z1))
    z2 = dot(w2_ref[...], (z1 * sig1).astype(BF16))
    sig2 = 1.0 / (1.0 + jnp.exp(-z2))
    u = jnp.sum(wout * (z2 * sig2), 0, keepdims=True)
    energy_ref[...] = env * u

    dz2 = (wout * env) * (sig2 * (1.0 + z2 * (1.0 - sig2)))
    dh = dot(w2t[...], dz2.astype(BF16)).astype(BF16).astype(F32)
    dz1 = dh * (sig1 * (1.0 + z1 * (1.0 - sig1)))
    dxv = dot(wpt[...], dz1.astype(BF16)).astype(BF16).astype(F32)
    acc = [jnp.zeros((8, EDGES), F32) for _ in range(8)]
    for k in range(CH // 8):
        for l, ms in ((1, (1, 2, 3)), (2, (4, 5, 6, 7, 8))):
            at = slice(l * CH + 8 * k, l * CH + 8 * k + 8)
            dq = dxv[2 * CH + at.start : 2 * CH + at.stop, :]
            di, dj = dq * sj[at, :], dq * si[at, :]
            for m in ms:
                acc[m - 1] = acc[m - 1] + di * rows_of(gi, m, k) + dj * rows_of(gj, m, k)
    h1, h2, h3, h4, h5, h6, h7, h8 = (jnp.sum(a, 0, keepdims=True) for a in acc)
    ax = root3 * h1 + root15 * (ny * h4 + nz * h7 + nx * h8)
    ay = root3 * h2 + root15 * (nx * h4 + nz * h5 - ny * h8)
    az = root3 * h3 + root15 * (ny * h5 + nx * h7) + (3.0 * root5) * nz * h6
    dr = jnp.sum(dxv[6 * CH - RB : 6 * CH, :] * slope, 0, keepdims=True)
    dr = dr - (ax * nx + ay * ny + az * nz) * inv
    denv = live * u * (2.0 * gap) * (-1.0 / (RADIUS * RADIUS))
    scale = dr * inv + 2.0 * denv
    gbuf[...] = jnp.zeros_like(gbuf)
    gbuf[0:1, :] = ax * inv + dx * scale
    gbuf[1:2, :] = ay * inv + dy * scale
    gbuf[2:3, :] = az * inv + dz * scale

    grad = gbuf[...]
    g_hi = grad.astype(BF16).astype(F32)
    both = jnp.concatenate([g_hi, grad - g_hi], 0).astype(BF16)
    part_p = dot_nt(both, ohp[...])
    part_p = part_p[0:8] + part_p[8:16]
    part_c = dot_nt(both, ohc[...])
    part_c = -(part_c[0:8] + part_c[8:16])

    def lanes(a, k):
        return a[:, k * ATOMS : (k + 1) * ATOMS]

    for slot, k in enumerate((0, 2, 4, 7, 3, 5, 6, 8)):
        pout[slot] = lanes(part_c, k)
    pout[8] = lanes(part_p, 0)
    pout[9] = lanes(part_p, 2)
    back = [remote(pout.at[k], pslot.at[k], psend.at[k], precv.at[k], home[k]) for k in range(NSLOT)]
    for c in back:
        c.start()
    total = lanes(part_p, 1) + lanes(part_c, 1)
    for c in (*meta, f_g_up, f_g_dn, f_part, *f_out, f_p_up, f_p_dn, *r_part, *r_up, *r_dn):
        c.wait_send()
    for k, c in enumerate(back):
        c.wait_recv()
        total = total + pslot[k]
    force_ref[...] = total[0:3, :]
    for c in back:
        c.wait_send()


def shards(positions, features, species, emb_table, edges, edge_count, w_first, w_second, w_out):
    vmem = pl.BlockSpec(memory_space=pltpu.VMEM)
    dma = pltpu.SemaphoreType.DMA
    forces, energy = pl.pallas_call(
        kernel,
        name="edge_forces",
        out_shape=(jax.ShapeDtypeStruct((3, ATOMS), F32), jax.ShapeDtypeStruct((1, EDGES), F32)),
        in_specs=[vmem, vmem, vmem, vmem, pl.BlockSpec(memory_space=pltpu.SMEM), vmem, vmem, vmem, vmem],
        out_specs=(vmem, vmem),
        scratch_shapes=[
            pltpu.VMEM((NSLOT, ROWS, ATOMS), BF16),
            pltpu.VMEM((16, ATOMS), BF16),
            pltpu.VMEM((NSLOT, 16, ATOMS), BF16),
            pltpu.VMEM((3 * ATOMS, EDGES), BF16),
            pltpu.VMEM((9 * ATOMS, EDGES), BF16),
            pltpu.VMEM((ROWS, EDGES), F32),
            pltpu.VMEM((ROWS, EDGES), F32),
            pltpu.VMEM((3 * CH, EDGES), F32),
            pltpu.VMEM((3 * CH, EDGES), F32),
            pltpu.VMEM((8, 8, EDGES), F32),
            pltpu.VMEM((6 * CH, EDGES), BF16),
            pltpu.VMEM((LAT, 6 * CH), F32),
            pltpu.VMEM((LAT, 6 * CH), BF16),
            pltpu.VMEM((6 * CH, LAT), BF16),
            pltpu.VMEM((LAT, CH), BF16),
            pltpu.VMEM((LAT, LAT), F32),
            pltpu.VMEM((8, EDGES), F32),
            pltpu.VMEM((16, EDGES), F32),
            pltpu.VMEM((NSLOT, 8, ATOMS), F32),
            pltpu.VMEM((NSLOT, 8, ATOMS), F32),
            dma((NSLOT,)),
            dma((NSLOT,)),
            dma((13,)),
            dma((13,)),
            dma((NSLOT,)),
            dma((NSLOT,)),
        ],
        compiler_params=pltpu.CompilerParams(collective_id=0, has_side_effects=True),
    )(
        positions.reshape(3, ATOMS),
        features.reshape(ROWS, ATOMS),
        species.reshape(1, ATOMS),
        edges.reshape(2, EDGES),
        edge_count.reshape(1, 1),
        emb_table,
        w_first,
        w_second,
        w_out.reshape(1, CH),
    )
    return (forces.reshape(1, 1, 1, 3, ATOMS), energy.reshape(1, 1, 1, EDGES))


def solution(mesh):
    placed = (
        P("plate", "tower", "gz", None, None),
        P("plate", "tower", "gz", None, None),
        P("plate", "tower", "gz", None),
        P(),
        P("plate", "tower", "gz", None, None),
        P("plate", "tower", "gz"),
        P(),
        P(),
        P(),
    )
    return jax.shard_map(
        shards,
        mesh=mesh,
        in_specs=placed,
        out_specs=(P("plate", "tower", "gz", None, None), P("plate", "tower", "gz", None)),
        check_vma=False,
    )
```

```python
import math

import jax
import jax.numpy as jnp
from jax import lax
from jax.experimental import pallas as pl
from jax.experimental.pallas import tpu as pltpu
from jax.sharding import PartitionSpec as P

ATOMS = 128
EDGES = 512
CH = 64
LAT = 128
RB = 8
ROWS = 9 * CH
HALF = ROWS // 2
RADIUS = 3.0
SOFTEN = 0.04
F32 = jnp.float32
BF16 = jnp.bfloat16

NSLOT = 10


def dot(a, b):
    return lax.dot_general(a, b, (((1,), (0,)), ((), ())), preferred_element_type=F32)


def dot_nt(a, b):
    return lax.dot_general(a, b, (((1,), (1,)), ((), ())), preferred_element_type=F32)


def sin_cos_pi(t):
    turns = jnp.floor(t + 0.5)
    x = (t - turns) * math.pi
    parity = turns - 2.0 * jnp.floor(turns * 0.5)
    sign = 1.0 - 2.0 * parity
    y = x * x
    s = -1.0 / 39916800.0
    for c in (1.0 / 362880.0, -1.0 / 5040.0, 1.0 / 120.0, -1.0 / 6.0, 1.0):
        s = s * y + c
    c_ = 1.0 / 479001600.0
    for c in (-1.0 / 3628800.0, 1.0 / 40320.0, -1.0 / 720.0, 1.0 / 24.0, -0.5, 1.0):
        c_ = c_ * y + c
    return sign * s * x, sign * c_


def remote(src, dst, ssem, rsem, to):
    return pltpu.make_async_remote_copy(
        src_ref=src,
        dst_ref=dst,
        send_sem=ssem,
        recv_sem=rsem,
        device_id=to,
        device_id_type=pl.DeviceIdType.MESH,
    )


def fetch(pairs, sems):
    copies = [pltpu.make_async_copy(src, dst, sems.at[n]) for n, (src, dst) in enumerate(pairs)]
    for c in copies:
        c.start()
    return copies


def pack_small(pos, spec, stage, out):
    stage[...] = jnp.zeros_like(stage)
    for k in range(3):
        hi = pos[k].astype(BF16).astype(F32)
        stage[k : k + 1, :] = hi
        stage[k + 3 : k + 4, :] = (pos[k] - hi).astype(BF16).astype(F32)
    stage[6:7, :] = spec[...].astype(F32)
    out[...] = stage[...].astype(BF16)


DEPTH = 16


def early_kernel(pos_any, feat_any, spec_any, sib_feat, sib_meta, pos, spec, stage, mown, lsem, ssem, rsem):
    n_plate = lax.axis_size("plate")
    p, t, g = (lax.axis_index(a) for a in ("plate", "tower", "gz"))
    sibling = {"plate": lax.rem(p + DEPTH, n_plate), "tower": t, "gz": g}

    @pl.when(lax.rem(p, DEPTH) == 0)
    def _():
        barrier = pltpu.get_barrier_semaphore()
        pl.semaphore_signal(barrier, inc=1, device_id=sibling, device_id_type=pl.DeviceIdType.MESH)
        for c in fetch([(pos_any, pos), (spec_any, spec)], lsem):
            c.wait()
        pack_small(pos, spec, stage, mown)
        pl.semaphore_wait(barrier, 1)
        copies = [
            remote(feat_any, sib_feat, ssem.at[0], rsem.at[0], sibling),
            remote(mown, sib_meta, ssem.at[1], rsem.at[1], sibling),
        ]
        for c in copies:
            c.start()
        for c in copies:
            c.wait()


def kernel(
    pos_any,
    feat_any,
    spec_any,
    edges_any,
    count_any,
    table_any,
    w1_any,
    w2_any,
    wout_any,
    sib_feat,
    sib_meta,
    force_ref,
    energy_ref,
    pos,
    feat_ref,
    spec_ref,
    edges_ref,
    count_ref,
    table_ref,
    w1_ref,
    w2_ref,
    wout_ref,
    sib_f,
    sib_m,
    relay,
    fslot,
    mown,
    mslot,
    ohp,
    ohc,
    gi,
    gj,
    si,
    sj,
    yb,
    xbuf,
    wtmp,
    wp,
    wpt,
    w2t,
    tmat,
    gbuf,
    stage,
    pout,
    pslot,
    lsem,
    xsem,
    msend,
    mrecv,
    fsend,
    frecv,
    psend,
    precv,
):
    n_plate, n_tower, n_gz = (lax.axis_size(a) for a in ("plate", "tower", "gz"))
    p, t, g = (lax.axis_index(a) for a in ("plate", "tower", "gz"))
    odd = lax.rem(t, 2)
    partner = t + 1 - 2 * odd
    outward = lax.rem(t + 2 * odd - 1 + n_tower, n_tower)
    g_up, g_dn = lax.rem(g + 1, n_gz), lax.rem(g + n_gz - 1, n_gz)
    p_up, p_dn = lax.rem(p + 1, n_plate), lax.rem(p + n_plate - 1, n_plate)
    z = lax.rem(p, DEPTH)
    last = z // (DEPTH - 1)
    first = lax.rem(z + DEPTH - 1, DEPTH) // (DEPTH - 1)

    def dev(pp, tt, gg):
        return {"plate": pp, "tower": tt, "gz": gg}

    dest = [
        dev(p, t, g_up), dev(p, t, g_dn), dev(p, partner, g), dev(p, outward, g),
        dev(p, partner, g_up), dev(p, partner, g_dn), dev(p, outward, g_up), dev(p, outward, g_dn),
        dev(p_up, t, g), dev(p_dn, t, g),
    ]
    home = [dest[k] for k in (1, 0, 2, 3, 5, 4, 7, 6, 9, 8)]
    sibling = dev(lax.rem(p + DEPTH, n_plate), t, g)
    below = dev(lax.rem(p + n_plate - 1 + DEPTH * first, n_plate), t, g)
    above = dev(lax.rem(p + 1 + DEPTH * last, n_plate), t, g)

    barrier = pltpu.get_barrier_semaphore()

    def greet(d):
        pl.semaphore_signal(barrier, inc=1, device_id=d, device_id_type=pl.DeviceIdType.MESH)

    for d in (below, above, *dest[:8]):
        greet(d)

    @pl.when(z == 0)
    def _():
        greet(dest[9])
        greet(sibling)

    small = fetch([(pos_any, pos), (spec_any, spec_ref)], lsem)
    rest = fetch(
        [
            (feat_any, feat_ref), (edges_any, edges_ref), (count_any, count_ref), (table_any, table_ref),
            (w1_any, w1_ref), (w2_any, w2_ref), (wout_any, wout_ref),
        ],
        xsem,
    )
    for c in small:
        c.wait()
    pack_small(pos, spec_ref, stage, mown)

    @pl.when(z == 0)
    def _():
        for c in fetch([(sib_feat, sib_f), (sib_meta, sib_m)], lsem):
            c.wait()

    meta = [remote(mown, mslot.at[k], msend.at[k], mrecv.at[k], dest[k]) for k in range(NSLOT - 1)]
    meta.append(remote(mown, mslot.at[9], msend.at[9], mrecv.at[9], below))
    meta_sib = remote(sib_m, mslot.at[9], msend.at[9], mrecv.at[9], below)
    top, low = pl.ds(0, HALF), pl.ds(HALF, HALF)

    def feature(n, src, slot, to, part=None):
        dst = fslot.at[slot]
        if part is not None:
            src, dst = src.at[part], dst.at[part]
        return remote(src, dst, fsend.at[n], frecv.at[n], to)

    f_g_up = feature(0, feat_ref, 0, dest[0])
    f_g_dn = feature(1, feat_ref, 1, dest[1])
    f_part = feature(2, feat_ref, 2, dest[2])
    f_out = [feature(3, feat_ref, 3, dest[3], top), feature(4, feat_ref, 3, dest[3], low)]
    f_p_dn = feature(6, feat_ref, 9, below)
    f_p_sib = feature(6, sib_f, 9, below)
    f_p_up = feature(5, feat_ref, 8, dest[8], top)
    f_p_low = feature(13, feat_ref, 8, above, low)
    f_p_via = remote(feat_ref.at[low], relay, fsend.at[13], frecv.at[14], above)
    r_up_low = remote(relay, fslot.at[8].at[low], fsend.at[14], frecv.at[13], sibling)
    r_part = [feature(7, fslot.at[0], 4, dest[2]), feature(8, fslot.at[1], 5, dest[2])]
    r_up = [feature(9, fslot.at[3], 6, dest[0], top), feature(10, fslot.at[3], 6, dest[0], low)]
    r_dn = [feature(11, fslot.at[3], 7, dest[1], top), feature(12, fslot.at[3], 7, dest[1], low)]

    rest[0].wait()
    pl.semaphore_wait(barrier, NSLOT + first + last)
    for c in meta[:9]:
        c.start()

    @pl.when(z == 0)
    def _():
        meta_sib.start()
        f_p_sib.start()

    @pl.when(z != 0)
    def _():
        meta[9].start()
        f_p_dn.start()

    f_p_up.start()

    @pl.when(last == 1)
    def _():
        f_p_via.start()

    @pl.when(last != 1)
    def _():
        f_p_low.start()

    for c in (f_out[0], f_out[1], f_g_up, f_g_dn, f_part):
        c.start()
    for c in rest[1:]:
        c.wait()

    left, right = edges_ref[0:1, :], edges_ref[1:2, :]
    row = lax.broadcasted_iota(jnp.int32, (3 * ATOMS, EDGES), 0)
    ohp[...] = jnp.where(row == left, 1.0, 0.0).astype(BF16)
    for k, u in enumerate((1, 2 - 2 * odd, 2 * odd)):
        shifted = right - 3 * ATOMS * u
        ohc[3 * ATOMS * k : 3 * ATOMS * (k + 1), :] = jnp.where(row == shifted, 1.0, 0.0).astype(BF16)

    tmat[...] = jnp.zeros_like(tmat)
    tmat[0:6, 0:CH] = table_ref[...].astype(F32)
    tmat[6:7, 0:CH] = wout_ref[...].astype(F32)
    turned = jnp.transpose(tmat[...])
    embt = turned[0:CH, :].astype(BF16)
    wout = turned[0:CH, 6:7]
    wtmp[0 : 5 * CH, :] = w1_ref[RB : RB + 5 * CH, :].astype(F32)
    wtmp[5 * CH : 6 * CH - RB, :] = jnp.zeros((CH - RB, LAT), F32)
    wtmp[6 * CH - RB : 6 * CH, :] = w1_ref[0:RB, :].astype(F32)
    wfull = wtmp[...]
    wpt[...] = wfull.astype(BF16)
    wp[...] = jnp.transpose(wfull).astype(BF16)
    w2t[...] = jnp.transpose(w2_ref[...].astype(F32)).astype(BF16)

    f_out[0].wait_recv()
    r_up[0].start()
    r_dn[0].start()
    f_out[1].wait_recv()
    r_up[1].start()
    r_dn[1].start()
    f_g_up.wait_recv()
    r_part[0].start()
    f_g_dn.wait_recv()
    r_part[1].start()

    @pl.when(z == 0)
    def _():
        f_p_via.wait_recv()
        r_up_low.start()

    for c in meta:
        c.wait_recv()
    mi = dot(jnp.concatenate([mslot[8], mown[...], mslot[9]], 1), ohp[...])
    order = [mslot[0], mown[...], mslot[1], mslot[4], mslot[2], mslot[5], mslot[6], mslot[3], mslot[7]]
    mj = dot(jnp.concatenate(order, 1), ohc[...])
    off_i = jnp.where(left < ATOMS, -1.0, jnp.where(left < 2 * ATOMS, 0.0, 1.0))
    off_u = jnp.where(right < 3 * ATOMS, 0, jnp.where(right < 6 * ATOMS, 1, 2))
    rest = right - 3 * ATOMS * off_u
    off_v = jnp.where(rest < ATOMS, -1.0, jnp.where(rest < 2 * ATOMS, 0.0, 1.0))
    dx = (mj[0:1] + mj[3:4]) - (mi[0:1] + mi[3:4] + off_i)
    dy = (mj[1:2] + mj[4:5] + (off_u.astype(F32) - 1.0)) - (mi[1:2] + mi[4:5])
    dz = (mj[2:3] + mj[5:6] + off_v) - (mi[2:3] + mi[5:6])
    r2 = dx * dx + dy * dy + dz * dz + SOFTEN
    r = jnp.sqrt(r2)
    inv = 1.0 / r
    nx, ny, nz = dx * inv, dy * inv, dz * inv
    root3, root5, root15 = math.sqrt(3.0), math.sqrt(5.0), math.sqrt(15.0)
    harm = (
        root3 * nx, root3 * ny, root3 * nz, root15 * nx * ny, root15 * ny * nz,
        0.5 * root5 * (3.0 * nz * nz - 1.0), root15 * nx * nz, 0.5 * root15 * (nx * nx - ny * ny),
    )
    for m in range(8):
        yb[m] = jnp.broadcast_to(harm[m], (8, EDGES))
    orders = (lax.broadcasted_iota(jnp.int32, (RB, EDGES), 0) + 1).astype(F32)
    sin_b, cos_b = sin_cos_pi(orders * (1.0 / RADIUS) * r)
    radial = sin_b * inv
    slope = (orders * (math.pi / RADIUS) * cos_b - radial) * inv
    live = jnp.where(lax.broadcasted_iota(jnp.int32, (1, EDGES), 1) < count_ref[0, 0], 1.0, 0.0)
    gap = jnp.maximum(1.0 - r2 * (1.0 / (RADIUS * RADIUS)), 0.0)
    env = live * gap * gap
    kinds = lax.broadcasted_iota(jnp.int32, (LAT, EDGES), 0)
    for k, m in enumerate((mi, mj)):
        pick = jnp.where(kinds == m[6:7].astype(jnp.int32), 1.0, 0.0).astype(BF16)
        xbuf[CH * k : CH * (k + 1), :] = dot(embt, pick).astype(BF16)
    xbuf[5 * CH : 6 * CH - 16, :] = jnp.zeros((CH - 16, EDGES), BF16)
    xbuf[6 * CH - 16 : 6 * CH, :] = jnp.concatenate([jnp.zeros_like(radial), radial], 0).astype(BF16)

    f_part.wait_recv()
    for c in (*r_part, *r_up, *r_dn):
        c.wait_recv()
    order = [fslot[0], feat_ref[...], fslot[1], fslot[4], fslot[2], fslot[5], fslot[6], fslot[3], fslot[7]]
    gj[...] = dot(jnp.concatenate(order, 1), ohc[...])
    f_p_dn.wait_recv()
    f_p_up.wait_recv()
    f_p_low.wait_recv()
    gi[...] = dot(jnp.concatenate([fslot[8], feat_ref[...], fslot[9]], 1), ohp[...])

    def rows_of(ref, m, k):
        return ref[m * CH + 8 * k : m * CH + 8 * k + 8, :]

    for k2 in range(CH // 16):
        prods = [[], [], []]
        for k in (2 * k2, 2 * k2 + 1):
            sums = []
            for ref in (gi, gj):
                one = [rows_of(ref, m, k) * yb[m - 1] for m in range(1, 9)]
                sums.append((
                    rows_of(ref, 0, k),
                    one[0] + one[1] + one[2],
                    one[3] + one[4] + one[5] + one[6] + one[7],
                ))
            for l in range(3):
                si[l * CH + 8 * k : l * CH + 8 * k + 8, :] = sums[0][l]
                sj[l * CH + 8 * k : l * CH + 8 * k + 8, :] = sums[1][l]
                prods[l].append(sums[0][l] * sums[1][l])
        for l in range(3):
            start = (2 + l) * CH + 16 * k2
            xbuf[start : start + 16, :] = jnp.concatenate(prods[l], 0).astype(BF16)
    z1 = dot(wp[...], xbuf[...])
    sig1 = 1.0 / (1.0 + jnp.exp(-z1))
    z2 = dot(w2_ref[...], (z1 * sig1).astype(BF16))
    sig2 = 1.0 / (1.0 + jnp.exp(-z2))
    u = jnp.sum(wout * (z2 * sig2), 0, keepdims=True)
    energy_ref[...] = env * u

    dz2 = (wout * env) * (sig2 * (1.0 + z2 * (1.0 - sig2)))
    dh = dot(w2t[...], dz2.astype(BF16)).astype(BF16).astype(F32)
    dz1 = dh * (sig1 * (1.0 + z1 * (1.0 - sig1)))
    dxv = dot(wpt[...], dz1.astype(BF16)).astype(BF16).astype(F32)
    acc = [jnp.zeros((8, EDGES), F32) for _ in range(8)]
    for k in range(CH // 8):
        for l, ms in ((1, (1, 2, 3)), (2, (4, 5, 6, 7, 8))):
            at = slice(l * CH + 8 * k, l * CH + 8 * k + 8)
            dq = dxv[2 * CH + at.start : 2 * CH + at.stop, :]
            di, dj = dq * sj[at, :], dq * si[at, :]
            for m in ms:
                acc[m - 1] = acc[m - 1] + di * rows_of(gi, m, k) + dj * rows_of(gj, m, k)
    h1, h2, h3, h4, h5, h6, h7, h8 = (jnp.sum(a, 0, keepdims=True) for a in acc)
    ax = root3 * h1 + root15 * (ny * h4 + nz * h7 + nx * h8)
    ay = root3 * h2 + root15 * (nx * h4 + nz * h5 - ny * h8)
    az = root3 * h3 + root15 * (ny * h5 + nx * h7) + (3.0 * root5) * nz * h6
    dr = jnp.sum(dxv[6 * CH - RB : 6 * CH, :] * slope, 0, keepdims=True)
    dr = dr - (ax * nx + ay * ny + az * nz) * inv
    denv = live * u * (2.0 * gap) * (-1.0 / (RADIUS * RADIUS))
    scale = dr * inv + 2.0 * denv
    gbuf[...] = jnp.zeros_like(gbuf)
    gbuf[0:1, :] = ax * inv + dx * scale
    gbuf[1:2, :] = ay * inv + dy * scale
    gbuf[2:3, :] = az * inv + dz * scale

    grad = gbuf[...]
    g_hi = grad.astype(BF16).astype(F32)
    both = jnp.concatenate([g_hi, grad - g_hi], 0).astype(BF16)
    part_p = dot_nt(both, ohp[...])
    part_p = part_p[0:8] + part_p[8:16]
    part_c = dot_nt(both, ohc[...])
    part_c = -(part_c[0:8] + part_c[8:16])

    def lanes(a, k):
        return a[:, k * ATOMS : (k + 1) * ATOMS]

    for slot, k in enumerate((0, 2, 4, 7, 3, 5, 6, 8)):
        pout[slot] = lanes(part_c, k)
    pout[8] = lanes(part_p, 0)
    pout[9] = lanes(part_p, 2)
    back = [remote(pout.at[k], pslot.at[k], psend.at[k], precv.at[k], home[k]) for k in range(NSLOT)]
    for c in back:
        c.start()
    total = lanes(part_p, 1) + lanes(part_c, 1)
    for c in (*meta, f_g_up, f_g_dn, f_part, *f_out, f_p_up, f_p_low, f_p_dn, *r_part, *r_up, *r_dn):
        c.wait_send()

    @pl.when(z == 0)
    def _():
        r_up_low.wait_send()

    for k, c in enumerate(back):
        c.wait_recv()
        total = total + pslot[k]
    for k in range(3):
        force_ref[k] = total[k : k + 1, :]
    for c in back:
        c.wait_send()


def shards(positions, features, species, emb_table, edges, edge_count, w_first, w_second, w_out):
    vmem = pl.BlockSpec(memory_space=pltpu.VMEM)
    hbm = pl.BlockSpec(memory_space=pl.ANY)
    dma = pltpu.SemaphoreType.DMA
    pos = jnp.transpose(positions.reshape(1, 3, ATOMS), (1, 0, 2))
    feat = features.reshape(ROWS, ATOMS)
    spec = species.reshape(1, ATOMS)
    small = [pltpu.VMEM((3, 1, ATOMS), F32), pltpu.VMEM((1, ATOMS), jnp.int32)]
    sib_feat, sib_meta = pl.pallas_call(
        early_kernel,
        name="early_exchange",
        out_shape=(jax.ShapeDtypeStruct((ROWS, ATOMS), BF16), jax.ShapeDtypeStruct((16, ATOMS), BF16)),
        in_specs=[hbm] * 3,
        out_specs=(hbm, hbm),
        scratch_shapes=[
            *small,
            pltpu.VMEM((16, ATOMS), F32),
            pltpu.VMEM((16, ATOMS), BF16),
            dma((2,)),
            dma((2,)),
            dma((2,)),
        ],
        compiler_params=pltpu.CompilerParams(collective_id=1, has_side_effects=True),
    )(pos, feat, spec)
    forces, energy = pl.pallas_call(
        kernel,
        name="edge_forces",
        out_shape=(jax.ShapeDtypeStruct((3, 1, ATOMS), F32), jax.ShapeDtypeStruct((1, EDGES), F32)),
        in_specs=[hbm] * 11,
        out_specs=(vmem, vmem),
        scratch_shapes=[
            small[0],
            pltpu.VMEM((ROWS, ATOMS), BF16),
            small[1],
            pltpu.VMEM((2, EDGES), jnp.int32),
            pltpu.SMEM((1, 1), jnp.int32),
            pltpu.VMEM((6, CH), BF16),
            pltpu.VMEM((RB + 5 * CH, LAT), BF16),
            pltpu.VMEM((CH, LAT), BF16),
            pltpu.VMEM((1, CH), BF16),
            pltpu.VMEM((ROWS, ATOMS), BF16),
            pltpu.VMEM((16, ATOMS), BF16),
            pltpu.VMEM((HALF, ATOMS), BF16),
            pltpu.VMEM((NSLOT, ROWS, ATOMS), BF16),
            pltpu.VMEM((16, ATOMS), BF16),
            pltpu.VMEM((NSLOT, 16, ATOMS), BF16),
            pltpu.VMEM((3 * ATOMS, EDGES), BF16),
            pltpu.VMEM((9 * ATOMS, EDGES), BF16),
            pltpu.VMEM((ROWS, EDGES), F32),
            pltpu.VMEM((ROWS, EDGES), F32),
            pltpu.VMEM((3 * CH, EDGES), F32),
            pltpu.VMEM((3 * CH, EDGES), F32),
            pltpu.VMEM((8, 8, EDGES), F32),
            pltpu.VMEM((6 * CH, EDGES), BF16),
            pltpu.VMEM((6 * CH, LAT), F32),
            pltpu.VMEM((LAT, 6 * CH), BF16),
            pltpu.VMEM((6 * CH, LAT), BF16),
            pltpu.VMEM((LAT, CH), BF16),
            pltpu.VMEM((LAT, LAT), F32),
            pltpu.VMEM((8, EDGES), F32),
            pltpu.VMEM((16, ATOMS), F32),
            pltpu.VMEM((NSLOT, 8, ATOMS), F32),
            pltpu.VMEM((NSLOT, 8, ATOMS), F32),
            dma((2,)),
            dma((7,)),
            dma((NSLOT,)),
            dma((NSLOT,)),
            dma((15,)),
            dma((15,)),
            dma((NSLOT,)),
            dma((NSLOT,)),
        ],
        compiler_params=pltpu.CompilerParams(collective_id=0, has_side_effects=True),
    )(
        pos,
        feat,
        spec,
        edges.reshape(2, EDGES),
        edge_count.reshape(1, 1),
        emb_table,
        w_first.T,
        w_second,
        w_out.reshape(1, CH),
        sib_feat,
        sib_meta,
    )
    return (
        jnp.transpose(forces, (1, 0, 2)).reshape(1, 1, 1, 3, ATOMS),
        energy.reshape(1, 1, 1, EDGES),
    )


def solution(mesh):
    placed = (
        P("plate", "tower", "gz", None, None),
        P("plate", "tower", "gz", None, None),
        P("plate", "tower", "gz", None),
        P(),
        P("plate", "tower", "gz", None, None),
        P("plate", "tower", "gz"),
        P(),
        P(),
        P(),
    )
    return jax.shard_map(
        shards,
        mesh=mesh,
        in_specs=placed,
        out_specs=(P("plate", "tower", "gz", None, None), P("plate", "tower", "gz", None)),
        check_vma=False,
    )
```

```python
import math

import jax
import jax.numpy as jnp
from jax import lax
from jax.experimental import pallas as pl
from jax.experimental.pallas import tpu as pltpu
from jax.sharding import PartitionSpec as P

ATOMS = 128
EDGES = 512
CH = 64
LAT = 128
RB = 8
ROWS = 9 * CH
HALF = ROWS // 2
RADIUS = 3.0
SOFTEN = 0.04
F32 = jnp.float32
BF16 = jnp.bfloat16

NSLOT = 10


def dot(a, b):
    return lax.dot_general(a, b, (((1,), (0,)), ((), ())), preferred_element_type=F32)


def dot_nt(a, b):
    return lax.dot_general(a, b, (((1,), (1,)), ((), ())), preferred_element_type=F32)


def sin_cos_pi(t):
    turns = jnp.floor(t + 0.5)
    x = (t - turns) * math.pi
    parity = turns - 2.0 * jnp.floor(turns * 0.5)
    sign = 1.0 - 2.0 * parity
    y = x * x
    s = -1.0 / 39916800.0
    for c in (1.0 / 362880.0, -1.0 / 5040.0, 1.0 / 120.0, -1.0 / 6.0, 1.0):
        s = s * y + c
    c_ = 1.0 / 479001600.0
    for c in (-1.0 / 3628800.0, 1.0 / 40320.0, -1.0 / 720.0, 1.0 / 24.0, -0.5, 1.0):
        c_ = c_ * y + c
    return sign * s * x, sign * c_


def remote(src, dst, ssem, rsem, to):
    return pltpu.make_async_remote_copy(
        src_ref=src,
        dst_ref=dst,
        send_sem=ssem,
        recv_sem=rsem,
        device_id=to,
        device_id_type=pl.DeviceIdType.MESH,
    )


def fetch(pairs, sems):
    copies = [pltpu.make_async_copy(src, dst, sems.at[n]) for n, (src, dst) in enumerate(pairs)]
    for c in copies:
        c.start()
    return copies


def pack_small(pos, spec, stage, out):
    stage[...] = jnp.zeros_like(stage)
    for k in range(3):
        hi = pos[k].astype(BF16).astype(F32)
        stage[k : k + 1, :] = hi
        stage[k + 3 : k + 4, :] = (pos[k] - hi).astype(BF16).astype(F32)
    stage[6:7, :] = spec[...].astype(F32)
    out[...] = stage[...].astype(BF16)


DEPTH = 16


def kernel(
    pos_any,
    feat_any,
    spec_any,
    edges_any,
    count_any,
    table_any,
    w1_any,
    w2_any,
    wout_any,
    force_ref,
    energy_ref,
    pos,
    feat_ref,
    spec_ref,
    edges_ref,
    count_ref,
    table_ref,
    w1_ref,
    w2_ref,
    wout_ref,
    sib_f,
    sib_m,
    fslot,
    mown,
    mslot,
    ohp,
    ohc,
    gi,
    gj,
    si,
    sj,
    yb,
    xbuf,
    wtmp,
    wp,
    wpt,
    w2t,
    tmat,
    gbuf,
    stage,
    pout,
    pslot,
    lsem,
    ready,
    msend,
    mrecv,
    fsend,
    frecv,
    psend,
    precv,
):
    n_plate, n_tower, n_gz = (lax.axis_size(a) for a in ("plate", "tower", "gz"))
    p, t, g = (lax.axis_index(a) for a in ("plate", "tower", "gz"))
    odd = lax.rem(t, 2)
    partner = t + 1 - 2 * odd
    outward = lax.rem(t + 2 * odd - 1 + n_tower, n_tower)
    g_up, g_dn = lax.rem(g + 1, n_gz), lax.rem(g + n_gz - 1, n_gz)
    p_up, p_dn = lax.rem(p + 1, n_plate), lax.rem(p + n_plate - 1, n_plate)
    z = lax.rem(p, DEPTH)
    last = z // (DEPTH - 1)
    first = lax.rem(z + DEPTH - 1, DEPTH) // (DEPTH - 1)

    def dev(pp, tt, gg):
        return {"plate": pp, "tower": tt, "gz": gg}

    dest = [
        dev(p, t, g_up), dev(p, t, g_dn), dev(p, partner, g), dev(p, outward, g),
        dev(p, partner, g_up), dev(p, partner, g_dn), dev(p, outward, g_up), dev(p, outward, g_dn),
        dev(p_up, t, g), dev(p_dn, t, g),
    ]
    home = [dest[k] for k in (1, 0, 2, 3, 5, 4, 7, 6, 9, 8)]
    sibling = dev(lax.rem(p + DEPTH, n_plate), t, g)
    below = dev(lax.rem(p + n_plate - 1 + DEPTH * first, n_plate), t, g)
    above = dev(lax.rem(p + 1 + DEPTH, n_plate), t, g)

    barrier = pltpu.get_barrier_semaphore()

    def greet(d):
        pl.semaphore_signal(barrier, inc=1, device_id=d, device_id_type=pl.DeviceIdType.MESH)

    for d in (below, *dest[:8]):
        greet(d)

    @pl.when(z == 0)
    def _():
        greet(dest[9])
        greet(sibling)

    @pl.when(last == 0)
    def _():
        greet(dest[8])

    small = fetch(
        [
            (pos_any, pos), (spec_any, spec_ref), (feat_any, feat_ref), (edges_any, edges_ref), (count_any, count_ref),
            (table_any, table_ref), (w1_any, w1_ref), (w2_any, w2_ref), (wout_any, wout_ref),
        ],
        lsem,
    )
    small, rest = small[:2], small[2:]
    for c in small:
        c.wait()
    pack_small(pos, spec_ref, stage, mown)

    meta = [remote(mown, mslot.at[k], msend.at[k], mrecv.at[k], dest[k]) for k in range(NSLOT - 1)]
    meta.append(remote(mown, mslot.at[9], msend.at[9], mrecv.at[9], below))
    meta_sib = remote(sib_m, mslot.at[9], msend.at[9], mrecv.at[9], below)
    top, low = pl.ds(0, HALF), pl.ds(HALF, HALF)

    def feature(n, src, slot, to, part=None):
        dst = fslot.at[slot]
        if part is not None:
            src, dst = src.at[part], dst.at[part]
        return remote(src, dst, fsend.at[n], frecv.at[n], to)

    f_g_up = feature(0, feat_ref, 0, dest[0])
    f_g_dn = feature(1, feat_ref, 1, dest[1])
    f_part = feature(2, feat_ref, 2, dest[2])
    f_out = [feature(3, feat_ref, 3, dest[3], top), feature(4, feat_ref, 3, dest[3], low)]
    f_p_dn = feature(6, feat_ref, 9, below)
    f_p_sib = feature(6, sib_f, 9, below)
    f_p_up = feature(5, feat_ref, 8, dest[8])
    sib_feat = remote(feat_ref, sib_f, fsend.at[13], frecv.at[13], sibling)
    sib_meta = remote(mown, sib_m, fsend.at[14], frecv.at[14], sibling)
    r_part = [feature(7, fslot.at[0], 4, dest[2]), feature(8, fslot.at[1], 5, dest[2])]
    r_up = [feature(9, fslot.at[3], 6, dest[0], top), feature(10, fslot.at[3], 6, dest[0], low)]
    r_dn = [feature(11, fslot.at[3], 7, dest[1], top), feature(12, fslot.at[3], 7, dest[1], low)]

    rest[0].wait()
    pl.semaphore_wait(barrier, NSLOT + last)

    @pl.when(last == 1)
    def _():
        pl.semaphore_signal(ready, inc=1, device_id=above, device_id_type=pl.DeviceIdType.MESH)

    @pl.when(z == 0)
    def _():
        sib_meta.start()
        sib_feat.start()

    for c in meta[:9]:
        c.start()
    f_p_up.start()

    @pl.when(z != 0)
    def _():
        meta[9].start()
        f_p_dn.start()

    for c in (f_out[0], f_out[1], f_g_up, f_g_dn, f_part):
        c.start()

    for c in rest[1:]:
        c.wait()

    left, right = edges_ref[0:1, :], edges_ref[1:2, :]
    row = lax.broadcasted_iota(jnp.int32, (3 * ATOMS, EDGES), 0)
    ohp[...] = jnp.where(row == left, 1.0, 0.0).astype(BF16)
    for k, u in enumerate((1, 2 - 2 * odd, 2 * odd)):
        shifted = right - 3 * ATOMS * u
        ohc[3 * ATOMS * k : 3 * ATOMS * (k + 1), :] = jnp.where(row == shifted, 1.0, 0.0).astype(BF16)

    tmat[...] = jnp.zeros_like(tmat)
    tmat[0:6, 0:CH] = table_ref[...].astype(F32)
    tmat[6:7, 0:CH] = wout_ref[...].astype(F32)
    turned = jnp.transpose(tmat[...])
    embt = turned[0:CH, :].astype(BF16)
    wout = turned[0:CH, 6:7]
    wtmp[0 : 5 * CH, :] = w1_ref[RB : RB + 5 * CH, :].astype(F32)
    wtmp[5 * CH : 6 * CH - RB, :] = jnp.zeros((CH - RB, LAT), F32)
    wtmp[6 * CH - RB : 6 * CH, :] = w1_ref[0:RB, :].astype(F32)
    wfull = wtmp[...]
    wpt[...] = wfull.astype(BF16)
    wp[...] = jnp.transpose(wfull).astype(BF16)
    w2t[...] = jnp.transpose(w2_ref[...].astype(F32)).astype(BF16)

    f_out[0].wait_recv()
    r_up[0].start()
    r_dn[0].start()
    f_out[1].wait_recv()
    r_up[1].start()
    r_dn[1].start()
    f_g_up.wait_recv()
    r_part[0].start()
    f_g_dn.wait_recv()
    r_part[1].start()

    @pl.when(z == 0)
    def _():
        sib_meta.wait_recv()
        sib_feat.wait_recv()
        pl.semaphore_wait(ready, 1)
        meta_sib.start()
        f_p_sib.start()

    for c in meta:
        c.wait_recv()
    mi = dot(jnp.concatenate([mslot[8], mown[...], mslot[9]], 1), ohp[...])
    order = [mslot[0], mown[...], mslot[1], mslot[4], mslot[2], mslot[5], mslot[6], mslot[3], mslot[7]]
    mj = dot(jnp.concatenate(order, 1), ohc[...])
    off_i = jnp.where(left < ATOMS, -1.0, jnp.where(left < 2 * ATOMS, 0.0, 1.0))
    off_u = jnp.where(right < 3 * ATOMS, 0, jnp.where(right < 6 * ATOMS, 1, 2))
    rest = right - 3 * ATOMS * off_u
    off_v = jnp.where(rest < ATOMS, -1.0, jnp.where(rest < 2 * ATOMS, 0.0, 1.0))
    dx = (mj[0:1] + mj[3:4]) - (mi[0:1] + mi[3:4] + off_i)
    dy = (mj[1:2] + mj[4:5] + (off_u.astype(F32) - 1.0)) - (mi[1:2] + mi[4:5])
    dz = (mj[2:3] + mj[5:6] + off_v) - (mi[2:3] + mi[5:6])
    r2 = dx * dx + dy * dy + dz * dz + SOFTEN
    r = jnp.sqrt(r2)
    inv = 1.0 / r
    nx, ny, nz = dx * inv, dy * inv, dz * inv
    root3, root5, root15 = math.sqrt(3.0), math.sqrt(5.0), math.sqrt(15.0)
    harm = (
        root3 * nx, root3 * ny, root3 * nz, root15 * nx * ny, root15 * ny * nz,
        0.5 * root5 * (3.0 * nz * nz - 1.0), root15 * nx * nz, 0.5 * root15 * (nx * nx - ny * ny),
    )
    for m in range(8):
        yb[m] = jnp.broadcast_to(harm[m], (8, EDGES))
    orders = (lax.broadcasted_iota(jnp.int32, (RB, EDGES), 0) + 1).astype(F32)
    sin_b, cos_b = sin_cos_pi(orders * (1.0 / RADIUS) * r)
    radial = sin_b * inv
    slope = (orders * (math.pi / RADIUS) * cos_b - radial) * inv
    live = jnp.where(lax.broadcasted_iota(jnp.int32, (1, EDGES), 1) < count_ref[0, 0], 1.0, 0.0)
    gap = jnp.maximum(1.0 - r2 * (1.0 / (RADIUS * RADIUS)), 0.0)
    env = live * gap * gap
    kinds = lax.broadcasted_iota(jnp.int32, (LAT, EDGES), 0)
    for k, m in enumerate((mi, mj)):
        pick = jnp.where(kinds == m[6:7].astype(jnp.int32), 1.0, 0.0).astype(BF16)
        xbuf[CH * k : CH * (k + 1), :] = dot(embt, pick).astype(BF16)
    xbuf[5 * CH : 6 * CH - 16, :] = jnp.zeros((CH - 16, EDGES), BF16)
    xbuf[6 * CH - 16 : 6 * CH, :] = jnp.concatenate([jnp.zeros_like(radial), radial], 0).astype(BF16)

    f_part.wait_recv()
    for c in (*r_part, *r_up, *r_dn):
        c.wait_recv()
    order = [fslot[0], feat_ref[...], fslot[1], fslot[4], fslot[2], fslot[5], fslot[6], fslot[3], fslot[7]]
    gj[...] = dot(jnp.concatenate(order, 1), ohc[...])
    f_p_dn.wait_recv()
    f_p_up.wait_recv()
    gi[...] = dot(jnp.concatenate([fslot[8], feat_ref[...], fslot[9]], 1), ohp[...])

    def rows_of(ref, m, k):
        return ref[m * CH + 8 * k : m * CH + 8 * k + 8, :]

    for k2 in range(CH // 16):
        prods = [[], [], []]
        for k in (2 * k2, 2 * k2 + 1):
            sums = []
            for ref in (gi, gj):
                one = [rows_of(ref, m, k) * yb[m - 1] for m in range(1, 9)]
                sums.append((
                    rows_of(ref, 0, k),
                    one[0] + one[1] + one[2],
                    one[3] + one[4] + one[5] + one[6] + one[7],
                ))
            for l in range(3):
                si[l * CH + 8 * k : l * CH + 8 * k + 8, :] = sums[0][l]
                sj[l * CH + 8 * k : l * CH + 8 * k + 8, :] = sums[1][l]
                prods[l].append(sums[0][l] * sums[1][l])
        for l in range(3):
            start = (2 + l) * CH + 16 * k2
            xbuf[start : start + 16, :] = jnp.concatenate(prods[l], 0).astype(BF16)
    z1 = dot(wp[...], xbuf[...])
    sig1 = 1.0 / (1.0 + jnp.exp(-z1))
    z2 = dot(w2_ref[...], (z1 * sig1).astype(BF16))
    sig2 = 1.0 / (1.0 + jnp.exp(-z2))
    u = jnp.sum(wout * (z2 * sig2), 0, keepdims=True)
    energy_ref[...] = env * u

    dz2 = (wout * env) * (sig2 * (1.0 + z2 * (1.0 - sig2)))
    dh = dot(w2t[...], dz2.astype(BF16)).astype(BF16).astype(F32)
    dz1 = dh * (sig1 * (1.0 + z1 * (1.0 - sig1)))
    dxv = dot(wpt[...], dz1.astype(BF16)).astype(BF16).astype(F32)
    acc = [jnp.zeros((8, EDGES), F32) for _ in range(8)]
    for k in range(CH // 8):
        for l, ms in ((1, (1, 2, 3)), (2, (4, 5, 6, 7, 8))):
            at = slice(l * CH + 8 * k, l * CH + 8 * k + 8)
            dq = dxv[2 * CH + at.start : 2 * CH + at.stop, :]
            di, dj = dq * sj[at, :], dq * si[at, :]
            for m in ms:
                acc[m - 1] = acc[m - 1] + di * rows_of(gi, m, k) + dj * rows_of(gj, m, k)
    h1, h2, h3, h4, h5, h6, h7, h8 = (jnp.sum(a, 0, keepdims=True) for a in acc)
    ax = root3 * h1 + root15 * (ny * h4 + nz * h7 + nx * h8)
    ay = root3 * h2 + root15 * (nx * h4 + nz * h5 - ny * h8)
    az = root3 * h3 + root15 * (ny * h5 + nx * h7) + (3.0 * root5) * nz * h6
    dr = jnp.sum(dxv[6 * CH - RB : 6 * CH, :] * slope, 0, keepdims=True)
    dr = dr - (ax * nx + ay * ny + az * nz) * inv
    denv = live * u * (2.0 * gap) * (-1.0 / (RADIUS * RADIUS))
    scale = dr * inv + 2.0 * denv
    gbuf[...] = jnp.zeros_like(gbuf)
    gbuf[0:1, :] = ax * inv + dx * scale
    gbuf[1:2, :] = ay * inv + dy * scale
    gbuf[2:3, :] = az * inv + dz * scale

    grad = gbuf[...]
    g_hi = grad.astype(BF16).astype(F32)
    both = jnp.concatenate([g_hi, grad - g_hi], 0).astype(BF16)
    part_p = dot_nt(both, ohp[...])
    part_p = part_p[0:8] + part_p[8:16]
    part_c = dot_nt(both, ohc[...])
    part_c = -(part_c[0:8] + part_c[8:16])

    def lanes(a, k):
        return a[:, k * ATOMS : (k + 1) * ATOMS]

    for slot, k in enumerate((0, 2, 4, 7, 3, 5, 6, 8)):
        pout[slot] = lanes(part_c, k)
    pout[8] = lanes(part_p, 0)
    pout[9] = lanes(part_p, 2)
    back = [remote(pout.at[k], pslot.at[k], psend.at[k], precv.at[k], home[k]) for k in range(NSLOT)]
    for c in back:
        c.start()
    total = lanes(part_p, 1) + lanes(part_c, 1)
    for c in (*meta, f_g_up, f_g_dn, f_part, *f_out, f_p_up, f_p_dn, *r_part, *r_up, *r_dn):
        c.wait_send()

    @pl.when(z == 0)
    def _():
        sib_meta.wait_send()
        sib_feat.wait_send()

    for k, c in enumerate(back):
        c.wait_recv()
        total = total + pslot[k]
    for k in range(3):
        force_ref[k] = total[k : k + 1, :]
    for c in back:
        c.wait_send()


def shards(positions, features, species, emb_table, edges, edge_count, w_first, w_second, w_out):
    vmem = pl.BlockSpec(memory_space=pltpu.VMEM)
    hbm = pl.BlockSpec(memory_space=pl.ANY)
    dma = pltpu.SemaphoreType.DMA
    pos = jnp.transpose(positions.reshape(1, 3, ATOMS), (1, 0, 2))
    feat = features.reshape(ROWS, ATOMS)
    spec = species.reshape(1, ATOMS)
    small = [pltpu.VMEM((3, 1, ATOMS), F32), pltpu.VMEM((1, ATOMS), jnp.int32)]
    forces, energy = pl.pallas_call(
        kernel,
        name="edge_forces",
        out_shape=(pltpu.VMEM((3, 1, ATOMS), F32), pltpu.VMEM((1, EDGES), F32)),
        in_specs=[hbm] * 9,
        out_specs=(vmem, vmem),
        scratch_shapes=[
            small[0],
            pltpu.VMEM((ROWS, ATOMS), BF16),
            small[1],
            pltpu.VMEM((2, EDGES), jnp.int32),
            pltpu.SMEM((1, 1), jnp.int32),
            pltpu.VMEM((6, CH), BF16),
            pltpu.VMEM((RB + 5 * CH, LAT), BF16),
            pltpu.VMEM((CH, LAT), BF16),
            pltpu.VMEM((1, CH), BF16),
            pltpu.VMEM((ROWS, ATOMS), BF16),
            pltpu.VMEM((16, ATOMS), BF16),
            pltpu.VMEM((NSLOT, ROWS, ATOMS), BF16),
            pltpu.VMEM((16, ATOMS), BF16),
            pltpu.VMEM((NSLOT, 16, ATOMS), BF16),
            pltpu.VMEM((3 * ATOMS, EDGES), BF16),
            pltpu.VMEM((9 * ATOMS, EDGES), BF16),
            pltpu.VMEM((ROWS, EDGES), F32),
            pltpu.VMEM((ROWS, EDGES), F32),
            pltpu.VMEM((3 * CH, EDGES), F32),
            pltpu.VMEM((3 * CH, EDGES), F32),
            pltpu.VMEM((8, 8, EDGES), F32),
            pltpu.VMEM((6 * CH, EDGES), BF16),
            pltpu.VMEM((6 * CH, LAT), F32),
            pltpu.VMEM((LAT, 6 * CH), BF16),
            pltpu.VMEM((6 * CH, LAT), BF16),
            pltpu.VMEM((LAT, CH), BF16),
            pltpu.VMEM((LAT, LAT), F32),
            pltpu.VMEM((8, EDGES), F32),
            pltpu.VMEM((16, ATOMS), F32),
            pltpu.VMEM((NSLOT, 8, ATOMS), F32),
            pltpu.VMEM((NSLOT, 8, ATOMS), F32),
            dma((9,)),
            pltpu.SemaphoreType.REGULAR,
            dma((NSLOT,)),
            dma((NSLOT,)),
            dma((15,)),
            dma((15,)),
            dma((NSLOT,)),
            dma((NSLOT,)),
        ],
        compiler_params=pltpu.CompilerParams(collective_id=0, has_side_effects=True),
    )(
        pos,
        feat,
        spec,
        edges.reshape(2, EDGES),
        edge_count.reshape(1, 1),
        emb_table,
        w_first.T,
        w_second,
        w_out.reshape(1, CH),
    )
    return (
        jnp.transpose(forces, (1, 0, 2)).reshape(1, 1, 1, 3, ATOMS),
        energy.reshape(1, 1, 1, EDGES),
    )


def solution(mesh):
    placed = (
        P("plate", "tower", "gz", None, None),
        P("plate", "tower", "gz", None, None),
        P("plate", "tower", "gz", None),
        P(),
        P("plate", "tower", "gz", None, None),
        P("plate", "tower", "gz"),
        P(),
        P(),
        P(),
    )
    return jax.shard_map(
        shards,
        mesh=mesh,
        in_specs=placed,
        out_specs=(P("plate", "tower", "gz", None, None), P("plate", "tower", "gz", None)),
        check_vma=False,
    )
```

```python
import math

import jax
import jax.numpy as jnp
from jax import lax
from jax.experimental import pallas as pl
from jax.experimental.pallas import tpu as pltpu
from jax.sharding import PartitionSpec as P

ATOMS = 128
EDGES = 512
CH = 64
LAT = 128
RB = 8
ROWS = 9 * CH
HALF = ROWS // 2
RADIUS = 3.0
SOFTEN = 0.04
F32 = jnp.float32
BF16 = jnp.bfloat16

NSLOT = 10


def dot(a, b):
    return lax.dot_general(a, b, (((1,), (0,)), ((), ())), preferred_element_type=F32)


def dot_nt(a, b):
    return lax.dot_general(a, b, (((1,), (1,)), ((), ())), preferred_element_type=F32)


def sin_cos_pi(t):
    turns = jnp.floor(t + 0.5)
    x = (t - turns) * math.pi
    parity = turns - 2.0 * jnp.floor(turns * 0.5)
    sign = 1.0 - 2.0 * parity
    y = x * x
    s = -1.0 / 39916800.0
    for c in (1.0 / 362880.0, -1.0 / 5040.0, 1.0 / 120.0, -1.0 / 6.0, 1.0):
        s = s * y + c
    c_ = 1.0 / 479001600.0
    for c in (-1.0 / 3628800.0, 1.0 / 40320.0, -1.0 / 720.0, 1.0 / 24.0, -0.5, 1.0):
        c_ = c_ * y + c
    return sign * s * x, sign * c_


def remote(src, dst, ssem, rsem, to):
    return pltpu.make_async_remote_copy(
        src_ref=src,
        dst_ref=dst,
        send_sem=ssem,
        recv_sem=rsem,
        device_id=to,
        device_id_type=pl.DeviceIdType.MESH,
    )


def fetch(pairs, sems):
    copies = [pltpu.make_async_copy(src, dst, sems.at[n]) for n, (src, dst) in enumerate(pairs)]
    for c in copies:
        c.start()
    return copies


def pack_small(pos, spec, stage, out):
    stage[...] = jnp.zeros_like(stage)
    for k in range(3):
        hi = pos[k].astype(BF16).astype(F32)
        stage[k : k + 1, :] = hi
        stage[k + 3 : k + 4, :] = (pos[k] - hi).astype(BF16).astype(F32)
    stage[6:7, :] = spec[...].astype(F32)
    out[...] = stage[...].astype(BF16)


DEPTH = 16


def kernel(
    pos_any,
    feat_any,
    spec_any,
    edges_any,
    count_any,
    table_any,
    w1_any,
    w2_any,
    wout_any,
    force_ref,
    energy_ref,
    pos,
    feat_ref,
    spec_ref,
    edges_ref,
    count_ref,
    table_ref,
    w1_ref,
    w2_ref,
    wout_ref,
    sib_f,
    sib_m,
    fslot,
    mown,
    mslot,
    ohp,
    ohc,
    gi,
    gj,
    si,
    sj,
    yb,
    xbuf,
    wtmp,
    wp,
    wpt,
    w2t,
    tmat,
    gbuf,
    stage,
    pout,
    pslot,
    lsem,
    ready,
    go,
    msend,
    mrecv,
    fsend,
    frecv,
    psend,
    precv,
):
    n_plate, n_tower, n_gz = (lax.axis_size(a) for a in ("plate", "tower", "gz"))
    p, t, g = (lax.axis_index(a) for a in ("plate", "tower", "gz"))
    odd = lax.rem(t, 2)
    partner = t + 1 - 2 * odd
    outward = lax.rem(t + 2 * odd - 1 + n_tower, n_tower)
    g_up, g_dn = lax.rem(g + 1, n_gz), lax.rem(g + n_gz - 1, n_gz)
    p_up, p_dn = lax.rem(p + 1, n_plate), lax.rem(p + n_plate - 1, n_plate)
    z = lax.rem(p, DEPTH)
    last = z // (DEPTH - 1)
    first = lax.rem(z + DEPTH - 1, DEPTH) // (DEPTH - 1)

    total = n_plate * n_tower * n_gz

    def dev(pp, tt, gg):
        return {"plate": pp, "tower": tt, "gz": gg}

    def is_late(d):
        return 1 - ((d["plate"] * n_tower + d["tower"]) * n_gz + d["gz"] + total - 1) // total


    dest = [
        dev(p, t, g_up), dev(p, t, g_dn), dev(p, partner, g), dev(p, outward, g),
        dev(p, partner, g_up), dev(p, partner, g_dn), dev(p, outward, g_up), dev(p, outward, g_dn),
        dev(p_up, t, g), dev(p_dn, t, g),
    ]
    home = [dest[k] for k in (1, 0, 2, 3, 5, 4, 7, 6, 9, 8)]
    sibling = dev(lax.rem(p + DEPTH, n_plate), t, g)
    below = dev(lax.rem(p + n_plate - 1 + DEPTH * first, n_plate), t, g)
    above = dev(lax.rem(p + 1 + DEPTH, n_plate), t, g)

    barrier = pltpu.get_barrier_semaphore()

    def greet(d):
        pl.semaphore_signal(barrier, inc=1, device_id=d, device_id_type=pl.DeviceIdType.MESH)

    late = is_late(dev(p, t, g))
    late_to = [is_late(d) for d in dest[:4]]
    late_sib = first * is_late(sibling)
    near = late_to[0] + late_to[1] + late_to[2] + late_to[3] + late_sib

    greet(below)

    @pl.when(late == 0)
    def _():
        for d in dest[:4]:
            greet(d)

    @pl.when(z == 0)
    def _():
        greet(dest[9])

    @pl.when(first - late == 1)
    def _():
        greet(sibling)

    @pl.when(last == 0)
    def _():
        greet(dest[8])

    small = fetch(
        [
            (pos_any, pos), (spec_any, spec_ref), (feat_any, feat_ref), (edges_any, edges_ref), (count_any, count_ref),
            (table_any, table_ref), (w1_any, w1_ref), (w2_any, w2_ref), (wout_any, wout_ref),
        ],
        lsem,
    )
    small, rest = small[:2], small[2:]
    for c in small:
        c.wait()
    pack_small(pos, spec_ref, stage, mown)

    def small_rows(src, k, to):
        return remote(src, mslot.at[k], msend.at[k], mrecv.at[k], to)

    meta = [small_rows(mown, k, dest[k]) for k in range(4)]
    m_part = [small_rows(mslot.at[k], 4 + k, dest[2]) for k in range(2)]
    m_up, m_dn = small_rows(mslot.at[3], 6, dest[0]), small_rows(mslot.at[3], 7, dest[1])
    meta += [*m_part, m_up, m_dn, small_rows(mown, 8, dest[8]), small_rows(mown, 9, below)]
    meta_sib = remote(sib_m, mslot.at[9], msend.at[9], mrecv.at[9], below)
    top, low = pl.ds(0, HALF), pl.ds(HALF, HALF)

    def feature(n, src, slot, to, part=None):
        dst = fslot.at[slot]
        if part is not None:
            src, dst = src.at[part], dst.at[part]
        return remote(src, dst, fsend.at[n], frecv.at[n], to)

    f_g_up = feature(0, feat_ref, 0, dest[0])
    f_g_dn = feature(1, feat_ref, 1, dest[1])
    f_part = feature(2, feat_ref, 2, dest[2])
    f_out = [feature(3, feat_ref, 3, dest[3], top), feature(4, feat_ref, 3, dest[3], low)]
    f_p_dn = feature(6, feat_ref, 9, below)
    f_p_sib = feature(6, sib_f, 9, below)
    f_p_up = feature(5, feat_ref, 8, dest[8])
    sib_feat = remote(feat_ref, sib_f, fsend.at[13], frecv.at[13], sibling)
    sib_meta = remote(mown, sib_m, fsend.at[14], frecv.at[14], sibling)
    r_part = [feature(7, fslot.at[0], 4, dest[2]), feature(8, fslot.at[1], 5, dest[2])]
    r_up = [feature(9, fslot.at[3], 6, dest[0], top), feature(10, fslot.at[3], 6, dest[0], low)]
    r_dn = [feature(11, fslot.at[3], 7, dest[1], top), feature(12, fslot.at[3], 7, dest[1], low)]

    rest[0].wait()
    pl.semaphore_wait(barrier, 6 + last - near)

    def tell(sem, d):
        pl.semaphore_signal(sem, inc=1, device_id=d, device_id_type=pl.DeviceIdType.MESH)

    @pl.when(last == 1)
    def _():
        tell(ready, above)

    @pl.when(late == 1)
    def _():
        for d in (*dest[:4], sibling):
            tell(go, d)

    @pl.when(first - late_sib == 1)
    def _():
        sib_meta.start()
        sib_feat.start()

    direct = ((meta[0], f_g_up), (meta[1], f_g_dn), (meta[2], f_part), (meta[3], *f_out))
    meta[8].start()
    f_p_up.start()

    @pl.when(z != 0)
    def _():
        meta[9].start()
        f_p_dn.start()

    for k in (3, 0, 1, 2):

        @pl.when(late_to[k] == 0)
        def _(k=k):
            for c in direct[k]:
                c.start()

    for c in rest[1:]:
        c.wait()

    left, right = edges_ref[0:1, :], edges_ref[1:2, :]
    row = lax.broadcasted_iota(jnp.int32, (3 * ATOMS, EDGES), 0)
    ohp[...] = jnp.where(row == left, 1.0, 0.0).astype(BF16)
    for k, u in enumerate((1, 2 - 2 * odd, 2 * odd)):
        shifted = right - 3 * ATOMS * u
        ohc[3 * ATOMS * k : 3 * ATOMS * (k + 1), :] = jnp.where(row == shifted, 1.0, 0.0).astype(BF16)

    tmat[...] = jnp.zeros_like(tmat)
    tmat[0:6, 0:CH] = table_ref[...].astype(F32)
    tmat[6:7, 0:CH] = wout_ref[...].astype(F32)
    turned = jnp.transpose(tmat[...])
    embt = turned[0:CH, :].astype(BF16)
    wout = turned[0:CH, 6:7]
    wtmp[0 : 5 * CH, :] = w1_ref[RB : RB + 5 * CH, :].astype(F32)
    wtmp[5 * CH : 6 * CH - RB, :] = jnp.zeros((CH - RB, LAT), F32)
    wtmp[6 * CH - RB : 6 * CH, :] = w1_ref[0:RB, :].astype(F32)
    wfull = wtmp[...]
    wpt[...] = wfull.astype(BF16)
    wp[...] = jnp.transpose(wfull).astype(BF16)
    w2t[...] = jnp.transpose(w2_ref[...].astype(F32)).astype(BF16)

    @pl.when(near == 1)
    def _():
        pl.semaphore_wait(go, 1)

        @pl.when(late_sib == 1)
        def _():
            sib_meta.start()
            sib_feat.start()

        for k in (3, 0, 1, 2):

            @pl.when(late_to[k] == 1)
            def _(k=k):
                for c in direct[k]:
                    c.start()

    meta[3].wait_recv()
    m_up.start()
    m_dn.start()
    f_out[0].wait_recv()
    r_up[0].start()
    r_dn[0].start()
    f_out[1].wait_recv()
    r_up[1].start()
    r_dn[1].start()
    for k, c in enumerate((f_g_up, f_g_dn)):
        meta[k].wait_recv()
        m_part[k].start()
        c.wait_recv()
        r_part[k].start()

    @pl.when(z == 0)
    def _():
        sib_meta.wait_recv()
        sib_feat.wait_recv()
        pl.semaphore_wait(ready, 1)
        meta_sib.start()
        f_p_sib.start()

    for c in (meta[2], *meta[8:], m_up, m_dn, *m_part):
        c.wait_recv()
    mi = dot(jnp.concatenate([mslot[8], mown[...], mslot[9]], 1), ohp[...])
    order = [mslot[0], mown[...], mslot[1], mslot[4], mslot[2], mslot[5], mslot[6], mslot[3], mslot[7]]
    mj = dot(jnp.concatenate(order, 1), ohc[...])
    off_i = jnp.where(left < ATOMS, -1.0, jnp.where(left < 2 * ATOMS, 0.0, 1.0))
    off_u = jnp.where(right < 3 * ATOMS, 0, jnp.where(right < 6 * ATOMS, 1, 2))
    rest = right - 3 * ATOMS * off_u
    off_v = jnp.where(rest < ATOMS, -1.0, jnp.where(rest < 2 * ATOMS, 0.0, 1.0))
    dx = (mj[0:1] + mj[3:4]) - (mi[0:1] + mi[3:4] + off_i)
    dy = (mj[1:2] + mj[4:5] + (off_u.astype(F32) - 1.0)) - (mi[1:2] + mi[4:5])
    dz = (mj[2:3] + mj[5:6] + off_v) - (mi[2:3] + mi[5:6])
    r2 = dx * dx + dy * dy + dz * dz + SOFTEN
    r = jnp.sqrt(r2)
    inv = 1.0 / r
    nx, ny, nz = dx * inv, dy * inv, dz * inv
    root3, root5, root15 = math.sqrt(3.0), math.sqrt(5.0), math.sqrt(15.0)
    harm = (
        root3 * nx, root3 * ny, root3 * nz, root15 * nx * ny, root15 * ny * nz,
        0.5 * root5 * (3.0 * nz * nz - 1.0), root15 * nx * nz, 0.5 * root15 * (nx * nx - ny * ny),
    )
    for m in range(8):
        yb[m] = jnp.broadcast_to(harm[m], (8, EDGES))
    orders = (lax.broadcasted_iota(jnp.int32, (RB, EDGES), 0) + 1).astype(F32)
    sin_b, cos_b = sin_cos_pi(orders * (1.0 / RADIUS) * r)
    radial = sin_b * inv
    slope = (orders * (math.pi / RADIUS) * cos_b - radial) * inv
    live = jnp.where(lax.broadcasted_iota(jnp.int32, (1, EDGES), 1) < count_ref[0, 0], 1.0, 0.0)
    gap = jnp.maximum(1.0 - r2 * (1.0 / (RADIUS * RADIUS)), 0.0)
    env = live * gap * gap
    kinds = lax.broadcasted_iota(jnp.int32, (LAT, EDGES), 0)
    for k, m in enumerate((mi, mj)):
        pick = jnp.where(kinds == m[6:7].astype(jnp.int32), 1.0, 0.0).astype(BF16)
        xbuf[CH * k : CH * (k + 1), :] = dot(embt, pick).astype(BF16)
    xbuf[5 * CH : 6 * CH - 16, :] = jnp.zeros((CH - 16, EDGES), BF16)
    xbuf[6 * CH - 16 : 6 * CH, :] = jnp.concatenate([jnp.zeros_like(radial), radial], 0).astype(BF16)

    f_part.wait_recv()
    for c in (*r_part, *r_up, *r_dn):
        c.wait_recv()
    order = [fslot[0], feat_ref[...], fslot[1], fslot[4], fslot[2], fslot[5], fslot[6], fslot[3], fslot[7]]
    gj[...] = dot(jnp.concatenate(order, 1), ohc[...])
    f_p_dn.wait_recv()
    f_p_up.wait_recv()
    gi[...] = dot(jnp.concatenate([fslot[8], feat_ref[...], fslot[9]], 1), ohp[...])

    def rows_of(ref, m, k):
        return ref[m * CH + 8 * k : m * CH + 8 * k + 8, :]

    for k2 in range(CH // 16):
        prods = [[], [], []]
        for k in (2 * k2, 2 * k2 + 1):
            sums = []
            for ref in (gi, gj):
                one = [rows_of(ref, m, k) * yb[m - 1] for m in range(1, 9)]
                sums.append((
                    rows_of(ref, 0, k),
                    one[0] + one[1] + one[2],
                    one[3] + one[4] + one[5] + one[6] + one[7],
                ))
            for l in range(3):
                si[l * CH + 8 * k : l * CH + 8 * k + 8, :] = sums[0][l]
                sj[l * CH + 8 * k : l * CH + 8 * k + 8, :] = sums[1][l]
                prods[l].append(sums[0][l] * sums[1][l])
        for l in range(3):
            start = (2 + l) * CH + 16 * k2
            xbuf[start : start + 16, :] = jnp.concatenate(prods[l], 0).astype(BF16)
    z1 = dot(wp[...], xbuf[...])
    sig1 = 1.0 / (1.0 + jnp.exp(-z1))
    z2 = dot(w2_ref[...], (z1 * sig1).astype(BF16))
    sig2 = 1.0 / (1.0 + jnp.exp(-z2))
    u = jnp.sum(wout * (z2 * sig2), 0, keepdims=True)
    energy_ref[...] = env * u

    dz2 = (wout * env) * (sig2 * (1.0 + z2 * (1.0 - sig2)))
    dh = dot(w2t[...], dz2.astype(BF16)).astype(BF16).astype(F32)
    dz1 = dh * (sig1 * (1.0 + z1 * (1.0 - sig1)))
    dxv = dot(wpt[...], dz1.astype(BF16)).astype(BF16).astype(F32)
    acc = [jnp.zeros((8, EDGES), F32) for _ in range(8)]
    for k in range(CH // 8):
        for l, ms in ((1, (1, 2, 3)), (2, (4, 5, 6, 7, 8))):
            at = slice(l * CH + 8 * k, l * CH + 8 * k + 8)
            dq = dxv[2 * CH + at.start : 2 * CH + at.stop, :]
            di, dj = dq * sj[at, :], dq * si[at, :]
            for m in ms:
                acc[m - 1] = acc[m - 1] + di * rows_of(gi, m, k) + dj * rows_of(gj, m, k)
    h1, h2, h3, h4, h5, h6, h7, h8 = (jnp.sum(a, 0, keepdims=True) for a in acc)
    ax = root3 * h1 + root15 * (ny * h4 + nz * h7 + nx * h8)
    ay = root3 * h2 + root15 * (nx * h4 + nz * h5 - ny * h8)
    az = root3 * h3 + root15 * (ny * h5 + nx * h7) + (3.0 * root5) * nz * h6
    dr = jnp.sum(dxv[6 * CH - RB : 6 * CH, :] * slope, 0, keepdims=True)
    dr = dr - (ax * nx + ay * ny + az * nz) * inv
    denv = live * u * (2.0 * gap) * (-1.0 / (RADIUS * RADIUS))
    scale = dr * inv + 2.0 * denv
    gbuf[...] = jnp.zeros_like(gbuf)
    gbuf[0:1, :] = ax * inv + dx * scale
    gbuf[1:2, :] = ay * inv + dy * scale
    gbuf[2:3, :] = az * inv + dz * scale

    grad = gbuf[...]
    g_hi = grad.astype(BF16).astype(F32)
    both = jnp.concatenate([g_hi, grad - g_hi], 0).astype(BF16)
    part_p = dot_nt(both, ohp[...])
    part_p = part_p[0:8] + part_p[8:16]
    part_c = dot_nt(both, ohc[...])
    part_c = -(part_c[0:8] + part_c[8:16])

    def lanes(a, k):
        return a[:, k * ATOMS : (k + 1) * ATOMS]

    for slot, k in enumerate((0, 2, 4, 7, 3, 5, 6, 8)):
        pout[slot] = lanes(part_c, k)
    pout[8] = lanes(part_p, 0)
    pout[9] = lanes(part_p, 2)
    back = [remote(pout.at[k], pslot.at[k], psend.at[k], precv.at[k], home[k]) for k in range(NSLOT)]
    for c in back:
        c.start()
    force = lanes(part_p, 1) + lanes(part_c, 1)
    for c in (*meta, f_g_up, f_g_dn, f_part, *f_out, f_p_up, f_p_dn, *r_part, *r_up, *r_dn):
        c.wait_send()

    @pl.when(z == 0)
    def _():
        sib_meta.wait_send()
        sib_feat.wait_send()

    for k, c in enumerate(back):
        c.wait_recv()
        force = force + pslot[k]
    for k in range(3):
        force_ref[k] = force[k : k + 1, :]
    for c in back:
        c.wait_send()


def shards(positions, features, species, emb_table, edges, edge_count, w_first, w_second, w_out):
    vmem = pl.BlockSpec(memory_space=pltpu.VMEM)
    hbm = pl.BlockSpec(memory_space=pl.ANY)
    dma = pltpu.SemaphoreType.DMA
    pos = jnp.transpose(positions.reshape(1, 3, ATOMS), (1, 0, 2))
    feat = features.reshape(ROWS, ATOMS)
    spec = species.reshape(1, ATOMS)
    small = [pltpu.VMEM((3, 1, ATOMS), F32), pltpu.VMEM((1, ATOMS), jnp.int32)]
    forces, energy = pl.pallas_call(
        kernel,
        name="edge_forces",
        out_shape=(pltpu.VMEM((3, 1, ATOMS), F32), pltpu.VMEM((1, EDGES), F32)),
        in_specs=[hbm] * 9,
        out_specs=(vmem, vmem),
        scratch_shapes=[
            small[0],
            pltpu.VMEM((ROWS, ATOMS), BF16),
            small[1],
            pltpu.VMEM((2, EDGES), jnp.int32),
            pltpu.SMEM((1, 1), jnp.int32),
            pltpu.VMEM((6, CH), BF16),
            pltpu.VMEM((RB + 5 * CH, LAT), BF16),
            pltpu.VMEM((CH, LAT), BF16),
            pltpu.VMEM((1, CH), BF16),
            pltpu.VMEM((ROWS, ATOMS), BF16),
            pltpu.VMEM((16, ATOMS), BF16),
            pltpu.VMEM((NSLOT, ROWS, ATOMS), BF16),
            pltpu.VMEM((16, ATOMS), BF16),
            pltpu.VMEM((NSLOT, 16, ATOMS), BF16),
            pltpu.VMEM((3 * ATOMS, EDGES), BF16),
            pltpu.VMEM((9 * ATOMS, EDGES), BF16),
            pltpu.VMEM((ROWS, EDGES), F32),
            pltpu.VMEM((ROWS, EDGES), F32),
            pltpu.VMEM((3 * CH, EDGES), F32),
            pltpu.VMEM((3 * CH, EDGES), F32),
            pltpu.VMEM((8, 8, EDGES), F32),
            pltpu.VMEM((6 * CH, EDGES), BF16),
            pltpu.VMEM((6 * CH, LAT), F32),
            pltpu.VMEM((LAT, 6 * CH), BF16),
            pltpu.VMEM((6 * CH, LAT), BF16),
            pltpu.VMEM((LAT, CH), BF16),
            pltpu.VMEM((LAT, LAT), F32),
            pltpu.VMEM((8, EDGES), F32),
            pltpu.VMEM((16, ATOMS), F32),
            pltpu.VMEM((NSLOT, 8, ATOMS), F32),
            pltpu.VMEM((NSLOT, 8, ATOMS), F32),
            dma((9,)),
            pltpu.SemaphoreType.REGULAR,
            pltpu.SemaphoreType.REGULAR,
            dma((NSLOT,)),
            dma((NSLOT,)),
            dma((15,)),
            dma((15,)),
            dma((NSLOT,)),
            dma((NSLOT,)),
        ],
        compiler_params=pltpu.CompilerParams(collective_id=0, has_side_effects=True),
    )(
        pos,
        feat,
        spec,
        edges.reshape(2, EDGES),
        edge_count.reshape(1, 1),
        emb_table,
        w_first.T,
        w_second,
        w_out.reshape(1, CH),
    )
    return (
        jnp.transpose(forces, (1, 0, 2)).reshape(1, 1, 1, 3, ATOMS),
        energy.reshape(1, 1, 1, EDGES),
    )


def solution(mesh):
    placed = (
        P("plate", "tower", "gz", None, None),
        P("plate", "tower", "gz", None, None),
        P("plate", "tower", "gz", None),
        P(),
        P("plate", "tower", "gz", None, None),
        P("plate", "tower", "gz"),
        P(),
        P(),
        P(),
    )
    return jax.shard_map(
        shards,
        mesh=mesh,
        in_specs=placed,
        out_specs=(P("plate", "tower", "gz", None, None), P("plate", "tower", "gz", None)),
        check_vma=False,
    )
```

```python
import math

import jax
import jax.numpy as jnp
from jax import lax
from jax.experimental import pallas as pl
from jax.experimental.pallas import tpu as pltpu
from jax.sharding import PartitionSpec as P

ATOMS = 128
EDGES = 512
CH = 64
LAT = 128
RB = 8
ROWS = 9 * CH
HALF = ROWS // 2
RADIUS = 3.0
SOFTEN = 0.04
F32 = jnp.float32
BF16 = jnp.bfloat16

NSLOT = 10


def dot(a, b):
    return lax.dot_general(a, b, (((1,), (0,)), ((), ())), preferred_element_type=F32)


def sin_cos_pi(t):
    turns = jnp.floor(t + 0.5)
    x = (t - turns) * math.pi
    parity = turns - 2.0 * jnp.floor(turns * 0.5)
    sign = 1.0 - 2.0 * parity
    y = x * x
    s = -1.0 / 39916800.0
    for c in (1.0 / 362880.0, -1.0 / 5040.0, 1.0 / 120.0, -1.0 / 6.0, 1.0):
        s = s * y + c
    c_ = 1.0 / 479001600.0
    for c in (-1.0 / 3628800.0, 1.0 / 40320.0, -1.0 / 720.0, 1.0 / 24.0, -0.5, 1.0):
        c_ = c_ * y + c
    return sign * s * x, sign * c_


def remote(src, dst, ssem, rsem, to):
    return pltpu.make_async_remote_copy(
        src_ref=src,
        dst_ref=dst,
        send_sem=ssem,
        recv_sem=rsem,
        device_id=to,
        device_id_type=pl.DeviceIdType.MESH,
    )


def fetch(pairs, sems):
    copies = [pltpu.make_async_copy(src, dst, sems.at[n]) for n, (src, dst) in enumerate(pairs)]
    for c in copies:
        c.start()
    return copies


def pack_small(pos, spec, stage, out):
    stage[...] = jnp.zeros_like(stage)
    for k in range(3):
        hi = pos[k].astype(BF16).astype(F32)
        stage[k : k + 1, :] = hi
        stage[k + 3 : k + 4, :] = (pos[k] - hi).astype(BF16).astype(F32)
    stage[6:7, :] = spec[...].astype(F32)
    out[...] = stage[...].astype(BF16)


DEPTH = 16


def kernel(
    pos_any,
    feat_any,
    spec_any,
    edges_any,
    count_any,
    table_any,
    w1_any,
    w2_any,
    wout_any,
    force_ref,
    energy_ref,
    pos,
    feat_ref,
    spec_ref,
    edges_ref,
    count_ref,
    table_ref,
    w1_ref,
    w2_ref,
    wout_ref,
    sib_f,
    sib_m,
    fslot,
    mown,
    mslot,
    ohp,
    ohc,
    ohpt,
    ohct,
    gi,
    gj,
    si,
    sj,
    yb,
    xbuf,
    wtmp,
    wp,
    wpt,
    w2t,
    tmat,
    gbuf,
    stage,
    pout,
    pslot,
    lsem,
    ready,
    go,
    msend,
    mrecv,
    fsend,
    frecv,
    psend,
    precv,
):
    n_plate, n_tower, n_gz = (lax.axis_size(a) for a in ("plate", "tower", "gz"))
    p, t, g = (lax.axis_index(a) for a in ("plate", "tower", "gz"))
    odd = lax.rem(t, 2)
    partner = t + 1 - 2 * odd
    outward = lax.rem(t + 2 * odd - 1 + n_tower, n_tower)
    g_up, g_dn = lax.rem(g + 1, n_gz), lax.rem(g + n_gz - 1, n_gz)
    p_up, p_dn = lax.rem(p + 1, n_plate), lax.rem(p + n_plate - 1, n_plate)
    z = lax.rem(p, DEPTH)
    last = z // (DEPTH - 1)
    first = lax.rem(z + DEPTH - 1, DEPTH) // (DEPTH - 1)

    total = n_plate * n_tower * n_gz

    def dev(pp, tt, gg):
        return {"plate": pp, "tower": tt, "gz": gg}

    def is_late(d):
        return 1 - ((d["plate"] * n_tower + d["tower"]) * n_gz + d["gz"] + total - 1) // total


    dest = [
        dev(p, t, g_up), dev(p, t, g_dn), dev(p, partner, g), dev(p, outward, g),
        dev(p, partner, g_up), dev(p, partner, g_dn), dev(p, outward, g_up), dev(p, outward, g_dn),
        dev(p_up, t, g), dev(p_dn, t, g),
    ]
    home = [dest[k] for k in (1, 0, 2, 3, 5, 4, 7, 6, 9, 8)]
    sibling = dev(lax.rem(p + DEPTH, n_plate), t, g)
    below = dev(lax.rem(p + n_plate - 1 + DEPTH * first, n_plate), t, g)
    above = dev(lax.rem(p + 1 + DEPTH, n_plate), t, g)

    barrier = pltpu.get_barrier_semaphore()

    def greet(d):
        pl.semaphore_signal(barrier, inc=1, device_id=d, device_id_type=pl.DeviceIdType.MESH)

    late = is_late(dev(p, t, g))
    late_to = [is_late(d) for d in dest[:4]]
    late_sib = first * is_late(sibling)
    near = late_to[0] + late_to[1] + late_to[2] + late_to[3] + late_sib

    greet(below)

    @pl.when(late == 0)
    def _():
        for d in dest[:4]:
            greet(d)

    @pl.when(z == 0)
    def _():
        greet(dest[9])

    @pl.when(first - late == 1)
    def _():
        greet(sibling)

    @pl.when(last == 0)
    def _():
        greet(dest[8])

    small = fetch(
        [
            (pos_any, pos), (spec_any, spec_ref), (feat_any, feat_ref), (edges_any, edges_ref), (count_any, count_ref),
            (table_any, table_ref), (w1_any, w1_ref), (w2_any, w2_ref), (wout_any, wout_ref),
        ],
        lsem,
    )
    small, rest = small[:2], small[2:]
    for c in small:
        c.wait()
    pack_small(pos, spec_ref, stage, mown)

    def small_rows(src, k, to):
        return remote(src, mslot.at[k], msend.at[k], mrecv.at[k], to)

    meta = [small_rows(mown, k, dest[k]) for k in range(4)]
    m_part = [small_rows(mslot.at[k], 4 + k, dest[2]) for k in range(2)]
    m_up, m_dn = small_rows(mslot.at[3], 6, dest[0]), small_rows(mslot.at[3], 7, dest[1])
    meta += [*m_part, m_up, m_dn, small_rows(mown, 8, dest[8]), small_rows(mown, 9, below)]
    meta_sib = remote(sib_m, mslot.at[9], msend.at[9], mrecv.at[9], below)
    top, low = pl.ds(0, HALF), pl.ds(HALF, HALF)

    def feature(n, src, slot, to, part=None):
        dst = fslot.at[slot]
        if part is not None:
            src, dst = src.at[part], dst.at[part]
        return remote(src, dst, fsend.at[n], frecv.at[n], to)

    f_g_up = feature(0, feat_ref, 0, dest[0])
    f_g_dn = feature(1, feat_ref, 1, dest[1])
    f_part = feature(2, feat_ref, 2, dest[2])
    f_out = [feature(3, feat_ref, 3, dest[3], top), feature(4, feat_ref, 3, dest[3], low)]
    f_p_dn = feature(6, feat_ref, 9, below)
    f_p_sib = feature(6, sib_f, 9, below)
    f_p_up = feature(5, feat_ref, 8, dest[8])
    sib_feat = remote(feat_ref, sib_f, fsend.at[13], frecv.at[13], sibling)
    sib_meta = remote(mown, sib_m, fsend.at[14], frecv.at[14], sibling)
    r_part = [feature(7, fslot.at[0], 4, dest[2]), feature(8, fslot.at[1], 5, dest[2])]
    r_up = [feature(9, fslot.at[3], 6, dest[0], top), feature(10, fslot.at[3], 6, dest[0], low)]
    r_dn = [feature(11, fslot.at[3], 7, dest[1], top), feature(12, fslot.at[3], 7, dest[1], low)]

    rest[0].wait()
    pl.semaphore_wait(barrier, 6 + last - near)

    def tell(sem, d):
        pl.semaphore_signal(sem, inc=1, device_id=d, device_id_type=pl.DeviceIdType.MESH)

    @pl.when(last == 1)
    def _():
        tell(ready, above)

    @pl.when(late == 1)
    def _():
        for d in (*dest[:4], sibling):
            tell(go, d)

    @pl.when(first - late_sib == 1)
    def _():
        sib_meta.start()
        sib_feat.start()

    direct = ((meta[0], f_g_up), (meta[1], f_g_dn), (meta[2], f_part), (meta[3], *f_out))
    meta[8].start()
    f_p_up.start()

    @pl.when(z != 0)
    def _():
        meta[9].start()
        f_p_dn.start()

    for k in (3, 0, 1, 2):

        @pl.when(late_to[k] == 0)
        def _(k=k):
            for c in direct[k]:
                c.start()

    for c in rest[1:]:
        c.wait()

    left, right = edges_ref[0:1, :], edges_ref[1:2, :]
    row = lax.broadcasted_iota(jnp.int32, (ATOMS, EDGES), 0)
    lane = lax.broadcasted_iota(jnp.int32, (EDGES, ATOMS), 1)

    def column_of(index):
        turned = jnp.transpose(jnp.broadcast_to(index.astype(F32), (8, EDGES)))
        return jnp.broadcast_to(turned[:, 0:1].astype(jnp.int32), (EDGES, ATOMS))

    left_col, right_col = column_of(left), column_of(right)

    def one_hot(match):
        return jnp.where(match, 1.0, 0.0).astype(BF16)

    for k in range(3):
        base = ATOMS * k
        ohp[base : base + ATOMS, :] = one_hot(row == left - base)
        ohpt[:, base : base + ATOMS] = one_hot(lane == left_col - base)
    u_part, u_out = 2 - 2 * odd, 2 * odd
    places = ((1, 0), (1, 1), (1, 2), (u_part, 1), (u_out, 1), (u_part, 0), (u_part, 2), (u_out, 0), (u_out, 2))
    for k, (u, v) in enumerate(places):
        base = (3 * u + v) * ATOMS
        ohc[ATOMS * k : ATOMS * (k + 1), :] = one_hot(row == right - base)
        ohct[:, ATOMS * k : ATOMS * (k + 1)] = one_hot(lane == right_col - base)

    tmat[...] = jnp.zeros_like(tmat)
    tmat[0:6, 0:CH] = table_ref[...].astype(F32)
    tmat[6:7, 0:CH] = wout_ref[...].astype(F32)
    turned = jnp.transpose(tmat[...])
    embt = turned[0:CH, :].astype(BF16)
    wout = turned[0:CH, 6:7]
    wtmp[0 : 5 * CH, :] = w1_ref[RB : RB + 5 * CH, :].astype(F32)
    wtmp[5 * CH : 6 * CH - RB, :] = jnp.zeros((CH - RB, LAT), F32)
    wtmp[6 * CH - RB : 6 * CH, :] = w1_ref[0:RB, :].astype(F32)
    wfull = wtmp[...]
    wpt[...] = wfull.astype(BF16)
    wp[...] = jnp.transpose(wfull).astype(BF16)
    w2t[...] = jnp.transpose(w2_ref[...].astype(F32)).astype(BF16)

    @pl.when(near == 1)
    def _():
        pl.semaphore_wait(go, 1)

        @pl.when(late_sib == 1)
        def _():
            sib_meta.start()
            sib_feat.start()

        for k in (3, 0, 1, 2):

            @pl.when(late_to[k] == 1)
            def _(k=k):
                for c in direct[k]:
                    c.start()

    meta[3].wait_recv()
    m_up.start()
    m_dn.start()
    f_out[0].wait_recv()
    r_up[0].start()
    r_dn[0].start()
    f_out[1].wait_recv()
    r_up[1].start()
    r_dn[1].start()
    for k, c in enumerate((f_g_up, f_g_dn)):
        meta[k].wait_recv()
        m_part[k].start()
        c.wait_recv()
        r_part[k].start()

    @pl.when(z == 0)
    def _():
        sib_meta.wait_recv()
        sib_feat.wait_recv()
        pl.semaphore_wait(ready, 1)
        meta_sib.start()
        f_p_sib.start()

    for c in (meta[2], *meta[8:], m_up, m_dn, *m_part):
        c.wait_recv()
    mi = dot(jnp.concatenate([mslot[8], mown[...], mslot[9]], 1), ohp[...])
    order = [mslot[0], mown[...], *(mslot[k] for k in range(1, 8))]
    mj = dot(jnp.concatenate(order, 1), ohc[...])
    off_i = jnp.where(left < ATOMS, -1.0, jnp.where(left < 2 * ATOMS, 0.0, 1.0))
    off_u = jnp.where(right < 3 * ATOMS, 0, jnp.where(right < 6 * ATOMS, 1, 2))
    rest = right - 3 * ATOMS * off_u
    off_v = jnp.where(rest < ATOMS, -1.0, jnp.where(rest < 2 * ATOMS, 0.0, 1.0))
    dx = (mj[0:1] + mj[3:4]) - (mi[0:1] + mi[3:4] + off_i)
    dy = (mj[1:2] + mj[4:5] + (off_u.astype(F32) - 1.0)) - (mi[1:2] + mi[4:5])
    dz = (mj[2:3] + mj[5:6] + off_v) - (mi[2:3] + mi[5:6])
    r2 = dx * dx + dy * dy + dz * dz + SOFTEN
    r = jnp.sqrt(r2)
    inv = 1.0 / r
    nx, ny, nz = dx * inv, dy * inv, dz * inv
    root3, root5, root15 = math.sqrt(3.0), math.sqrt(5.0), math.sqrt(15.0)
    harm = (
        root3 * nx, root3 * ny, root3 * nz, root15 * nx * ny, root15 * ny * nz,
        0.5 * root5 * (3.0 * nz * nz - 1.0), root15 * nx * nz, 0.5 * root15 * (nx * nx - ny * ny),
    )
    for m in range(8):
        yb[m] = jnp.broadcast_to(harm[m], (8, EDGES))
    orders = (lax.broadcasted_iota(jnp.int32, (RB, EDGES), 0) + 1).astype(F32)
    sin_b, cos_b = sin_cos_pi(orders * (1.0 / RADIUS) * r)
    radial = sin_b * inv
    slope = (orders * (math.pi / RADIUS) * cos_b - radial) * inv
    live = jnp.where(lax.broadcasted_iota(jnp.int32, (1, EDGES), 1) < count_ref[0, 0], 1.0, 0.0)
    gap = jnp.maximum(1.0 - r2 * (1.0 / (RADIUS * RADIUS)), 0.0)
    env = live * gap * gap
    kinds = lax.broadcasted_iota(jnp.int32, (LAT, EDGES), 0)
    for k, m in enumerate((mi, mj)):
        pick = jnp.where(kinds == m[6:7].astype(jnp.int32), 1.0, 0.0).astype(BF16)
        xbuf[CH * k : CH * (k + 1), :] = dot(embt, pick).astype(BF16)
    xbuf[5 * CH : 6 * CH - 16, :] = jnp.zeros((CH - 16, EDGES), BF16)
    xbuf[6 * CH - 16 : 6 * CH, :] = jnp.concatenate([jnp.zeros_like(radial), radial], 0).astype(BF16)

    def rows_of(ref, m, k):
        return ref[m * CH + 8 * k : m * CH + 8 * k + 8, :]

    def degree_sums(ref, out, other=None):
        for k2 in range(CH // 16):
            prods = [[], [], []]
            for k in (2 * k2, 2 * k2 + 1):
                one = [rows_of(ref, m, k) * yb[m - 1] for m in range(1, 9)]
                sums = (
                    rows_of(ref, 0, k),
                    one[0] + one[1] + one[2],
                    one[3] + one[4] + one[5] + one[6] + one[7],
                )
                for l in range(3):
                    at = slice(l * CH + 8 * k, l * CH + 8 * k + 8)
                    out[at, :] = sums[l]
                    if other is not None:
                        prods[l].append(sums[l] * other[at, :])
            if other is not None:
                for l in range(3):
                    start = (2 + l) * CH + 16 * k2
                    xbuf[start : start + 16, :] = jnp.concatenate(prods[l], 0).astype(BF16)

    def last_columns():
        for c in (*r_up, *r_dn):
            c.wait_recv()
        gj[...] = gj[...] + dot(jnp.concatenate([fslot[6], fslot[7]], 1), ohc[7 * ATOMS :, :])

    f_part.wait_recv()
    for c in r_part:
        c.wait_recv()
    order = [fslot[0], feat_ref[...], *(fslot[k] for k in range(1, 6))]
    gj[...] = dot(jnp.concatenate(order, 1), ohc[0 : 7 * ATOMS, :])

    @pl.when(z == 0)
    def _():
        f_p_dn.wait_recv()
        gi[...] = dot(jnp.concatenate([feat_ref[...], fslot[9]], 1), ohp[ATOMS:, :])
        last_columns()
        degree_sums(gj, sj)
        f_p_up.wait_recv()
        gi[...] = gi[...] + dot(fslot[8], ohp[0:ATOMS, :])
        degree_sums(gi, si, sj)

    @pl.when(z != 0)
    def _():
        f_p_dn.wait_recv()
        f_p_up.wait_recv()
        gi[...] = dot(jnp.concatenate([fslot[8], feat_ref[...], fslot[9]], 1), ohp[...])
        degree_sums(gi, si)
        last_columns()
        degree_sums(gj, sj, si)

    z1 = dot(wp[...], xbuf[...])
    sig1 = 1.0 / (1.0 + jnp.exp(-z1))
    z2 = dot(w2_ref[...], (z1 * sig1).astype(BF16))
    sig2 = 1.0 / (1.0 + jnp.exp(-z2))
    u = jnp.sum(wout * (z2 * sig2), 0, keepdims=True)
    energy_ref[...] = env * u

    dz2 = (wout * env) * (sig2 * (1.0 + z2 * (1.0 - sig2)))
    dh = dot(w2t[...], dz2.astype(BF16)).astype(BF16).astype(F32)
    dz1 = dh * (sig1 * (1.0 + z1 * (1.0 - sig1)))
    dxv = dot(wpt[...], dz1.astype(BF16)).astype(BF16).astype(F32)
    acc = [jnp.zeros((8, EDGES), F32) for _ in range(8)]
    for k in range(CH // 8):
        for l, ms in ((1, (1, 2, 3)), (2, (4, 5, 6, 7, 8))):
            at = slice(l * CH + 8 * k, l * CH + 8 * k + 8)
            dq = dxv[2 * CH + at.start : 2 * CH + at.stop, :]
            di, dj = dq * sj[at, :], dq * si[at, :]
            for m in ms:
                acc[m - 1] = acc[m - 1] + di * rows_of(gi, m, k) + dj * rows_of(gj, m, k)
    h1, h2, h3, h4, h5, h6, h7, h8 = (jnp.sum(a, 0, keepdims=True) for a in acc)
    ax = root3 * h1 + root15 * (ny * h4 + nz * h7 + nx * h8)
    ay = root3 * h2 + root15 * (nx * h4 + nz * h5 - ny * h8)
    az = root3 * h3 + root15 * (ny * h5 + nx * h7) + (3.0 * root5) * nz * h6
    dr = jnp.sum(dxv[6 * CH - RB : 6 * CH, :] * slope, 0, keepdims=True)
    dr = dr - (ax * nx + ay * ny + az * nz) * inv
    denv = live * u * (2.0 * gap) * (-1.0 / (RADIUS * RADIUS))
    scale = dr * inv + 2.0 * denv
    gbuf[...] = jnp.zeros_like(gbuf)
    gbuf[0:1, :] = ax * inv + dx * scale
    gbuf[1:2, :] = ay * inv + dy * scale
    gbuf[2:3, :] = az * inv + dz * scale

    grad = gbuf[...]
    g_hi = grad.astype(BF16).astype(F32)
    both = jnp.concatenate([g_hi, grad - g_hi], 0).astype(BF16)

    def lanes(a, k):
        return a[:, k * ATOMS : (k + 1) * ATOMS]

    back = [remote(pout.at[k], pslot.at[k], psend.at[k], precv.at[k], home[k]) for k in range(NSLOT)]
    part_p = dot(both, ohpt[...])
    part_p = part_p[0:8] + part_p[8:16]
    pout[8] = lanes(part_p, 0)
    pout[9] = lanes(part_p, 2)
    back[8].start()
    back[9].start()
    part_c = dot(both, ohct[...])
    part_c = -(part_c[0:8] + part_c[8:16])
    for slot, k in enumerate((0, 2, 3, 4, 5, 6, 7, 8)):
        pout[slot] = lanes(part_c, k)
        back[slot].start()
    force = lanes(part_p, 1) + lanes(part_c, 1)
    for c in (*meta, f_g_up, f_g_dn, f_part, *f_out, f_p_up, f_p_dn, *r_part, *r_up, *r_dn):
        c.wait_send()

    @pl.when(z == 0)
    def _():
        sib_meta.wait_send()
        sib_feat.wait_send()

    for k, c in enumerate(back):
        c.wait_recv()
        force = force + pslot[k]
    for k in range(3):
        force_ref[k] = force[k : k + 1, :]
    for c in back:
        c.wait_send()


def finish(force_ref, energy_ref, force_out, energy_out, sems):
    copies = fetch([(force_ref, force_out), (energy_ref, energy_out)], sems)
    for c in copies:
        c.wait()


def shards(positions, features, species, emb_table, edges, edge_count, w_first, w_second, w_out):
    vmem = pl.BlockSpec(memory_space=pltpu.VMEM)
    hbm = pl.BlockSpec(memory_space=pl.ANY)
    dma = pltpu.SemaphoreType.DMA
    pos = jnp.transpose(positions.reshape(1, 3, ATOMS), (1, 0, 2))
    feat = features.reshape(ROWS, ATOMS)
    spec = species.reshape(1, ATOMS)
    small = [pltpu.VMEM((3, 1, ATOMS), F32), pltpu.VMEM((1, ATOMS), jnp.int32)]
    forces, energy = pl.pallas_call(
        kernel,
        name="edge_forces",
        out_shape=(pltpu.VMEM((3, 1, ATOMS), F32), pltpu.VMEM((1, EDGES), F32)),
        in_specs=[hbm] * 9,
        out_specs=(vmem, vmem),
        scratch_shapes=[
            small[0],
            pltpu.VMEM((ROWS, ATOMS), BF16),
            small[1],
            pltpu.VMEM((2, EDGES), jnp.int32),
            pltpu.SMEM((1, 1), jnp.int32),
            pltpu.VMEM((6, CH), BF16),
            pltpu.VMEM((RB + 5 * CH, LAT), BF16),
            pltpu.VMEM((CH, LAT), BF16),
            pltpu.VMEM((1, CH), BF16),
            pltpu.VMEM((ROWS, ATOMS), BF16),
            pltpu.VMEM((16, ATOMS), BF16),
            pltpu.VMEM((NSLOT, ROWS, ATOMS), BF16),
            pltpu.VMEM((16, ATOMS), BF16),
            pltpu.VMEM((NSLOT, 16, ATOMS), BF16),
            pltpu.VMEM((3 * ATOMS, EDGES), BF16),
            pltpu.VMEM((9 * ATOMS, EDGES), BF16),
            pltpu.VMEM((EDGES, 3 * ATOMS), BF16),
            pltpu.VMEM((EDGES, 9 * ATOMS), BF16),
            pltpu.VMEM((ROWS, EDGES), F32),
            pltpu.VMEM((ROWS, EDGES), F32),
            pltpu.VMEM((3 * CH, EDGES), F32),
            pltpu.VMEM((3 * CH, EDGES), F32),
            pltpu.VMEM((8, 8, EDGES), F32),
            pltpu.VMEM((6 * CH, EDGES), BF16),
            pltpu.VMEM((6 * CH, LAT), F32),
            pltpu.VMEM((LAT, 6 * CH), BF16),
            pltpu.VMEM((6 * CH, LAT), BF16),
            pltpu.VMEM((LAT, CH), BF16),
            pltpu.VMEM((LAT, LAT), F32),
            pltpu.VMEM((8, EDGES), F32),
            pltpu.VMEM((16, ATOMS), F32),
            pltpu.VMEM((NSLOT, 8, ATOMS), F32),
            pltpu.VMEM((NSLOT, 8, ATOMS), F32),
            dma((9,)),
            pltpu.SemaphoreType.REGULAR,
            pltpu.SemaphoreType.REGULAR,
            dma((NSLOT,)),
            dma((NSLOT,)),
            dma((15,)),
            dma((15,)),
            dma((NSLOT,)),
            dma((NSLOT,)),
        ],
        compiler_params=pltpu.CompilerParams(collective_id=0, has_side_effects=True),
    )(
        pos,
        feat,
        spec,
        edges.reshape(2, EDGES),
        edge_count.reshape(1, 1),
        emb_table,
        w_first.T,
        w_second,
        w_out.reshape(1, CH),
    )
    forces, energy = pl.pallas_call(
        finish,
        name="finish",
        out_shape=(jax.ShapeDtypeStruct((3, 1, ATOMS), F32), jax.ShapeDtypeStruct((1, EDGES), F32)),
        in_specs=[vmem, vmem],
        out_specs=(hbm, hbm),
        scratch_shapes=[dma((2,))],
    )(
        pltpu.with_memory_space_constraint(forces, pltpu.VMEM),
        pltpu.with_memory_space_constraint(energy, pltpu.VMEM),
    )
    return (
        jnp.transpose(forces, (1, 0, 2)).reshape(1, 1, 1, 3, ATOMS),
        energy.reshape(1, 1, 1, EDGES),
    )


def solution(mesh):
    placed = (
        P("plate", "tower", "gz", None, None),
        P("plate", "tower", "gz", None, None),
        P("plate", "tower", "gz", None),
        P(),
        P("plate", "tower", "gz", None, None),
        P("plate", "tower", "gz"),
        P(),
        P(),
        P(),
    )
    return jax.shard_map(
        shards,
        mesh=mesh,
        in_specs=placed,
        out_specs=(P("plate", "tower", "gz", None, None), P("plate", "tower", "gz", None)),
        check_vma=False,
    )
```

```python
import math

import jax
import jax.numpy as jnp
from jax import lax
from jax.experimental import pallas as pl
from jax.experimental.pallas import tpu as pltpu
from jax.sharding import PartitionSpec as P

ATOMS = 128
EDGES = 512
CH = 64
LAT = 128
RB = 8
ROWS = 9 * CH
PART = ROWS // 4
RADIUS = 3.0
SOFTEN = 0.04
F32 = jnp.float32
BF16 = jnp.bfloat16

NSLOT = 10


def dot(a, b):
    return lax.dot_general(a, b, (((1,), (0,)), ((), ())), preferred_element_type=F32)


def sin_cos_pi(t):
    turns = jnp.floor(t + 0.5)
    x = (t - turns) * math.pi
    parity = turns - 2.0 * jnp.floor(turns * 0.5)
    sign = 1.0 - 2.0 * parity
    y = x * x
    s = -1.0 / 39916800.0
    for c in (1.0 / 362880.0, -1.0 / 5040.0, 1.0 / 120.0, -1.0 / 6.0, 1.0):
        s = s * y + c
    c_ = 1.0 / 479001600.0
    for c in (-1.0 / 3628800.0, 1.0 / 40320.0, -1.0 / 720.0, 1.0 / 24.0, -0.5, 1.0):
        c_ = c_ * y + c
    return sign * s * x, sign * c_


def remote(src, dst, ssem, rsem, to):
    return pltpu.make_async_remote_copy(
        src_ref=src,
        dst_ref=dst,
        send_sem=ssem,
        recv_sem=rsem,
        device_id=to,
        device_id_type=pl.DeviceIdType.MESH,
    )


def fetch(pairs, sems):
    copies = [pltpu.make_async_copy(src, dst, sems.at[n]) for n, (src, dst) in enumerate(pairs)]
    for c in copies:
        c.start()
    return copies


def pack_small(pos, spec, stage, out):
    stage[...] = jnp.zeros_like(stage)
    for k in range(3):
        hi = pos[k].astype(BF16).astype(F32)
        stage[k : k + 1, :] = hi
        stage[k + 3 : k + 4, :] = (pos[k] - hi).astype(BF16).astype(F32)
    stage[6:7, :] = spec[...].astype(F32)
    out[...] = stage[...].astype(BF16)


DEPTH = 16


def kernel(
    pos_any,
    feat_any,
    spec_any,
    edges_any,
    count_ref,
    table_any,
    w1_any,
    w2_any,
    wout_any,
    force_ref,
    energy_ref,
    pos,
    feat_ref,
    spec_ref,
    edges_ref,
    table_ref,
    w1_ref,
    w2_ref,
    wout_ref,
    sib_f,
    sib_m,
    fslot,
    mown,
    mslot,
    ohp,
    ohc,
    ohpt,
    ohct,
    gi,
    gj,
    si,
    sj,
    yb,
    xbuf,
    wtmp,
    wp,
    wpt,
    w2t,
    tmat,
    gbuf,
    stage,
    pout,
    pslot,
    lsem,
    ready,
    go,
    msend,
    mrecv,
    fsend,
    frecv,
    ssend,
    srecv,
    psend,
    precv,
):
    n_plate, n_tower, n_gz = (lax.axis_size(a) for a in ("plate", "tower", "gz"))
    p, t, g = (lax.axis_index(a) for a in ("plate", "tower", "gz"))
    odd = lax.rem(t, 2)
    partner = t + 1 - 2 * odd
    outward = lax.rem(t + 2 * odd - 1 + n_tower, n_tower)
    g_up, g_dn = lax.rem(g + 1, n_gz), lax.rem(g + n_gz - 1, n_gz)
    p_up, p_dn = lax.rem(p + 1, n_plate), lax.rem(p + n_plate - 1, n_plate)
    z = lax.rem(p, DEPTH)
    last = z // (DEPTH - 1)
    first = lax.rem(z + DEPTH - 1, DEPTH) // (DEPTH - 1)

    total = n_plate * n_tower * n_gz

    def dev(pp, tt, gg):
        return {"plate": pp, "tower": tt, "gz": gg}

    def is_late(d):
        return 1 - ((d["plate"] * n_tower + d["tower"]) * n_gz + d["gz"] + total - 1) // total


    dest = [
        dev(p, t, g_up), dev(p, t, g_dn), dev(p, partner, g), dev(p, outward, g),
        dev(p, partner, g_up), dev(p, partner, g_dn), dev(p, outward, g_up), dev(p, outward, g_dn),
        dev(p_up, t, g), dev(p_dn, t, g),
    ]
    home = [dest[k] for k in (1, 0, 2, 3, 5, 4, 7, 6, 9, 8)]
    sibling = dev(lax.rem(p + DEPTH, n_plate), t, g)
    below = dev(lax.rem(p + n_plate - 1 + DEPTH * first, n_plate), t, g)
    above = dev(lax.rem(p + 1 + DEPTH, n_plate), t, g)

    loads = fetch(
        [
            (feat_any, feat_ref), (pos_any, pos), (spec_any, spec_ref), (edges_any, edges_ref),
            (table_any, table_ref), (w1_any, w1_ref), (w2_any, w2_ref), (wout_any, wout_ref),
        ],
        lsem,
    )
    barrier = pltpu.get_barrier_semaphore()

    def greet(d):
        pl.semaphore_signal(barrier, inc=1, device_id=d, device_id_type=pl.DeviceIdType.MESH)

    late = is_late(dev(p, t, g))
    late_to = [is_late(d) for d in dest[:4]]
    late_sib = first * is_late(sibling)
    near = late_to[0] + late_to[1] + late_to[2] + late_to[3] + late_sib

    via_lo = last * (1 - p // DEPTH)

    greet(below)

    @pl.when(late == 0)
    def _():
        for d in dest[:4]:
            greet(d)

    @pl.when(z == 0)
    def _():
        greet(dest[9])

    @pl.when(first - late == 1)
    def _():
        greet(sibling)

    @pl.when(last == 0)
    def _():
        greet(dest[8])

    for c in loads[1:3]:
        c.wait()
    pack_small(pos, spec_ref, stage, mown)

    def small_rows(src, k, to):
        n = {0: 0, 1: 1, 3: 2}.get(k, 3)
        return remote(src, mslot.at[k], msend, mrecv.at[n], to)

    meta = [small_rows(mown, k, dest[k]) for k in range(4)]
    m_part = [small_rows(mslot.at[k], 4 + k, dest[2]) for k in range(2)]
    m_up, m_dn = small_rows(mslot.at[3], 6, dest[0]), small_rows(mslot.at[3], 7, dest[1])
    meta += [small_rows(mown, 8, dest[8]), small_rows(mown, 9, below)]
    meta_sib = small_rows(sib_m, 9, below)
    def of_size(ref, ssem, rsem):
        return remote(ref, ref, ssem, rsem, dest[0])

    parts = [pl.ds(PART * k, PART) for k in range(ROWS // PART)]

    def feature(n, src, slot, to, part=None):
        dst = fslot.at[slot]
        if part is not None:
            src, dst = src.at[part], dst.at[part]
        return remote(src, dst, fsend, frecv.at[n], to)

    f_g_up = feature(0, feat_ref, 0, dest[0])
    f_g_dn = feature(1, feat_ref, 1, dest[1])
    f_part = feature(2, feat_ref, 2, dest[2])
    r_part = [feature(2, fslot.at[0], 4, dest[2]), feature(2, fslot.at[1], 5, dest[2])]
    r_up = [feature(3, fslot.at[3], 6, dest[0], c) for c in parts]
    r_dn = [feature(3, fslot.at[3], 7, dest[1], c) for c in parts]
    f_p_up = [feature(4, feat_ref, 8, dest[8], pl.ds(ROWS // 2 * k, ROWS // 2)) for k in range(2)]
    up_all = of_size(fslot.at[8], fsend, frecv.at[4])
    f_p_dn = feature(5, feat_ref, 9, below)
    f_p_sib = feature(5, sib_f, 9, below)
    f_out = [feature(6 + k, feat_ref, 3, dest[3], c) for k, c in enumerate(parts)]
    sib_feat = remote(feat_ref, sib_f, ssend.at[0], srecv.at[0], sibling)
    sib_meta = remote(mown, sib_m, ssend.at[1], srecv.at[1], sibling)

    meta_sent, feat_sent = of_size(mslot, msend, msend), of_size(fslot, fsend, fsend)
    meta_rest = of_size(mslot.at[pl.ds(3, 7)], msend, mrecv.at[3])
    near_come = of_size(fslot.at[pl.ds(4, 3)], fsend, frecv.at[2])
    far_come = of_size(fslot.at[pl.ds(6, 2)], fsend, frecv.at[3])
    back_all = of_size(pslot, psend, precv)

    loads[0].wait()
    pl.semaphore_wait(barrier, 6 + last - near)

    def tell(sem, d):
        pl.semaphore_signal(sem, inc=1, device_id=d, device_id_type=pl.DeviceIdType.MESH)

    @pl.when(last == 1)
    def _():
        tell(ready, above)

    @pl.when(late == 1)
    def _():
        for d in (*dest[:4], sibling):
            tell(go, d)

    @pl.when(first - late_sib == 1)
    def _():
        sib_meta.start()
        sib_feat.start()

    direct = ((meta[0], f_g_up), (meta[1], f_g_dn), (meta[2], f_part), (meta[3], *f_out))
    meta[4].start()
    f_p_up[0].start()

    @pl.when(via_lo == 0)
    def _():
        f_p_up[1].start()

    @pl.when(z != 0)
    def _():
        meta[5].start()
        f_p_dn.start()

    for k in (3, 0, 1, 2):

        @pl.when(late_to[k] == 0)
        def _(k=k):
            for c in direct[k]:
                c.start()

    for c in loads[3:]:
        c.wait()

    left, right = edges_ref[0:1, :], edges_ref[1:2, :]
    row = lax.broadcasted_iota(jnp.int32, (ATOMS, EDGES), 0)
    lane = lax.broadcasted_iota(jnp.int32, (EDGES, ATOMS), 1)

    def column_of(index):
        turned = jnp.transpose(jnp.broadcast_to(index.astype(F32), (8, EDGES)))
        return jnp.broadcast_to(turned[:, 0:1].astype(jnp.int32), (EDGES, ATOMS))

    left_col, right_col = column_of(left), column_of(right)

    def one_hot(match):
        return jnp.where(match, 1.0, 0.0).astype(BF16)

    for k in range(3):
        base = ATOMS * k
        ohp[base : base + ATOMS, :] = one_hot(row == left - base)
        ohpt[:, base : base + ATOMS] = one_hot(lane == left_col - base)
    u_part, u_out = 2 - 2 * odd, 2 * odd
    places = ((1, 0), (1, 1), (1, 2), (u_part, 1), (u_out, 1), (u_part, 0), (u_part, 2), (u_out, 0), (u_out, 2))
    for k, (u, v) in enumerate(places):
        base = (3 * u + v) * ATOMS
        ohc[ATOMS * k : ATOMS * (k + 1), :] = one_hot(row == right - base)
        ohct[:, ATOMS * k : ATOMS * (k + 1)] = one_hot(lane == right_col - base)

    tmat[...] = jnp.zeros_like(tmat)
    tmat[0:6, 0:CH] = table_ref[...].astype(F32)
    tmat[6:7, 0:CH] = wout_ref[...].astype(F32)
    turned = jnp.transpose(tmat[...])
    embt = turned[0:CH, :].astype(BF16)
    wout = turned[0:CH, 6:7]
    wtmp[0 : 5 * CH, :] = w1_ref[RB : RB + 5 * CH, :].astype(F32)
    wtmp[5 * CH : 6 * CH - RB, :] = jnp.zeros((CH - RB, LAT), F32)
    wtmp[6 * CH - RB : 6 * CH, :] = w1_ref[0:RB, :].astype(F32)
    wfull = wtmp[...]
    wpt[...] = wfull.astype(BF16)
    wp[...] = jnp.transpose(wfull).astype(BF16)
    w2t[...] = jnp.transpose(w2_ref[...].astype(F32)).astype(BF16)

    @pl.when(near == 1)
    def _():
        pl.semaphore_wait(go, 1)

        @pl.when(late_sib == 1)
        def _():
            sib_meta.start()
            sib_feat.start()

        for k in (3, 0, 1, 2):

            @pl.when(late_to[k] == 1)
            def _(k=k):
                for c in direct[k]:
                    c.start()

    meta[3].wait_recv()
    m_up.start()
    m_dn.start()
    for k, c in enumerate(f_out):
        c.wait_recv()
        r_up[k].start()
        r_dn[k].start()
    @pl.when(via_lo == 1)
    def _():
        f_p_up[1].start()

    for k, c in enumerate((f_g_up, f_g_dn)):
        meta[k].wait_recv()
        m_part[k].start()
        c.wait_recv()
        r_part[k].start()

    @pl.when(z == 0)
    def _():
        sib_meta.wait_recv()
        sib_feat.wait_recv()
        pl.semaphore_wait(ready, 1)
        meta_sib.start()
        f_p_sib.start()

    meta_rest.wait_recv()
    mi = dot(jnp.concatenate([mslot[8], mown[...], mslot[9]], 1), ohp[...])
    order = [mslot[0], mown[...], *(mslot[k] for k in range(1, 8))]
    mj = dot(jnp.concatenate(order, 1), ohc[...])
    off_i = jnp.where(left < ATOMS, -1.0, jnp.where(left < 2 * ATOMS, 0.0, 1.0))
    off_u = jnp.where(right < 3 * ATOMS, 0, jnp.where(right < 6 * ATOMS, 1, 2))
    rest = right - 3 * ATOMS * off_u
    off_v = jnp.where(rest < ATOMS, -1.0, jnp.where(rest < 2 * ATOMS, 0.0, 1.0))
    dx = (mj[0:1] + mj[3:4]) - (mi[0:1] + mi[3:4] + off_i)
    dy = (mj[1:2] + mj[4:5] + (off_u.astype(F32) - 1.0)) - (mi[1:2] + mi[4:5])
    dz = (mj[2:3] + mj[5:6] + off_v) - (mi[2:3] + mi[5:6])
    r2 = dx * dx + dy * dy + dz * dz + SOFTEN
    r = jnp.sqrt(r2)
    inv = 1.0 / r
    nx, ny, nz = dx * inv, dy * inv, dz * inv
    root3, root5, root15 = math.sqrt(3.0), math.sqrt(5.0), math.sqrt(15.0)
    harm = (
        root3 * nx, root3 * ny, root3 * nz, root15 * nx * ny, root15 * ny * nz,
        0.5 * root5 * (3.0 * nz * nz - 1.0), root15 * nx * nz, 0.5 * root15 * (nx * nx - ny * ny),
    )
    for m in range(8):
        yb[m] = jnp.broadcast_to(harm[m], (8, EDGES))
    orders = (lax.broadcasted_iota(jnp.int32, (RB, EDGES), 0) + 1).astype(F32)
    sin_b, cos_b = sin_cos_pi(orders * (1.0 / RADIUS) * r)
    radial = sin_b * inv
    slope = (orders * (math.pi / RADIUS) * cos_b - radial) * inv
    live = jnp.where(lax.broadcasted_iota(jnp.int32, (1, EDGES), 1) < count_ref[0, 0], 1.0, 0.0)
    gap = jnp.maximum(1.0 - r2 * (1.0 / (RADIUS * RADIUS)), 0.0)
    env = live * gap * gap
    kinds = lax.broadcasted_iota(jnp.int32, (LAT, EDGES), 0)
    for k, m in enumerate((mi, mj)):
        pick = jnp.where(kinds == m[6:7].astype(jnp.int32), 1.0, 0.0).astype(BF16)
        xbuf[CH * k : CH * (k + 1), :] = dot(embt, pick).astype(BF16)
    xbuf[5 * CH : 6 * CH - 16, :] = jnp.zeros((CH - 16, EDGES), BF16)
    xbuf[6 * CH - 16 : 6 * CH, :] = jnp.concatenate([jnp.zeros_like(radial), radial], 0).astype(BF16)

    def rows_of(ref, m, k):
        return ref[m * CH + 8 * k : m * CH + 8 * k + 8, :]

    def degree_sums(ref, out, other=None):
        for k2 in range(CH // 16):
            prods = [[], [], []]
            for k in (2 * k2, 2 * k2 + 1):
                one = [rows_of(ref, m, k) * yb[m - 1] for m in range(1, 9)]
                sums = (
                    rows_of(ref, 0, k),
                    one[0] + one[1] + one[2],
                    one[3] + one[4] + one[5] + one[6] + one[7],
                )
                for l in range(3):
                    at = slice(l * CH + 8 * k, l * CH + 8 * k + 8)
                    out[at, :] = sums[l]
                    if other is not None:
                        prods[l].append(sums[l] * other[at, :])
            if other is not None:
                for l in range(3):
                    start = (2 + l) * CH + 16 * k2
                    xbuf[start : start + 16, :] = jnp.concatenate(prods[l], 0).astype(BF16)

    def last_columns():
        far_come.wait_recv()
        gj[...] = gj[...] + dot(jnp.concatenate([fslot[6], fslot[7]], 1), ohc[7 * ATOMS :, :])

    near_come.wait_recv()
    order = [fslot[0], feat_ref[...], *(fslot[k] for k in range(1, 6))]
    gj[...] = dot(jnp.concatenate(order, 1), ohc[0 : 7 * ATOMS, :])

    @pl.when(z == 0)
    def _():
        f_p_dn.wait_recv()
        gi[...] = dot(jnp.concatenate([feat_ref[...], fslot[9]], 1), ohp[ATOMS:, :])
        last_columns()
        degree_sums(gj, sj)
        up_all.wait_recv()
        gi[...] = gi[...] + dot(fslot[8], ohp[0:ATOMS, :])
        degree_sums(gi, si, sj)

    @pl.when(z != 0)
    def _():
        f_p_dn.wait_recv()
        up_all.wait_recv()
        gi[...] = dot(jnp.concatenate([fslot[8], feat_ref[...], fslot[9]], 1), ohp[...])
        degree_sums(gi, si)
        last_columns()
        degree_sums(gj, sj, si)

    z1 = dot(wp[...], xbuf[...])
    sig1 = 1.0 / (1.0 + jnp.exp(-z1))
    z2 = dot(w2_ref[...], (z1 * sig1).astype(BF16))
    sig2 = 1.0 / (1.0 + jnp.exp(-z2))
    u = jnp.sum(wout * (z2 * sig2), 0, keepdims=True)
    energy_ref[...] = env * u

    dz2 = (wout * env) * (sig2 * (1.0 + z2 * (1.0 - sig2)))
    dh = dot(w2t[...], dz2.astype(BF16)).astype(BF16).astype(F32)
    dz1 = dh * (sig1 * (1.0 + z1 * (1.0 - sig1)))
    dxv = dot(wpt[...], dz1.astype(BF16)).astype(BF16).astype(F32)
    acc = [jnp.zeros((8, EDGES), F32) for _ in range(8)]
    for k in range(CH // 8):
        for l, ms in ((1, (1, 2, 3)), (2, (4, 5, 6, 7, 8))):
            at = slice(l * CH + 8 * k, l * CH + 8 * k + 8)
            dq = dxv[2 * CH + at.start : 2 * CH + at.stop, :]
            di, dj = dq * sj[at, :], dq * si[at, :]
            for m in ms:
                acc[m - 1] = acc[m - 1] + di * rows_of(gi, m, k) + dj * rows_of(gj, m, k)
    h1, h2, h3, h4, h5, h6, h7, h8 = (jnp.sum(a, 0, keepdims=True) for a in acc)
    ax = root3 * h1 + root15 * (ny * h4 + nz * h7 + nx * h8)
    ay = root3 * h2 + root15 * (nx * h4 + nz * h5 - ny * h8)
    az = root3 * h3 + root15 * (ny * h5 + nx * h7) + (3.0 * root5) * nz * h6
    dr = jnp.sum(dxv[6 * CH - RB : 6 * CH, :] * slope, 0, keepdims=True)
    dr = dr - (ax * nx + ay * ny + az * nz) * inv
    denv = live * u * (2.0 * gap) * (-1.0 / (RADIUS * RADIUS))
    scale = dr * inv + 2.0 * denv
    gbuf[...] = jnp.zeros_like(gbuf)
    gbuf[0:1, :] = ax * inv + dx * scale
    gbuf[1:2, :] = ay * inv + dy * scale
    gbuf[2:3, :] = az * inv + dz * scale

    grad = gbuf[...]
    g_hi = grad.astype(BF16).astype(F32)
    both = jnp.concatenate([g_hi, grad - g_hi], 0).astype(BF16)

    def lanes(a, k):
        return a[:, k * ATOMS : (k + 1) * ATOMS]

    back = [remote(pout.at[k], pslot.at[k], psend, precv, home[k]) for k in range(NSLOT)]
    part_p = dot(both, ohpt[...])
    part_p = part_p[0:8] + part_p[8:16]
    pout[8] = lanes(part_p, 0)
    pout[9] = lanes(part_p, 2)
    back[8].start()
    back[9].start()
    part_c = dot(both, ohct[...])
    part_c = -(part_c[0:8] + part_c[8:16])
    for slot, k in enumerate((0, 2, 3, 4, 5, 6, 7, 8)):
        pout[slot] = lanes(part_c, k)
        back[slot].start()
    force = lanes(part_p, 1) + lanes(part_c, 1)
    meta_sent.wait_send()
    feat_sent.wait_send()

    @pl.when(first == 1)
    def _():
        sib_meta.wait_send()
        sib_feat.wait_send()

    back_all.wait_recv()
    for k in range(NSLOT):
        force = force + pslot[k]
    for k in range(3):
        force_ref[k] = force[k : k + 1, :]
    back_all.wait_send()


def finish(force_ref, energy_ref, force_out, energy_out, sems):
    copies = fetch([(force_ref, force_out), (energy_ref, energy_out)], sems)
    for c in copies:
        c.wait()


def shards(positions, features, species, emb_table, edges, edge_count, w_first, w_second, w_out):
    vmem = pl.BlockSpec(memory_space=pltpu.VMEM)
    hbm = pl.BlockSpec(memory_space=pl.ANY)
    dma = pltpu.SemaphoreType.DMA
    pos = jnp.transpose(positions.reshape(1, 3, ATOMS), (1, 0, 2))
    feat = features.reshape(ROWS, ATOMS)
    spec = species.reshape(1, ATOMS)
    small = [pltpu.VMEM((3, 1, ATOMS), F32), pltpu.VMEM((1, ATOMS), jnp.int32)]
    forces, energy = pl.pallas_call(
        kernel,
        name="edge_forces",
        out_shape=(pltpu.VMEM((3, 1, ATOMS), F32), pltpu.VMEM((1, EDGES), F32)),
        in_specs=[*[hbm] * 4, pl.BlockSpec(memory_space=pltpu.SMEM), *[hbm] * 4],
        out_specs=(vmem, vmem),
        scratch_shapes=[
            small[0],
            pltpu.VMEM((ROWS, ATOMS), BF16),
            small[1],
            pltpu.VMEM((2, EDGES), jnp.int32),
            pltpu.VMEM((6, CH), BF16),
            pltpu.VMEM((RB + 5 * CH, LAT), BF16),
            pltpu.VMEM((CH, LAT), BF16),
            pltpu.VMEM((1, CH), BF16),
            pltpu.VMEM((ROWS, ATOMS), BF16),
            pltpu.VMEM((16, ATOMS), BF16),
            pltpu.VMEM((NSLOT, ROWS, ATOMS), BF16),
            pltpu.VMEM((16, ATOMS), BF16),
            pltpu.VMEM((NSLOT, 16, ATOMS), BF16),
            pltpu.VMEM((3 * ATOMS, EDGES), BF16),
            pltpu.VMEM((9 * ATOMS, EDGES), BF16),
            pltpu.VMEM((EDGES, 3 * ATOMS), BF16),
            pltpu.VMEM((EDGES, 9 * ATOMS), BF16),
            pltpu.VMEM((ROWS, EDGES), F32),
            pltpu.VMEM((ROWS, EDGES), F32),
            pltpu.VMEM((3 * CH, EDGES), F32),
            pltpu.VMEM((3 * CH, EDGES), F32),
            pltpu.VMEM((8, 8, EDGES), F32),
            pltpu.VMEM((6 * CH, EDGES), BF16),
            pltpu.VMEM((6 * CH, LAT), F32),
            pltpu.VMEM((LAT, 6 * CH), BF16),
            pltpu.VMEM((6 * CH, LAT), BF16),
            pltpu.VMEM((LAT, CH), BF16),
            pltpu.VMEM((LAT, LAT), F32),
            pltpu.VMEM((8, EDGES), F32),
            pltpu.VMEM((16, ATOMS), F32),
            pltpu.VMEM((NSLOT, 8, ATOMS), F32),
            pltpu.VMEM((NSLOT, 8, ATOMS), F32),
            dma((8,)),
            pltpu.SemaphoreType.REGULAR,
            pltpu.SemaphoreType.REGULAR,
            dma,
            dma((4,)),
            dma,
            dma((6 + ROWS // PART,)),
            dma((2,)),
            dma((2,)),
            dma,
            dma,
        ],
        compiler_params=pltpu.CompilerParams(collective_id=0, has_side_effects=True),
    )(
        pos,
        feat,
        spec,
        edges.reshape(2, EDGES),
        edge_count.reshape(1, 1),
        emb_table,
        w_first.T,
        w_second,
        w_out.reshape(1, CH),
    )
    forces, energy = pl.pallas_call(
        finish,
        name="finish",
        out_shape=(jax.ShapeDtypeStruct((3, 1, ATOMS), F32), jax.ShapeDtypeStruct((1, EDGES), F32)),
        in_specs=[vmem, vmem],
        out_specs=(hbm, hbm),
        scratch_shapes=[dma((2,))],
    )(
        pltpu.with_memory_space_constraint(forces, pltpu.VMEM),
        pltpu.with_memory_space_constraint(energy, pltpu.VMEM),
    )
    return (
        jnp.transpose(forces, (1, 0, 2)).reshape(1, 1, 1, 3, ATOMS),
        energy.reshape(1, 1, 1, EDGES),
    )


def solution(mesh):
    placed = (
        P("plate", "tower", "gz", None, None),
        P("plate", "tower", "gz", None, None),
        P("plate", "tower", "gz", None),
        P(),
        P("plate", "tower", "gz", None, None),
        P("plate", "tower", "gz"),
        P(),
        P(),
        P(),
    )
    return jax.shard_map(
        shards,
        mesh=mesh,
        in_specs=placed,
        out_specs=(P("plate", "tower", "gz", None, None), P("plate", "tower", "gz", None)),
        check_vma=False,
    )
```

```python
import math

import jax
import jax.numpy as jnp
from jax import lax
from jax.experimental import pallas as pl
from jax.experimental.pallas import tpu as pltpu
from jax.sharding import PartitionSpec as P

ATOMS = 128
EDGES = 512
CH = 64
LAT = 128
RB = 8
ROWS = 9 * CH
PART = ROWS // 4
RADIUS = 3.0
SOFTEN = 0.04
F32 = jnp.float32
BF16 = jnp.bfloat16

NSLOT = 10


def dot(a, b):
    return lax.dot_general(a, b, (((1,), (0,)), ((), ())), preferred_element_type=F32)


def sin_cos_pi(t):
    turns = jnp.floor(t + 0.5)
    x = (t - turns) * math.pi
    parity = turns - 2.0 * jnp.floor(turns * 0.5)
    sign = 1.0 - 2.0 * parity
    y = x * x
    s = -1.0 / 39916800.0
    for c in (1.0 / 362880.0, -1.0 / 5040.0, 1.0 / 120.0, -1.0 / 6.0, 1.0):
        s = s * y + c
    c_ = 1.0 / 479001600.0
    for c in (-1.0 / 3628800.0, 1.0 / 40320.0, -1.0 / 720.0, 1.0 / 24.0, -0.5, 1.0):
        c_ = c_ * y + c
    return sign * s * x, sign * c_


def remote(src, dst, ssem, rsem, to):
    return pltpu.make_async_remote_copy(
        src_ref=src,
        dst_ref=dst,
        send_sem=ssem,
        recv_sem=rsem,
        device_id=to,
        device_id_type=pl.DeviceIdType.MESH,
    )


def fetch(pairs, sems, base=0):
    copies = [pltpu.make_async_copy(src, dst, sems.at[base + n]) for n, (src, dst) in enumerate(pairs)]
    for c in copies:
        c.start()
    return copies


def pack_small(pos, spec, stage, out):
    stage[...] = jnp.zeros_like(stage)
    for k in range(3):
        hi = pos[k].astype(BF16).astype(F32)
        stage[k : k + 1, :] = hi
        stage[k + 3 : k + 4, :] = (pos[k] - hi).astype(BF16).astype(F32)
    stage[6:7, :] = spec[...].astype(F32)
    out[...] = stage[...].astype(BF16)


DEPTH = 16


def kernel(
    pos_any,
    feat_any,
    spec_any,
    edges_any,
    count_any,
    table_any,
    w1_any,
    w2_any,
    wout_any,
    force_ref,
    energy_ref,
    pos,
    feat_ref,
    spec_ref,
    edges_ref,
    count_ref,
    table_ref,
    w1_ref,
    w2_ref,
    wout_ref,
    sib_f,
    sib_m,
    fslot,
    mown,
    mslot,
    ohp,
    ohc,
    ohpt,
    ohct,
    gi,
    gj,
    si,
    sj,
    yb,
    xbuf,
    wtmp,
    wp,
    wpt,
    w2t,
    tmat,
    gbuf,
    stage,
    pout,
    pslot,
    lsem,
    ready,
    go,
    msend,
    mrecv,
    fsend,
    frecv,
    ssend,
    srecv,
    psend,
    precv,
):
    n_plate, n_tower, n_gz = (lax.axis_size(a) for a in ("plate", "tower", "gz"))
    p, t, g = (lax.axis_index(a) for a in ("plate", "tower", "gz"))
    odd = lax.rem(t, 2)
    partner = t + 1 - 2 * odd
    outward = lax.rem(t + 2 * odd - 1 + n_tower, n_tower)
    g_up, g_dn = lax.rem(g + 1, n_gz), lax.rem(g + n_gz - 1, n_gz)
    p_up, p_dn = lax.rem(p + 1, n_plate), lax.rem(p + n_plate - 1, n_plate)
    z = lax.rem(p, DEPTH)
    last = z // (DEPTH - 1)
    first = lax.rem(z + DEPTH - 1, DEPTH) // (DEPTH - 1)

    total = n_plate * n_tower * n_gz

    def dev(pp, tt, gg):
        return {"plate": pp, "tower": tt, "gz": gg}

    def is_late(d):
        return 1 - ((d["plate"] * n_tower + d["tower"]) * n_gz + d["gz"] + total - 1) // total


    dest = [
        dev(p, t, g_up), dev(p, t, g_dn), dev(p, partner, g), dev(p, outward, g),
        dev(p, partner, g_up), dev(p, partner, g_dn), dev(p, outward, g_up), dev(p, outward, g_dn),
        dev(p_up, t, g), dev(p_dn, t, g),
    ]
    home = [dest[k] for k in (1, 0, 2, 3, 5, 4, 7, 6, 9, 8)]
    sibling = dev(lax.rem(p + DEPTH, n_plate), t, g)
    below = dev(lax.rem(p + n_plate - 1 + DEPTH * first, n_plate), t, g)
    above = dev(lax.rem(p + 1 + DEPTH, n_plate), t, g)

    loads = fetch([(feat_any, feat_ref)], lsem)
    barrier = pltpu.get_barrier_semaphore()

    def greet(d):
        pl.semaphore_signal(barrier, inc=1, device_id=d, device_id_type=pl.DeviceIdType.MESH)

    late = is_late(dev(p, t, g))
    late_to = [is_late(d) for d in dest[:4]]
    late_sib = first * is_late(sibling)
    near = late_to[0] + late_to[1] + late_to[2] + late_to[3] + late_sib

    via_lo = last * (1 - p // DEPTH)

    greet(below)

    @pl.when(late == 0)
    def _():
        for d in dest[:4]:
            greet(d)

    @pl.when(z == 0)
    def _():
        greet(dest[9])

    @pl.when(first - late == 1)
    def _():
        greet(sibling)

    @pl.when(last == 0)
    def _():
        greet(dest[8])

    loads += fetch(
        [
            (pos_any, pos), (spec_any, spec_ref), (edges_any, edges_ref), (count_any, count_ref),
            (table_any, table_ref), (w1_any, w1_ref), (w2_any, w2_ref), (wout_any, wout_ref),
        ],
        lsem,
        1,
    )
    for c in loads[1:3]:
        c.wait()
    pack_small(pos, spec_ref, stage, mown)

    def small_rows(src, k, to):
        n = {0: 0, 1: 1, 3: 2}.get(k, 3)
        return remote(src, mslot.at[k], msend, mrecv.at[n], to)

    meta = [small_rows(mown, k, dest[k]) for k in range(4)]
    m_part = [small_rows(mslot.at[k], 4 + k, dest[2]) for k in range(2)]
    m_up, m_dn = small_rows(mslot.at[3], 6, dest[0]), small_rows(mslot.at[3], 7, dest[1])
    meta += [small_rows(mown, 8, dest[8]), small_rows(mown, 9, below)]
    meta_sib = small_rows(sib_m, 9, below)
    def of_size(ref, ssem, rsem):
        return remote(ref, ref, ssem, rsem, dest[0])

    parts = [pl.ds(PART * k, PART) for k in range(ROWS // PART)]

    def feature(n, src, slot, to, part=None):
        dst = fslot.at[slot]
        if part is not None:
            src, dst = src.at[part], dst.at[part]
        return remote(src, dst, fsend, frecv.at[n], to)

    head = pl.ds(0, ROWS - PART)
    n_parts = len(parts)
    f_g = [feature(k, feat_ref, k, dest[k], head) for k in range(2)]
    f_g_last = [feature(6 + n_parts + k, feat_ref, k, dest[k], parts[-1]) for k in range(2)]
    r_out = [feature(3, fslot.at[k], 6 + k, dest[3], parts[-1]) for k in range(2)]
    f_part = feature(2, feat_ref, 2, dest[2])
    r_part = [feature(3, fslot.at[0], 4, dest[2]), feature(3, fslot.at[1], 5, dest[2])]
    r_up = [feature(3, fslot.at[3], 6, dest[0], c) for c in parts]
    r_dn = [feature(3, fslot.at[3], 7, dest[1], c) for c in parts]
    f_p_up = [feature(4, feat_ref, 8, dest[8], pl.ds(ROWS // 2 * k, ROWS // 2)) for k in range(2)]
    up_all = of_size(fslot.at[8], fsend, frecv.at[4])
    f_p_dn = feature(5, feat_ref, 9, below)
    f_p_sib = feature(5, sib_f, 9, below)
    f_out = [feature(6 + k, feat_ref, 3, dest[3], c) for k, c in enumerate(parts)]
    sib_feat = remote(feat_ref, sib_f, ssend.at[0], srecv.at[0], sibling)
    sib_meta = remote(mown, sib_m, ssend.at[1], srecv.at[1], sibling)

    meta_sent, feat_sent = of_size(mslot, msend, msend), of_size(fslot, fsend, fsend)
    meta_rest = of_size(mslot.at[pl.ds(3, 7)], msend, mrecv.at[3])
    corners = of_size(fslot.at[pl.ds(4, 4)], fsend, frecv.at[3])
    back_all = of_size(pslot, psend, precv)

    loads[0].wait()
    pl.semaphore_wait(barrier, 6 + last - near)

    def tell(sem, d):
        pl.semaphore_signal(sem, inc=1, device_id=d, device_id_type=pl.DeviceIdType.MESH)

    @pl.when(last == 1)
    def _():
        tell(ready, above)

    @pl.when(late == 1)
    def _():
        for d in (*dest[:4], sibling):
            tell(go, d)

    @pl.when(first - late_sib == 1)
    def _():
        sib_meta.start()
        sib_feat.start()

    direct = ((meta[0], f_g_last[0], f_g[0]), (meta[1], f_g_last[1], f_g[1]), (meta[2], f_part), (meta[3], *f_out))
    meta[4].start()
    f_p_up[0].start()

    @pl.when(via_lo == 0)
    def _():
        f_p_up[1].start()

    @pl.when(z != 0)
    def _():
        meta[5].start()
        f_p_dn.start()

    for k in (3, 0, 1, 2):

        @pl.when(late_to[k] == 0)
        def _(k=k):
            for c in direct[k]:
                c.start()

    for c in loads[3:]:
        c.wait()

    left, right = edges_ref[0:1, :], edges_ref[1:2, :]
    row = lax.broadcasted_iota(jnp.int32, (ATOMS, EDGES), 0)
    lane = lax.broadcasted_iota(jnp.int32, (EDGES, ATOMS), 1)

    def column_of(index):
        turned = jnp.transpose(jnp.broadcast_to(index.astype(F32), (8, EDGES)))
        return jnp.broadcast_to(turned[:, 0:1].astype(jnp.int32), (EDGES, ATOMS))

    left_col, right_col = column_of(left), column_of(right)

    def one_hot(match):
        return jnp.where(match, 1.0, 0.0).astype(BF16)

    for k in range(3):
        base = ATOMS * k
        ohp[base : base + ATOMS, :] = one_hot(row == left - base)
        ohpt[:, base : base + ATOMS] = one_hot(lane == left_col - base)
    u_part, u_out = 2 - 2 * odd, 2 * odd
    places = ((1, 0), (1, 1), (1, 2), (u_part, 1), (u_out, 1), (u_part, 0), (u_part, 2), (u_out, 0), (u_out, 2))
    for k, (u, v) in enumerate(places):
        base = (3 * u + v) * ATOMS
        ohc[ATOMS * k : ATOMS * (k + 1), :] = one_hot(row == right - base)
        ohct[:, ATOMS * k : ATOMS * (k + 1)] = one_hot(lane == right_col - base)

    tmat[...] = jnp.zeros_like(tmat)
    tmat[0:6, 0:CH] = table_ref[...].astype(F32)
    tmat[6:7, 0:CH] = wout_ref[...].astype(F32)
    turned = jnp.transpose(tmat[...])
    embt = turned[0:CH, :].astype(BF16)
    wout = turned[0:CH, 6:7]
    wtmp[0 : 5 * CH, :] = w1_ref[RB : RB + 5 * CH, :].astype(F32)
    wtmp[5 * CH : 6 * CH - RB, :] = jnp.zeros((CH - RB, LAT), F32)
    wtmp[6 * CH - RB : 6 * CH, :] = w1_ref[0:RB, :].astype(F32)
    wfull = wtmp[...]
    wpt[...] = wfull.astype(BF16)
    wp[...] = jnp.transpose(wfull).astype(BF16)
    w2t[...] = jnp.transpose(w2_ref[...].astype(F32)).astype(BF16)

    @pl.when(near == 1)
    def _():
        pl.semaphore_wait(go, 1)

        @pl.when(late_sib == 1)
        def _():
            sib_meta.start()
            sib_feat.start()

        for k in (3, 0, 1, 2):

            @pl.when(late_to[k] == 1)
            def _(k=k):
                for c in direct[k]:
                    c.start()

    meta[3].wait_recv()
    m_up.start()
    m_dn.start()
    for k in range(2):
        meta[k].wait_recv()
        m_part[k].start()
    for k, c in enumerate(f_out[:-1]):
        c.wait_recv()
        r_up[k].start()
        r_dn[k].start()
        if k == 0:
            for c_last in f_g_last:
                c_last.wait_recv()

            @pl.when(z != 0)
            def _():
                for c_out in r_out:
                    c_out.start()

    f_out[-1].wait_recv()

    @pl.when(z == 0)
    def _():
        r_up[-1].start()
        r_dn[-1].start()

    def to_partner():
        for k in range(2):
            f_g[k].wait_recv()
            r_part[k].start()

    @pl.when(via_lo == 1)
    def _():
        f_p_up[1].start()

    @pl.when(z == 0)
    def _():
        to_partner()
        sib_meta.wait_recv()
        sib_feat.wait_recv()
        pl.semaphore_wait(ready, 1)
        meta_sib.start()
        f_p_sib.start()

    meta_rest.wait_recv()
    mi = dot(jnp.concatenate([mslot[8], mown[...], mslot[9]], 1), ohp[...])
    order = [mslot[0], mown[...], *(mslot[k] for k in range(1, 8))]
    mj = dot(jnp.concatenate(order, 1), ohc[...])
    off_i = jnp.where(left < ATOMS, -1.0, jnp.where(left < 2 * ATOMS, 0.0, 1.0))
    off_u = jnp.where(right < 3 * ATOMS, 0, jnp.where(right < 6 * ATOMS, 1, 2))
    rest = right - 3 * ATOMS * off_u
    off_v = jnp.where(rest < ATOMS, -1.0, jnp.where(rest < 2 * ATOMS, 0.0, 1.0))
    dx = (mj[0:1] + mj[3:4]) - (mi[0:1] + mi[3:4] + off_i)
    dy = (mj[1:2] + mj[4:5] + (off_u.astype(F32) - 1.0)) - (mi[1:2] + mi[4:5])
    dz = (mj[2:3] + mj[5:6] + off_v) - (mi[2:3] + mi[5:6])
    r2 = dx * dx + dy * dy + dz * dz + SOFTEN
    r = jnp.sqrt(r2)
    inv = 1.0 / r
    nx, ny, nz = dx * inv, dy * inv, dz * inv
    root3, root5, root15 = math.sqrt(3.0), math.sqrt(5.0), math.sqrt(15.0)
    harm = (
        root3 * nx, root3 * ny, root3 * nz, root15 * nx * ny, root15 * ny * nz,
        0.5 * root5 * (3.0 * nz * nz - 1.0), root15 * nx * nz, 0.5 * root15 * (nx * nx - ny * ny),
    )
    for m in range(8):
        yb[m] = jnp.broadcast_to(harm[m], (8, EDGES))
    orders = (lax.broadcasted_iota(jnp.int32, (RB, EDGES), 0) + 1).astype(F32)
    sin_b, cos_b = sin_cos_pi(orders * (1.0 / RADIUS) * r)
    radial = sin_b * inv
    slope = (orders * (math.pi / RADIUS) * cos_b - radial) * inv
    live = jnp.where(lax.broadcasted_iota(jnp.int32, (1, EDGES), 1) < count_ref[0, 0], 1.0, 0.0)
    gap = jnp.maximum(1.0 - r2 * (1.0 / (RADIUS * RADIUS)), 0.0)
    env = live * gap * gap
    kinds = lax.broadcasted_iota(jnp.int32, (LAT, EDGES), 0)
    for k, m in enumerate((mi, mj)):
        pick = jnp.where(kinds == m[6:7].astype(jnp.int32), 1.0, 0.0).astype(BF16)
        xbuf[CH * k : CH * (k + 1), :] = dot(embt, pick).astype(BF16)
    xbuf[5 * CH : 6 * CH - 16, :] = jnp.zeros((CH - 16, EDGES), BF16)
    xbuf[6 * CH - 16 : 6 * CH, :] = jnp.concatenate([jnp.zeros_like(radial), radial], 0).astype(BF16)

    def rows_of(ref, m, k):
        return ref[m * CH + 8 * k : m * CH + 8 * k + 8, :]

    def degree_sums(ref, out, other=None):
        for k2 in range(CH // 16):
            prods = [[], [], []]
            for k in (2 * k2, 2 * k2 + 1):
                one = [rows_of(ref, m, k) * yb[m - 1] for m in range(1, 9)]
                sums = (
                    rows_of(ref, 0, k),
                    one[0] + one[1] + one[2],
                    one[3] + one[4] + one[5] + one[6] + one[7],
                )
                for l in range(3):
                    at = slice(l * CH + 8 * k, l * CH + 8 * k + 8)
                    out[at, :] = sums[l]
                    if other is not None:
                        prods[l].append(sums[l] * other[at, :])
            if other is not None:
                for l in range(3):
                    start = (2 + l) * CH + 16 * k2
                    xbuf[start : start + 16, :] = jnp.concatenate(prods[l], 0).astype(BF16)

    def last_columns():
        corners.wait_recv()
        late_blocks = jnp.concatenate([fslot[k] for k in range(4, 8)], 1)
        gj[...] = gj[...] + dot(late_blocks, ohc[5 * ATOMS :, :])

    pl.when(z != 0)(to_partner)
    f_part.wait_recv()
    order = [fslot[0], feat_ref[...], fslot[1], fslot[2], fslot[3]]
    gj[...] = dot(jnp.concatenate(order, 1), ohc[0 : 5 * ATOMS, :])

    @pl.when(z == 0)
    def _():
        f_p_dn.wait_recv()
        gi[...] = dot(jnp.concatenate([feat_ref[...], fslot[9]], 1), ohp[ATOMS:, :])
        last_columns()
        degree_sums(gj, sj)
        up_all.wait_recv()
        gi[...] = gi[...] + dot(fslot[8], ohp[0:ATOMS, :])
        degree_sums(gi, si, sj)

    @pl.when(z != 0)
    def _():
        f_p_dn.wait_recv()
        up_all.wait_recv()
        gi[...] = dot(jnp.concatenate([fslot[8], feat_ref[...], fslot[9]], 1), ohp[...])
        degree_sums(gi, si)
        last_columns()
        degree_sums(gj, sj, si)

    z1 = dot(wp[...], xbuf[...])
    sig1 = 1.0 / (1.0 + jnp.exp(-z1))
    z2 = dot(w2_ref[...], (z1 * sig1).astype(BF16))
    sig2 = 1.0 / (1.0 + jnp.exp(-z2))
    u = jnp.sum(wout * (z2 * sig2), 0, keepdims=True)
    energy_ref[...] = env * u

    dz2 = (wout * env) * (sig2 * (1.0 + z2 * (1.0 - sig2)))
    dh = dot(w2t[...], dz2.astype(BF16)).astype(BF16).astype(F32)
    dz1 = dh * (sig1 * (1.0 + z1 * (1.0 - sig1)))
    dxv = dot(wpt[...], dz1.astype(BF16)).astype(BF16).astype(F32)
    acc = [jnp.zeros((8, EDGES), F32) for _ in range(8)]
    for k in range(CH // 8):
        for l, ms in ((1, (1, 2, 3)), (2, (4, 5, 6, 7, 8))):
            at = slice(l * CH + 8 * k, l * CH + 8 * k + 8)
            dq = dxv[2 * CH + at.start : 2 * CH + at.stop, :]
            di, dj = dq * sj[at, :], dq * si[at, :]
            for m in ms:
                acc[m - 1] = acc[m - 1] + di * rows_of(gi, m, k) + dj * rows_of(gj, m, k)
    h1, h2, h3, h4, h5, h6, h7, h8 = (jnp.sum(a, 0, keepdims=True) for a in acc)
    ax = root3 * h1 + root15 * (ny * h4 + nz * h7 + nx * h8)
    ay = root3 * h2 + root15 * (nx * h4 + nz * h5 - ny * h8)
    az = root3 * h3 + root15 * (ny * h5 + nx * h7) + (3.0 * root5) * nz * h6
    dr = jnp.sum(dxv[6 * CH - RB : 6 * CH, :] * slope, 0, keepdims=True)
    dr = dr - (ax * nx + ay * ny + az * nz) * inv
    denv = live * u * (2.0 * gap) * (-1.0 / (RADIUS * RADIUS))
    scale = dr * inv + 2.0 * denv
    gbuf[...] = jnp.zeros_like(gbuf)
    gbuf[0:1, :] = ax * inv + dx * scale
    gbuf[1:2, :] = ay * inv + dy * scale
    gbuf[2:3, :] = az * inv + dz * scale

    grad = gbuf[...]
    g_hi = grad.astype(BF16).astype(F32)
    both = jnp.concatenate([g_hi, grad - g_hi], 0).astype(BF16)

    def lanes(a, k):
        return a[:, k * ATOMS : (k + 1) * ATOMS]

    back = [remote(pout.at[k], pslot.at[k], psend, precv, home[k]) for k in range(NSLOT)]
    part_p = dot(both, ohpt[...])
    part_p = part_p[0:8] + part_p[8:16]
    pout[8] = lanes(part_p, 0)
    pout[9] = lanes(part_p, 2)
    back[8].start()
    back[9].start()
    part_c = dot(both, ohct[...])
    part_c = -(part_c[0:8] + part_c[8:16])
    for slot, k in enumerate((0, 2, 3, 4, 5, 6, 7, 8)):
        pout[slot] = lanes(part_c, k)
        back[slot].start()
    force = lanes(part_p, 1) + lanes(part_c, 1)
    meta_sent.wait_send()
    feat_sent.wait_send()

    @pl.when(first == 1)
    def _():
        sib_meta.wait_send()
        sib_feat.wait_send()

    back_all.wait_recv()
    for k in range(NSLOT):
        force = force + pslot[k]
    for k in range(3):
        force_ref[k] = force[k : k + 1, :]
    back_all.wait_send()


def finish(force_ref, energy_ref, force_out, energy_out, sems):
    copies = fetch([(force_ref, force_out), (energy_ref, energy_out)], sems)
    for c in copies:
        c.wait()


def shards(positions, features, species, emb_table, edges, edge_count, w_first, w_second, w_out):
    vmem = pl.BlockSpec(memory_space=pltpu.VMEM)
    hbm = pl.BlockSpec(memory_space=pl.ANY)
    dma = pltpu.SemaphoreType.DMA
    pos = jnp.transpose(positions.reshape(1, 3, ATOMS), (1, 0, 2))
    feat = features.reshape(ROWS, ATOMS)
    spec = species.reshape(1, ATOMS)
    small = [pltpu.VMEM((3, 1, ATOMS), F32), pltpu.VMEM((1, ATOMS), jnp.int32)]
    forces, energy = pl.pallas_call(
        kernel,
        name="edge_forces",
        out_shape=(pltpu.VMEM((3, 1, ATOMS), F32), pltpu.VMEM((1, EDGES), F32)),
        in_specs=[hbm] * 9,
        out_specs=(vmem, vmem),
        scratch_shapes=[
            small[0],
            pltpu.VMEM((ROWS, ATOMS), BF16),
            small[1],
            pltpu.VMEM((2, EDGES), jnp.int32),
            pltpu.SMEM((1, 1), jnp.int32),
            pltpu.VMEM((6, CH), BF16),
            pltpu.VMEM((RB + 5 * CH, LAT), BF16),
            pltpu.VMEM((CH, LAT), BF16),
            pltpu.VMEM((1, CH), BF16),
            pltpu.VMEM((ROWS, ATOMS), BF16),
            pltpu.VMEM((16, ATOMS), BF16),
            pltpu.VMEM((NSLOT, ROWS, ATOMS), BF16),
            pltpu.VMEM((16, ATOMS), BF16),
            pltpu.VMEM((NSLOT, 16, ATOMS), BF16),
            pltpu.VMEM((3 * ATOMS, EDGES), BF16),
            pltpu.VMEM((9 * ATOMS, EDGES), BF16),
            pltpu.VMEM((EDGES, 3 * ATOMS), BF16),
            pltpu.VMEM((EDGES, 9 * ATOMS), BF16),
            pltpu.VMEM((ROWS, EDGES), F32),
            pltpu.VMEM((ROWS, EDGES), F32),
            pltpu.VMEM((3 * CH, EDGES), F32),
            pltpu.VMEM((3 * CH, EDGES), F32),
            pltpu.VMEM((8, 8, EDGES), F32),
            pltpu.VMEM((6 * CH, EDGES), BF16),
            pltpu.VMEM((6 * CH, LAT), F32),
            pltpu.VMEM((LAT, 6 * CH), BF16),
            pltpu.VMEM((6 * CH, LAT), BF16),
            pltpu.VMEM((LAT, CH), BF16),
            pltpu.VMEM((LAT, LAT), F32),
            pltpu.VMEM((8, EDGES), F32),
            pltpu.VMEM((16, ATOMS), F32),
            pltpu.VMEM((NSLOT, 8, ATOMS), F32),
            pltpu.VMEM((NSLOT, 8, ATOMS), F32),
            dma((9,)),
            pltpu.SemaphoreType.REGULAR,
            pltpu.SemaphoreType.REGULAR,
            dma,
            dma((4,)),
            dma,
            dma((8 + ROWS // PART,)),
            dma((2,)),
            dma((2,)),
            dma,
            dma,
        ],
        compiler_params=pltpu.CompilerParams(collective_id=0, has_side_effects=True),
    )(
        pos,
        feat,
        spec,
        edges.reshape(2, EDGES),
        edge_count.reshape(1, 1),
        emb_table,
        w_first.T,
        w_second,
        w_out.reshape(1, CH),
    )
    forces, energy = pl.pallas_call(
        finish,
        name="finish",
        out_shape=(jax.ShapeDtypeStruct((3, 1, ATOMS), F32), jax.ShapeDtypeStruct((1, EDGES), F32)),
        in_specs=[vmem, vmem],
        out_specs=(hbm, hbm),
        scratch_shapes=[dma((2,))],
    )(
        pltpu.with_memory_space_constraint(forces, pltpu.VMEM),
        pltpu.with_memory_space_constraint(energy, pltpu.VMEM),
    )
    return (
        jnp.transpose(forces, (1, 0, 2)).reshape(1, 1, 1, 3, ATOMS),
        energy.reshape(1, 1, 1, EDGES),
    )


def solution(mesh):
    placed = (
        P("plate", "tower", "gz", None, None),
        P("plate", "tower", "gz", None, None),
        P("plate", "tower", "gz", None),
        P(),
        P("plate", "tower", "gz", None, None),
        P("plate", "tower", "gz"),
        P(),
        P(),
        P(),
    )
    return jax.shard_map(
        shards,
        mesh=mesh,
        in_specs=placed,
        out_specs=(P("plate", "tower", "gz", None, None), P("plate", "tower", "gz", None)),
        check_vma=False,
    )
```

```python
import math

import jax
import jax.numpy as jnp
from jax import lax
from jax.experimental import pallas as pl
from jax.experimental.pallas import tpu as pltpu
from jax.sharding import PartitionSpec as P

ATOMS = 128
EDGES = 512
CH = 64
LAT = 128
RB = 8
ROWS = 9 * CH
PART = ROWS // 3
RADIUS = 3.0
SOFTEN = 0.04
F32 = jnp.float32
BF16 = jnp.bfloat16

NSLOT = 10


def dot(a, b):
    return lax.dot_general(a, b, (((1,), (0,)), ((), ())), preferred_element_type=F32)


def sin_cos_pi(t):
    turns = jnp.floor(t + 0.5)
    x = (t - turns) * math.pi
    parity = turns - 2.0 * jnp.floor(turns * 0.5)
    sign = 1.0 - 2.0 * parity
    y = x * x
    s = -1.0 / 39916800.0
    for c in (1.0 / 362880.0, -1.0 / 5040.0, 1.0 / 120.0, -1.0 / 6.0, 1.0):
        s = s * y + c
    c_ = 1.0 / 479001600.0
    for c in (-1.0 / 3628800.0, 1.0 / 40320.0, -1.0 / 720.0, 1.0 / 24.0, -0.5, 1.0):
        c_ = c_ * y + c
    return sign * s * x, sign * c_


def remote(src, dst, ssem, rsem, to):
    return pltpu.make_async_remote_copy(
        src_ref=src,
        dst_ref=dst,
        send_sem=ssem,
        recv_sem=rsem,
        device_id=to,
        device_id_type=pl.DeviceIdType.MESH,
    )


def fetch(pairs, sems, base=0):
    copies = [pltpu.make_async_copy(src, dst, sems.at[base + n]) for n, (src, dst) in enumerate(pairs)]
    for c in copies:
        c.start()
    return copies


def pack_small(pos, spec, stage, out):
    stage[...] = jnp.zeros_like(stage)
    for k in range(3):
        hi = pos[k].astype(BF16).astype(F32)
        stage[k : k + 1, :] = hi
        stage[k + 3 : k + 4, :] = (pos[k] - hi).astype(BF16).astype(F32)
    stage[6:7, :] = spec[...].astype(F32)
    out[...] = stage[...].astype(BF16)


DEPTH = 16


def kernel(
    pos_any,
    feat_any,
    spec_any,
    edges_any,
    count_any,
    table_any,
    w1_any,
    w2_any,
    wout_any,
    force_ref,
    energy_ref,
    pos,
    feat_ref,
    spec_ref,
    edges_ref,
    count_ref,
    table_ref,
    w1_ref,
    w2_ref,
    wout_ref,
    sib_f,
    sib_m,
    fslot,
    mown,
    mslot,
    ohp,
    ohc,
    ohpt,
    ohct,
    gi,
    gj,
    si,
    sj,
    yb,
    xbuf,
    wtmp,
    wp,
    wpt,
    w2t,
    tmat,
    gbuf,
    stage,
    pout,
    pslot,
    lsem,
    ready,
    go,
    msend,
    mrecv,
    fsend,
    frecv,
    ssend,
    srecv,
    psend,
    precv,
):
    n_plate, n_tower, n_gz = (lax.axis_size(a) for a in ("plate", "tower", "gz"))
    p, t, g = (lax.axis_index(a) for a in ("plate", "tower", "gz"))
    odd = lax.rem(t, 2)
    partner = t + 1 - 2 * odd
    outward = lax.rem(t + 2 * odd - 1 + n_tower, n_tower)
    g_up, g_dn = lax.rem(g + 1, n_gz), lax.rem(g + n_gz - 1, n_gz)
    p_up, p_dn = lax.rem(p + 1, n_plate), lax.rem(p + n_plate - 1, n_plate)
    z = lax.rem(p, DEPTH)
    last = z // (DEPTH - 1)
    first = lax.rem(z + DEPTH - 1, DEPTH) // (DEPTH - 1)

    total = n_plate * n_tower * n_gz

    def dev(pp, tt, gg):
        return {"plate": pp, "tower": tt, "gz": gg}

    def is_late(d):
        return 1 - ((d["plate"] * n_tower + d["tower"]) * n_gz + d["gz"] + total - 1) // total


    dest = [
        dev(p, t, g_up), dev(p, t, g_dn), dev(p, partner, g), dev(p, outward, g),
        dev(p, partner, g_up), dev(p, partner, g_dn), dev(p, outward, g_up), dev(p, outward, g_dn),
        dev(p_up, t, g), dev(p_dn, t, g),
    ]
    home = [dest[k] for k in (1, 0, 2, 3, 5, 4, 7, 6, 9, 8)]
    sibling = dev(lax.rem(p + DEPTH, n_plate), t, g)
    below = dev(lax.rem(p + n_plate - 1 + DEPTH * first, n_plate), t, g)
    above = dev(lax.rem(p + 1 + DEPTH, n_plate), t, g)

    loads = fetch([(feat_any, feat_ref)], lsem)
    barrier = pltpu.get_barrier_semaphore()

    def greet(d):
        pl.semaphore_signal(barrier, inc=1, device_id=d, device_id_type=pl.DeviceIdType.MESH)

    late = is_late(dev(p, t, g))
    late_to = [is_late(d) for d in dest[:4]]
    late_sib = first * is_late(sibling)
    near = late_to[0] + late_to[1] + late_to[2] + late_to[3] + late_sib

    via_lo = last * (1 - p // DEPTH)

    greet(below)

    @pl.when(late == 0)
    def _():
        for d in dest[:4]:
            greet(d)

    @pl.when(z == 0)
    def _():
        greet(dest[9])

    @pl.when(first - late == 1)
    def _():
        greet(sibling)

    @pl.when(last == 0)
    def _():
        greet(dest[8])

    loads += fetch(
        [
            (pos_any, pos), (spec_any, spec_ref), (edges_any, edges_ref), (count_any, count_ref),
            (table_any, table_ref), (w1_any, w1_ref), (w2_any, w2_ref), (wout_any, wout_ref),
        ],
        lsem,
        1,
    )
    for c in loads[1:3]:
        c.wait()
    pack_small(pos, spec_ref, stage, mown)

    def small_rows(src, k, to):
        n = {0: 0, 1: 1, 3: 2}.get(k, 3)
        return remote(src, mslot.at[k], msend, mrecv.at[n], to)

    meta = [small_rows(mown, k, dest[k]) for k in range(4)]
    m_part = [small_rows(mslot.at[k], 4 + k, dest[2]) for k in range(2)]
    m_up, m_dn = small_rows(mslot.at[3], 6, dest[0]), small_rows(mslot.at[3], 7, dest[1])
    meta += [small_rows(mown, 8, dest[8]), small_rows(mown, 9, below)]
    meta_sib = small_rows(sib_m, 9, below)
    def of_size(ref, ssem, rsem):
        return remote(ref, ref, ssem, rsem, dest[0])

    parts = [pl.ds(PART * k, PART) for k in range(ROWS // PART)]

    def feature(n, src, slot, to, part=None):
        dst = fslot.at[slot]
        if part is not None:
            src, dst = src.at[part], dst.at[part]
        return remote(src, dst, fsend, frecv.at[n], to)

    head = pl.ds(0, ROWS - PART)
    n_parts = len(parts)
    f_g = [feature(k, feat_ref, k, dest[k], head) for k in range(2)]
    f_g_last = [feature(6 + n_parts + k, feat_ref, k, dest[k], parts[-1]) for k in range(2)]
    r_out = [feature(3, fslot.at[k], 6 + k, dest[3], parts[-1]) for k in range(2)]
    f_part = feature(2, feat_ref, 2, dest[2])
    r_part = [feature(3, fslot.at[0], 4, dest[2]), feature(3, fslot.at[1], 5, dest[2])]
    r_up = [feature(3, fslot.at[3], 6, dest[0], c) for c in parts]
    r_dn = [feature(3, fslot.at[3], 7, dest[1], c) for c in parts]
    f_p_up = [feature(4, feat_ref, 8, dest[8], pl.ds(ROWS // 2 * k, ROWS // 2)) for k in range(2)]
    up_all = of_size(fslot.at[8], fsend, frecv.at[4])
    f_p_dn = feature(5, feat_ref, 9, below)
    f_p_sib = feature(5, sib_f, 9, below)
    f_out = [feature(6 + k, feat_ref, 3, dest[3], c) for k, c in enumerate(parts)]
    sib_feat = remote(feat_ref, sib_f, ssend.at[0], srecv.at[0], sibling)
    sib_meta = remote(mown, sib_m, ssend.at[1], srecv.at[1], sibling)

    meta_sent, feat_sent = of_size(mslot, msend, msend), of_size(fslot, fsend, fsend)
    meta_rest = of_size(mslot.at[pl.ds(3, 7)], msend, mrecv.at[3])
    corners = of_size(fslot.at[pl.ds(4, 4)], fsend, frecv.at[3])
    back_all = of_size(pslot, psend, precv)

    loads[0].wait()
    pl.semaphore_wait(barrier, 6 + last - near)

    def tell(sem, d):
        pl.semaphore_signal(sem, inc=1, device_id=d, device_id_type=pl.DeviceIdType.MESH)

    @pl.when(last == 1)
    def _():
        tell(ready, above)

    @pl.when(late == 1)
    def _():
        for d in (*dest[:4], sibling):
            tell(go, d)

    @pl.when(first - late_sib == 1)
    def _():
        sib_meta.start()
        sib_feat.start()

    direct = ((meta[0], f_g_last[0], f_g[0]), (meta[1], f_g_last[1], f_g[1]), (meta[2], f_part), (meta[3], *f_out))
    meta[4].start()
    f_p_up[0].start()

    @pl.when(via_lo == 0)
    def _():
        f_p_up[1].start()

    @pl.when(z != 0)
    def _():
        meta[5].start()
        f_p_dn.start()

    for k in (3, 0, 1, 2):

        @pl.when(late_to[k] == 0)
        def _(k=k):
            for c in direct[k]:
                c.start()

    for c in loads[3:]:
        c.wait()

    left, right = edges_ref[0:1, :], edges_ref[1:2, :]
    row = lax.broadcasted_iota(jnp.int32, (ATOMS, EDGES), 0)
    lane = lax.broadcasted_iota(jnp.int32, (EDGES, ATOMS), 1)

    def column_of(index):
        turned = jnp.transpose(jnp.broadcast_to(index.astype(F32), (8, EDGES)))
        return jnp.broadcast_to(turned[:, 0:1].astype(jnp.int32), (EDGES, ATOMS))

    left_col, right_col = column_of(left), column_of(right)

    def one_hot(match):
        return jnp.where(match, 1.0, 0.0).astype(BF16)

    for k in range(3):
        base = ATOMS * k
        ohp[base : base + ATOMS, :] = one_hot(row == left - base)
        ohpt[:, base : base + ATOMS] = one_hot(lane == left_col - base)
    u_part, u_out = 2 - 2 * odd, 2 * odd
    places = ((1, 0), (1, 1), (1, 2), (u_part, 1), (u_out, 1), (u_part, 0), (u_part, 2), (u_out, 0), (u_out, 2))
    for k, (u, v) in enumerate(places):
        base = (3 * u + v) * ATOMS
        ohc[ATOMS * k : ATOMS * (k + 1), :] = one_hot(row == right - base)
        ohct[:, ATOMS * k : ATOMS * (k + 1)] = one_hot(lane == right_col - base)

    tmat[...] = jnp.zeros_like(tmat)
    tmat[0:6, 0:CH] = table_ref[...].astype(F32)
    tmat[6:7, 0:CH] = wout_ref[...].astype(F32)
    turned = jnp.transpose(tmat[...])
    embt = turned[0:CH, :].astype(BF16)
    wout = turned[0:CH, 6:7]
    wtmp[0 : 5 * CH, :] = w1_ref[RB : RB + 5 * CH, :].astype(F32)
    wtmp[5 * CH : 6 * CH - RB, :] = jnp.zeros((CH - RB, LAT), F32)
    wtmp[6 * CH - RB : 6 * CH, :] = w1_ref[0:RB, :].astype(F32)
    wfull = wtmp[...]
    wpt[...] = wfull.astype(BF16)
    wp[...] = jnp.transpose(wfull).astype(BF16)
    w2t[...] = jnp.transpose(w2_ref[...].astype(F32)).astype(BF16)

    @pl.when(near == 1)
    def _():
        pl.semaphore_wait(go, 1)

        @pl.when(late_sib == 1)
        def _():
            sib_meta.start()
            sib_feat.start()

        for k in (3, 0, 1, 2):

            @pl.when(late_to[k] == 1)
            def _(k=k):
                for c in direct[k]:
                    c.start()

    meta[3].wait_recv()
    m_up.start()
    m_dn.start()
    for k in range(2):
        meta[k].wait_recv()
        m_part[k].start()
    for k, c in enumerate(f_out[:-1]):
        c.wait_recv()
        r_up[k].start()
        r_dn[k].start()
        if k == 0:
            for c_last in f_g_last:
                c_last.wait_recv()

            @pl.when(z != 0)
            def _():
                for c_out in r_out:
                    c_out.start()

    f_out[-1].wait_recv()

    @pl.when(z == 0)
    def _():
        r_up[-1].start()
        r_dn[-1].start()

    def to_partner():
        for k in range(2):
            f_g[k].wait_recv()
            r_part[k].start()

    @pl.when(via_lo == 1)
    def _():
        f_p_up[1].start()

    @pl.when(z == 0)
    def _():
        to_partner()
        sib_meta.wait_recv()
        sib_feat.wait_recv()
        pl.semaphore_wait(ready, 1)
        meta_sib.start()
        f_p_sib.start()

    meta_rest.wait_recv()
    mi = dot(jnp.concatenate([mslot[8], mown[...], mslot[9]], 1), ohp[...])
    order = [mslot[0], mown[...], *(mslot[k] for k in range(1, 8))]
    mj = dot(jnp.concatenate(order, 1), ohc[...])
    off_i = jnp.where(left < ATOMS, -1.0, jnp.where(left < 2 * ATOMS, 0.0, 1.0))
    off_u = jnp.where(right < 3 * ATOMS, 0, jnp.where(right < 6 * ATOMS, 1, 2))
    rest = right - 3 * ATOMS * off_u
    off_v = jnp.where(rest < ATOMS, -1.0, jnp.where(rest < 2 * ATOMS, 0.0, 1.0))
    dx = (mj[0:1] + mj[3:4]) - (mi[0:1] + mi[3:4] + off_i)
    dy = (mj[1:2] + mj[4:5] + (off_u.astype(F32) - 1.0)) - (mi[1:2] + mi[4:5])
    dz = (mj[2:3] + mj[5:6] + off_v) - (mi[2:3] + mi[5:6])
    r2 = dx * dx + dy * dy + dz * dz + SOFTEN
    r = jnp.sqrt(r2)
    inv = 1.0 / r
    nx, ny, nz = dx * inv, dy * inv, dz * inv
    root3, root5, root15 = math.sqrt(3.0), math.sqrt(5.0), math.sqrt(15.0)
    harm = (
        root3 * nx, root3 * ny, root3 * nz, root15 * nx * ny, root15 * ny * nz,
        0.5 * root5 * (3.0 * nz * nz - 1.0), root15 * nx * nz, 0.5 * root15 * (nx * nx - ny * ny),
    )
    for m in range(8):
        yb[m] = jnp.broadcast_to(harm[m], (8, EDGES))
    orders = (lax.broadcasted_iota(jnp.int32, (RB, EDGES), 0) + 1).astype(F32)
    sin_b, cos_b = sin_cos_pi(orders * (1.0 / RADIUS) * r)
    radial = sin_b * inv
    slope = (orders * (math.pi / RADIUS) * cos_b - radial) * inv
    live = jnp.where(lax.broadcasted_iota(jnp.int32, (1, EDGES), 1) < count_ref[0, 0], 1.0, 0.0)
    gap = jnp.maximum(1.0 - r2 * (1.0 / (RADIUS * RADIUS)), 0.0)
    env = live * gap * gap
    kinds = lax.broadcasted_iota(jnp.int32, (LAT, EDGES), 0)
    for k, m in enumerate((mi, mj)):
        pick = jnp.where(kinds == m[6:7].astype(jnp.int32), 1.0, 0.0).astype(BF16)
        xbuf[CH * k : CH * (k + 1), :] = dot(embt, pick).astype(BF16)
    xbuf[5 * CH : 6 * CH - 16, :] = jnp.zeros((CH - 16, EDGES), BF16)
    xbuf[6 * CH - 16 : 6 * CH, :] = jnp.concatenate([jnp.zeros_like(radial), radial], 0).astype(BF16)

    def rows_of(ref, m, k):
        return ref[m * CH + 8 * k : m * CH + 8 * k + 8, :]

    def degree_sums(ref, out, other=None):
        for k2 in range(CH // 16):
            prods = [[], [], []]
            for k in (2 * k2, 2 * k2 + 1):
                one = [rows_of(ref, m, k) * yb[m - 1] for m in range(1, 9)]
                sums = (
                    rows_of(ref, 0, k),
                    one[0] + one[1] + one[2],
                    one[3] + one[4] + one[5] + one[6] + one[7],
                )
                for l in range(3):
                    at = slice(l * CH + 8 * k, l * CH + 8 * k + 8)
                    out[at, :] = sums[l]
                    if other is not None:
                        prods[l].append(sums[l] * other[at, :])
            if other is not None:
                for l in range(3):
                    start = (2 + l) * CH + 16 * k2
                    xbuf[start : start + 16, :] = jnp.concatenate(prods[l], 0).astype(BF16)

    def last_columns():
        corners.wait_recv()
        late_blocks = jnp.concatenate([fslot[k] for k in range(4, 8)], 1)
        gj[...] = gj[...] + dot(late_blocks, ohc[5 * ATOMS :, :])

    pl.when(z != 0)(to_partner)
    f_part.wait_recv()
    order = [fslot[0], feat_ref[...], fslot[1], fslot[2], fslot[3]]
    gj[...] = dot(jnp.concatenate(order, 1), ohc[0 : 5 * ATOMS, :])

    @pl.when(z == 0)
    def _():
        f_p_dn.wait_recv()
        gi[...] = dot(jnp.concatenate([feat_ref[...], fslot[9]], 1), ohp[ATOMS:, :])
        last_columns()
        degree_sums(gj, sj)
        up_all.wait_recv()
        gi[...] = gi[...] + dot(fslot[8], ohp[0:ATOMS, :])
        degree_sums(gi, si, sj)

    @pl.when(z != 0)
    def _():
        f_p_dn.wait_recv()
        up_all.wait_recv()
        gi[...] = dot(jnp.concatenate([fslot[8], feat_ref[...], fslot[9]], 1), ohp[...])
        degree_sums(gi, si)
        last_columns()
        degree_sums(gj, sj, si)

    z1 = dot(wp[...], xbuf[...])
    sig1 = 1.0 / (1.0 + jnp.exp(-z1))
    z2 = dot(w2_ref[...], (z1 * sig1).astype(BF16))
    sig2 = 1.0 / (1.0 + jnp.exp(-z2))
    u = jnp.sum(wout * (z2 * sig2), 0, keepdims=True)
    energy_ref[...] = env * u

    dz2 = (wout * env) * (sig2 * (1.0 + z2 * (1.0 - sig2)))
    dh = dot(w2t[...], dz2.astype(BF16)).astype(BF16).astype(F32)
    dz1 = dh * (sig1 * (1.0 + z1 * (1.0 - sig1)))
    dxv = dot(wpt[...], dz1.astype(BF16)).astype(BF16).astype(F32)
    acc = [jnp.zeros((8, EDGES), F32) for _ in range(8)]
    for k in range(CH // 8):
        for l, ms in ((1, (1, 2, 3)), (2, (4, 5, 6, 7, 8))):
            at = slice(l * CH + 8 * k, l * CH + 8 * k + 8)
            dq = dxv[2 * CH + at.start : 2 * CH + at.stop, :]
            di, dj = dq * sj[at, :], dq * si[at, :]
            for m in ms:
                acc[m - 1] = acc[m - 1] + di * rows_of(gi, m, k) + dj * rows_of(gj, m, k)
    h1, h2, h3, h4, h5, h6, h7, h8 = (jnp.sum(a, 0, keepdims=True) for a in acc)
    ax = root3 * h1 + root15 * (ny * h4 + nz * h7 + nx * h8)
    ay = root3 * h2 + root15 * (nx * h4 + nz * h5 - ny * h8)
    az = root3 * h3 + root15 * (ny * h5 + nx * h7) + (3.0 * root5) * nz * h6
    dr = jnp.sum(dxv[6 * CH - RB : 6 * CH, :] * slope, 0, keepdims=True)
    dr = dr - (ax * nx + ay * ny + az * nz) * inv
    denv = live * u * (2.0 * gap) * (-1.0 / (RADIUS * RADIUS))
    scale = dr * inv + 2.0 * denv
    gbuf[...] = jnp.zeros_like(gbuf)
    gbuf[0:1, :] = ax * inv + dx * scale
    gbuf[1:2, :] = ay * inv + dy * scale
    gbuf[2:3, :] = az * inv + dz * scale

    grad = gbuf[...]
    g_hi = grad.astype(BF16).astype(F32)
    both = jnp.concatenate([g_hi, grad - g_hi], 0).astype(BF16)

    def lanes(a, k):
        return a[:, k * ATOMS : (k + 1) * ATOMS]

    back = [remote(pout.at[k], pslot.at[k], psend, precv, home[k]) for k in range(NSLOT)]
    part_p = dot(both, ohpt[...])
    part_p = part_p[0:8] + part_p[8:16]
    pout[8] = lanes(part_p, 0)
    pout[9] = lanes(part_p, 2)
    back[8].start()
    back[9].start()
    part_c = dot(both, ohct[...])
    part_c = -(part_c[0:8] + part_c[8:16])
    for slot, k in enumerate((0, 2, 3, 4, 5, 6, 7, 8)):
        pout[slot] = lanes(part_c, k)
        back[slot].start()
    force = lanes(part_p, 1) + lanes(part_c, 1)
    meta_sent.wait_send()
    feat_sent.wait_send()

    @pl.when(first == 1)
    def _():
        sib_meta.wait_send()
        sib_feat.wait_send()

    back_all.wait_recv()
    for k in range(NSLOT):
        force = force + pslot[k]
    for k in range(3):
        force_ref[k] = force[k : k + 1, :]
    back_all.wait_send()


def finish(force_ref, energy_ref, force_out, energy_out, sems):
    copies = fetch([(force_ref, force_out), (energy_ref, energy_out)], sems)
    for c in copies:
        c.wait()


def shards(positions, features, species, emb_table, edges, edge_count, w_first, w_second, w_out):
    vmem = pl.BlockSpec(memory_space=pltpu.VMEM)
    hbm = pl.BlockSpec(memory_space=pl.ANY)
    dma = pltpu.SemaphoreType.DMA
    pos = jnp.transpose(positions.reshape(1, 3, ATOMS), (1, 0, 2))
    feat = features.reshape(ROWS, ATOMS)
    spec = species.reshape(1, ATOMS)
    small = [pltpu.VMEM((3, 1, ATOMS), F32), pltpu.VMEM((1, ATOMS), jnp.int32)]
    forces, energy = pl.pallas_call(
        kernel,
        name="edge_forces",
        out_shape=(pltpu.VMEM((3, 1, ATOMS), F32), pltpu.VMEM((1, EDGES), F32)),
        in_specs=[hbm] * 9,
        out_specs=(vmem, vmem),
        scratch_shapes=[
            small[0],
            pltpu.VMEM((ROWS, ATOMS), BF16),
            small[1],
            pltpu.VMEM((2, EDGES), jnp.int32),
            pltpu.SMEM((1, 1), jnp.int32),
            pltpu.VMEM((6, CH), BF16),
            pltpu.VMEM((RB + 5 * CH, LAT), BF16),
            pltpu.VMEM((CH, LAT), BF16),
            pltpu.VMEM((1, CH), BF16),
            pltpu.VMEM((ROWS, ATOMS), BF16),
            pltpu.VMEM((16, ATOMS), BF16),
            pltpu.VMEM((NSLOT, ROWS, ATOMS), BF16),
            pltpu.VMEM((16, ATOMS), BF16),
            pltpu.VMEM((NSLOT, 16, ATOMS), BF16),
            pltpu.VMEM((3 * ATOMS, EDGES), BF16),
            pltpu.VMEM((9 * ATOMS, EDGES), BF16),
            pltpu.VMEM((EDGES, 3 * ATOMS), BF16),
            pltpu.VMEM((EDGES, 9 * ATOMS), BF16),
            pltpu.VMEM((ROWS, EDGES), F32),
            pltpu.VMEM((ROWS, EDGES), F32),
            pltpu.VMEM((3 * CH, EDGES), F32),
            pltpu.VMEM((3 * CH, EDGES), F32),
            pltpu.VMEM((8, 8, EDGES), F32),
            pltpu.VMEM((6 * CH, EDGES), BF16),
            pltpu.VMEM((6 * CH, LAT), F32),
            pltpu.VMEM((LAT, 6 * CH), BF16),
            pltpu.VMEM((6 * CH, LAT), BF16),
            pltpu.VMEM((LAT, CH), BF16),
            pltpu.VMEM((LAT, LAT), F32),
            pltpu.VMEM((8, EDGES), F32),
            pltpu.VMEM((16, ATOMS), F32),
            pltpu.VMEM((NSLOT, 8, ATOMS), F32),
            pltpu.VMEM((NSLOT, 8, ATOMS), F32),
            dma((9,)),
            pltpu.SemaphoreType.REGULAR,
            pltpu.SemaphoreType.REGULAR,
            dma,
            dma((4,)),
            dma,
            dma((8 + ROWS // PART,)),
            dma((2,)),
            dma((2,)),
            dma,
            dma,
        ],
        compiler_params=pltpu.CompilerParams(collective_id=0, has_side_effects=True),
    )(
        pos,
        feat,
        spec,
        edges.reshape(2, EDGES),
        edge_count.reshape(1, 1),
        emb_table,
        w_first.T,
        w_second,
        w_out.reshape(1, CH),
    )
    forces, energy = pl.pallas_call(
        finish,
        name="finish",
        out_shape=(jax.ShapeDtypeStruct((3, 1, ATOMS), F32), jax.ShapeDtypeStruct((1, EDGES), F32)),
        in_specs=[vmem, vmem],
        out_specs=(hbm, hbm),
        scratch_shapes=[dma((2,))],
    )(
        pltpu.with_memory_space_constraint(forces, pltpu.VMEM),
        pltpu.with_memory_space_constraint(energy, pltpu.VMEM),
    )
    return (
        jnp.transpose(forces, (1, 0, 2)).reshape(1, 1, 1, 3, ATOMS),
        energy.reshape(1, 1, 1, EDGES),
    )


def solution(mesh):
    placed = (
        P("plate", "tower", "gz", None, None),
        P("plate", "tower", "gz", None, None),
        P("plate", "tower", "gz", None),
        P(),
        P("plate", "tower", "gz", None, None),
        P("plate", "tower", "gz"),
        P(),
        P(),
        P(),
    )
    return jax.shard_map(
        shards,
        mesh=mesh,
        in_specs=placed,
        out_specs=(P("plate", "tower", "gz", None, None), P("plate", "tower", "gz", None)),
        check_vma=False,
    )
```

```python
import math

import jax
import jax.numpy as jnp
from jax import lax
from jax.experimental import pallas as pl
from jax.experimental.pallas import tpu as pltpu
from jax.sharding import PartitionSpec as P

ATOMS = 128
EDGES = 512
CH = 64
LAT = 128
RB = 8
ROWS = 9 * CH
PART = ROWS // 3
LOTS = 2
RADIUS = 3.0
SOFTEN = 0.04
F32 = jnp.float32
BF16 = jnp.bfloat16

NSLOT = 10


def dot(a, b):
    return lax.dot_general(a, b, (((1,), (0,)), ((), ())), preferred_element_type=F32)


def sin_cos_pi(t):
    turns = jnp.floor(t + 0.5)
    x = (t - turns) * math.pi
    parity = turns - 2.0 * jnp.floor(turns * 0.5)
    sign = 1.0 - 2.0 * parity
    y = x * x
    s = -1.0 / 39916800.0
    for c in (1.0 / 362880.0, -1.0 / 5040.0, 1.0 / 120.0, -1.0 / 6.0, 1.0):
        s = s * y + c
    c_ = 1.0 / 479001600.0
    for c in (-1.0 / 3628800.0, 1.0 / 40320.0, -1.0 / 720.0, 1.0 / 24.0, -0.5, 1.0):
        c_ = c_ * y + c
    return sign * s * x, sign * c_


def remote(src, dst, ssem, rsem, to):
    return pltpu.make_async_remote_copy(
        src_ref=src,
        dst_ref=dst,
        send_sem=ssem,
        recv_sem=rsem,
        device_id=to,
        device_id_type=pl.DeviceIdType.MESH,
    )


def fetch(pairs, sems, base=0):
    copies = [pltpu.make_async_copy(src, dst, sems.at[base + n]) for n, (src, dst) in enumerate(pairs)]
    for c in copies:
        c.start()
    return copies


def pack_small(pos, spec, stage, out):
    stage[...] = jnp.zeros_like(stage)
    for k in range(3):
        hi = pos[k].astype(BF16).astype(F32)
        stage[k : k + 1, :] = hi
        stage[k + 3 : k + 4, :] = (pos[k] - hi).astype(BF16).astype(F32)
    stage[6:7, :] = spec[...].astype(F32)
    out[...] = stage[...].astype(BF16)


DEPTH = 16


def kernel(
    pos_any,
    feat_any,
    spec_any,
    edges_any,
    count_any,
    table_any,
    w1_any,
    w2_any,
    wout_any,
    force_ref,
    energy_ref,
    pos,
    feat_ref,
    spec_ref,
    edges_ref,
    count_ref,
    table_ref,
    w1_ref,
    w2_ref,
    wout_ref,
    sib_f,
    sib_m,
    fslot,
    mown,
    mslot,
    ohp,
    ohc,
    ohpt,
    ohct,
    gi,
    gj,
    si,
    sj,
    yb,
    xbuf,
    wtmp,
    wp,
    wpt,
    w2t,
    tmat,
    gbuf,
    stage,
    pout,
    pslot,
    lsem,
    ready,
    go,
    msend,
    mrecv,
    fsend,
    frecv,
    ssend,
    srecv,
    psend,
    precv,
):
    n_plate, n_tower, n_gz = (lax.axis_size(a) for a in ("plate", "tower", "gz"))
    p, t, g = (lax.axis_index(a) for a in ("plate", "tower", "gz"))
    odd = lax.rem(t, 2)
    partner = t + 1 - 2 * odd
    outward = lax.rem(t + 2 * odd - 1 + n_tower, n_tower)
    g_up, g_dn = lax.rem(g + 1, n_gz), lax.rem(g + n_gz - 1, n_gz)
    p_up, p_dn = lax.rem(p + 1, n_plate), lax.rem(p + n_plate - 1, n_plate)
    z = lax.rem(p, DEPTH)
    last = z // (DEPTH - 1)
    first = lax.rem(z + DEPTH - 1, DEPTH) // (DEPTH - 1)

    total = n_plate * n_tower * n_gz

    def dev(pp, tt, gg):
        return {"plate": pp, "tower": tt, "gz": gg}

    def is_late(d):
        return 1 - ((d["plate"] * n_tower + d["tower"]) * n_gz + d["gz"] + total - 1) // total


    dest = [
        dev(p, t, g_up), dev(p, t, g_dn), dev(p, partner, g), dev(p, outward, g),
        dev(p, partner, g_up), dev(p, partner, g_dn), dev(p, outward, g_up), dev(p, outward, g_dn),
        dev(p_up, t, g), dev(p_dn, t, g),
    ]
    home = [dest[k] for k in (1, 0, 2, 3, 5, 4, 7, 6, 9, 8)]
    sibling = dev(lax.rem(p + DEPTH, n_plate), t, g)
    below = dev(lax.rem(p + n_plate - 1 + DEPTH * first, n_plate), t, g)
    above = dev(lax.rem(p + 1 + DEPTH, n_plate), t, g)

    loads = fetch([(feat_any, feat_ref)], lsem)
    barrier = pltpu.get_barrier_semaphore()

    def greet(d):
        pl.semaphore_signal(barrier, inc=1, device_id=d, device_id_type=pl.DeviceIdType.MESH)

    late = is_late(dev(p, t, g))
    late_to = [is_late(d) for d in dest[:4]]
    late_sib = first * is_late(sibling)
    near = late_to[0] + late_to[1] + late_to[2] + late_to[3] + late_sib

    via_lo = last * (1 - p // DEPTH)

    greet(below)

    @pl.when(late == 0)
    def _():
        for d in dest[:4]:
            greet(d)

    @pl.when(z == 0)
    def _():
        greet(dest[9])

    @pl.when(first - late == 1)
    def _():
        greet(sibling)

    @pl.when(last == 0)
    def _():
        greet(dest[8])

    loads += fetch(
        [
            (pos_any, pos), (spec_any, spec_ref), (edges_any, edges_ref), (count_any, count_ref),
            (table_any, table_ref), (w1_any, w1_ref), (w2_any, w2_ref), (wout_any, wout_ref),
        ],
        lsem,
        1,
    )
    for c in loads[1:3]:
        c.wait()
    pack_small(pos, spec_ref, stage, mown)

    def small_rows(src, k, to):
        n = {0: 0, 1: 1, 3: 2}.get(k, 3)
        return remote(src, mslot.at[k], msend, mrecv.at[n], to)

    meta = [small_rows(mown, k, dest[k]) for k in range(4)]
    m_part = [small_rows(mslot.at[k], 4 + k, dest[2]) for k in range(2)]
    m_up, m_dn = small_rows(mslot.at[3], 6, dest[0]), small_rows(mslot.at[3], 7, dest[1])
    meta += [small_rows(mown, 8, dest[8]), small_rows(mown, 9, below)]
    meta_sib = small_rows(sib_m, 9, below)
    def of_size(ref, ssem, rsem):
        return remote(ref, ref, ssem, rsem, dest[0])

    parts = [pl.ds(PART * k, PART) for k in range(ROWS // PART)]

    def feature(n, src, slot, to, part=None):
        dst = fslot.at[slot]
        if part is not None:
            src, dst = src.at[part], dst.at[part]
        return remote(src, dst, fsend, frecv.at[n], to)

    head = pl.ds(0, ROWS - PART)
    n_parts = len(parts)
    f_g = [feature(k, feat_ref, k, dest[k], head) for k in range(2)]
    f_g_last = [feature(6 + n_parts + k, feat_ref, k, dest[k], parts[-1]) for k in range(2)]
    r_out = [feature(3, fslot.at[k], 6 + k, dest[3], parts[-1]) for k in range(2)]
    f_part = feature(2, feat_ref, 2, dest[2])
    r_part = [feature(3, fslot.at[0], 4, dest[2]), feature(3, fslot.at[1], 5, dest[2])]
    r_up = [feature(3, fslot.at[3], 6, dest[0], c) for c in parts]
    r_dn = [feature(3, fslot.at[3], 7, dest[1], c) for c in parts]
    f_p_up = [feature(4, feat_ref, 8, dest[8], pl.ds(ROWS // 2 * k, ROWS // 2)) for k in range(2)]
    up_all = of_size(fslot.at[8], fsend, frecv.at[4])
    f_p_dn = feature(5, feat_ref, 9, below)
    f_p_sib = feature(5, sib_f, 9, below)
    f_out = [feature(6 + k, feat_ref, 3, dest[3], c) for k, c in enumerate(parts)]
    sib_feat = remote(feat_ref, sib_f, ssend.at[0], srecv.at[0], sibling)
    sib_meta = remote(mown, sib_m, ssend.at[1], srecv.at[1], sibling)

    meta_sent, feat_sent = of_size(mslot, msend, msend), of_size(fslot, fsend, fsend)
    meta_rest = of_size(mslot.at[pl.ds(3, 7)], msend, mrecv.at[3])
    corners = of_size(fslot.at[pl.ds(4, 4)], fsend, frecv.at[3])
    back_all = of_size(pslot, psend, precv)

    loads[0].wait()
    pl.semaphore_wait(barrier, 6 + last - near)

    def tell(sem, d):
        pl.semaphore_signal(sem, inc=1, device_id=d, device_id_type=pl.DeviceIdType.MESH)

    @pl.when(last == 1)
    def _():
        tell(ready, above)

    @pl.when(late == 1)
    def _():
        for d in (*dest[:4], sibling):
            tell(go, d)

    @pl.when(first - late_sib == 1)
    def _():
        sib_meta.start()
        sib_feat.start()

    direct = ((meta[0], f_g_last[0], f_g[0]), (meta[1], f_g_last[1], f_g[1]), (meta[2], f_part), (meta[3], *f_out))
    meta[4].start()
    f_p_up[0].start()

    @pl.when(via_lo == 0)
    def _():
        f_p_up[1].start()

    @pl.when(z != 0)
    def _():
        meta[5].start()
        f_p_dn.start()

    for k in (3, 0, 1, 2):

        @pl.when(late_to[k] == 0)
        def _(k=k):
            for c in direct[k]:
                c.start()

    for c in loads[3:]:
        c.wait()

    left, right = edges_ref[0:1, :], edges_ref[1:2, :]
    row = lax.broadcasted_iota(jnp.int32, (ATOMS, EDGES), 0)
    lane = lax.broadcasted_iota(jnp.int32, (EDGES, ATOMS), 1)

    def column_of(index):
        turned = jnp.transpose(jnp.broadcast_to(index.astype(F32), (8, EDGES)))
        return jnp.broadcast_to(turned[:, 0:1].astype(jnp.int32), (EDGES, ATOMS))

    left_col, right_col = column_of(left), column_of(right)

    def one_hot(match):
        return jnp.where(match, 1.0, 0.0).astype(BF16)

    for k in range(3):
        base = ATOMS * k
        ohp[base : base + ATOMS, :] = one_hot(row == left - base)
        ohpt[:, base : base + ATOMS] = one_hot(lane == left_col - base)
    u_part, u_out = 2 - 2 * odd, 2 * odd
    places = ((1, 0), (1, 1), (1, 2), (u_part, 1), (u_out, 1), (u_part, 0), (u_part, 2), (u_out, 0), (u_out, 2))
    for k, (u, v) in enumerate(places):
        base = (3 * u + v) * ATOMS
        ohc[ATOMS * k : ATOMS * (k + 1), :] = one_hot(row == right - base)
        ohct[:, ATOMS * k : ATOMS * (k + 1)] = one_hot(lane == right_col - base)

    tmat[...] = jnp.zeros_like(tmat)
    tmat[0:6, 0:CH] = table_ref[...].astype(F32)
    tmat[6:7, 0:CH] = wout_ref[...].astype(F32)
    turned = jnp.transpose(tmat[...])
    embt = turned[0:CH, :].astype(BF16)
    wout = turned[0:CH, 6:7]
    wtmp[0 : 5 * CH, :] = w1_ref[RB : RB + 5 * CH, :].astype(F32)
    wtmp[5 * CH : 6 * CH - RB, :] = jnp.zeros((CH - RB, LAT), F32)
    wtmp[6 * CH - RB : 6 * CH, :] = w1_ref[0:RB, :].astype(F32)
    wfull = wtmp[...]
    wpt[...] = wfull.astype(BF16)
    wp[...] = jnp.transpose(wfull).astype(BF16)
    w2t[...] = jnp.transpose(w2_ref[...].astype(F32)).astype(BF16)

    @pl.when(near == 1)
    def _():
        pl.semaphore_wait(go, 1)

        @pl.when(late_sib == 1)
        def _():
            sib_meta.start()
            sib_feat.start()

        for k in (3, 0, 1, 2):

            @pl.when(late_to[k] == 1)
            def _(k=k):
                for c in direct[k]:
                    c.start()

    meta[3].wait_recv()
    m_up.start()
    m_dn.start()
    for k in range(2):
        meta[k].wait_recv()
        m_part[k].start()
    for k, c in enumerate(f_out[:-1]):
        c.wait_recv()
        r_up[k].start()
        r_dn[k].start()
        if k == 0:
            for c_last in f_g_last:
                c_last.wait_recv()

            @pl.when(z != 0)
            def _():
                for c_out in r_out:
                    c_out.start()

    f_out[-1].wait_recv()

    @pl.when(z == 0)
    def _():
        r_up[-1].start()
        r_dn[-1].start()

    def to_partner():
        for k in range(2):
            f_g[k].wait_recv()
            r_part[k].start()

    @pl.when(via_lo == 1)
    def _():
        f_p_up[1].start()

    @pl.when(z == 0)
    def _():
        to_partner()
        sib_meta.wait_recv()
        sib_feat.wait_recv()
        pl.semaphore_wait(ready, 1)
        meta_sib.start()
        f_p_sib.start()

    meta_rest.wait_recv()
    mi = dot(jnp.concatenate([mslot[8], mown[...], mslot[9]], 1), ohp[...])
    order = [mslot[0], mown[...], *(mslot[k] for k in range(1, 8))]
    mj = dot(jnp.concatenate(order, 1), ohc[...])
    off_i = jnp.where(left < ATOMS, -1.0, jnp.where(left < 2 * ATOMS, 0.0, 1.0))
    off_u = jnp.where(right < 3 * ATOMS, 0, jnp.where(right < 6 * ATOMS, 1, 2))
    rest = right - 3 * ATOMS * off_u
    off_v = jnp.where(rest < ATOMS, -1.0, jnp.where(rest < 2 * ATOMS, 0.0, 1.0))
    dx = (mj[0:1] + mj[3:4]) - (mi[0:1] + mi[3:4] + off_i)
    dy = (mj[1:2] + mj[4:5] + (off_u.astype(F32) - 1.0)) - (mi[1:2] + mi[4:5])
    dz = (mj[2:3] + mj[5:6] + off_v) - (mi[2:3] + mi[5:6])
    r2 = dx * dx + dy * dy + dz * dz + SOFTEN
    r = jnp.sqrt(r2)
    inv = 1.0 / r
    nx, ny, nz = dx * inv, dy * inv, dz * inv
    root3, root5, root15 = math.sqrt(3.0), math.sqrt(5.0), math.sqrt(15.0)
    harm = (
        root3 * nx, root3 * ny, root3 * nz, root15 * nx * ny, root15 * ny * nz,
        0.5 * root5 * (3.0 * nz * nz - 1.0), root15 * nx * nz, 0.5 * root15 * (nx * nx - ny * ny),
    )
    for m in range(8):
        yb[m] = jnp.broadcast_to(harm[m], (8, EDGES))
    orders = (lax.broadcasted_iota(jnp.int32, (RB, EDGES), 0) + 1).astype(F32)
    sin_b, cos_b = sin_cos_pi(orders * (1.0 / RADIUS) * r)
    radial = sin_b * inv
    slope = (orders * (math.pi / RADIUS) * cos_b - radial) * inv
    live = jnp.where(lax.broadcasted_iota(jnp.int32, (1, EDGES), 1) < count_ref[0, 0], 1.0, 0.0)
    gap = jnp.maximum(1.0 - r2 * (1.0 / (RADIUS * RADIUS)), 0.0)
    env = live * gap * gap
    kinds = lax.broadcasted_iota(jnp.int32, (LAT, EDGES), 0)
    for k, m in enumerate((mi, mj)):
        pick = jnp.where(kinds == m[6:7].astype(jnp.int32), 1.0, 0.0).astype(BF16)
        xbuf[CH * k : CH * (k + 1), :] = dot(embt, pick).astype(BF16)
    xbuf[5 * CH : 6 * CH - 16, :] = jnp.zeros((CH - 16, EDGES), BF16)
    xbuf[6 * CH - 16 : 6 * CH, :] = jnp.concatenate([jnp.zeros_like(radial), radial], 0).astype(BF16)

    def rows_of(ref, m, k, lanes=slice(None)):
        return ref[m * CH + 8 * k : m * CH + 8 * k + 8, lanes]

    def degree_sums(ref, out, other=None):
        for k2 in range(CH // 16):
            prods = [[], [], []]
            for k in (2 * k2, 2 * k2 + 1):
                one = [rows_of(ref, m, k) * yb[m - 1] for m in range(1, 9)]
                sums = (
                    rows_of(ref, 0, k),
                    one[0] + one[1] + one[2],
                    one[3] + one[4] + one[5] + one[6] + one[7],
                )
                for l in range(3):
                    at = slice(l * CH + 8 * k, l * CH + 8 * k + 8)
                    out[at, :] = sums[l]
                    if other is not None:
                        prods[l].append(sums[l] * other[at, :])
            if other is not None:
                for l in range(3):
                    start = (2 + l) * CH + 16 * k2
                    xbuf[start : start + 16, :] = jnp.concatenate(prods[l], 0).astype(BF16)

    def last_columns():
        corners.wait_recv()
        late_blocks = jnp.concatenate([fslot[k] for k in range(4, 8)], 1)
        gj[...] = gj[...] + dot(late_blocks, ohc[5 * ATOMS :, :])

    pl.when(z != 0)(to_partner)
    f_part.wait_recv()
    order = [fslot[0], feat_ref[...], fslot[1], fslot[2], fslot[3]]
    gj[...] = dot(jnp.concatenate(order, 1), ohc[0 : 5 * ATOMS, :])

    @pl.when(z == 0)
    def _():
        f_p_dn.wait_recv()
        gi[...] = dot(jnp.concatenate([feat_ref[...], fslot[9]], 1), ohp[ATOMS:, :])
        last_columns()
        degree_sums(gj, sj)
        up_all.wait_recv()
        gi[...] = gi[...] + dot(fslot[8], ohp[0:ATOMS, :])
        degree_sums(gi, si, sj)

    @pl.when(z != 0)
    def _():
        f_p_dn.wait_recv()
        up_all.wait_recv()
        gi[...] = dot(jnp.concatenate([fslot[8], feat_ref[...], fslot[9]], 1), ohp[...])
        degree_sums(gi, si)
        last_columns()
        degree_sums(gj, sj, si)

    lots = [slice(EDGES // LOTS * h, EDGES // LOTS * (h + 1)) for h in range(LOTS)]

    def cut(a):
        return [a[:, e] for e in lots]

    def each(fn, *lists):
        return [fn(*args) for args in zip(*lists)]

    env_, live_, gap_, inv_ = cut(env), cut(live), cut(gap), cut(inv)
    nx_, ny_, nz_, slope_ = cut(nx), cut(ny), cut(nz), cut(slope)
    d_ = [cut(dx), cut(dy), cut(dz)]
    z1 = [dot(wp[...], xbuf[:, e]) for e in lots]
    sig1 = each(lambda v: 1.0 / (1.0 + jnp.exp(-v)), z1)
    z2 = each(lambda v, s: dot(w2_ref[...], (v * s).astype(BF16)), z1, sig1)
    sig2 = each(lambda v: 1.0 / (1.0 + jnp.exp(-v)), z2)

    dz2 = each(lambda v, s, w: (wout * w) * (s * (1.0 + v * (1.0 - s))), z2, sig2, env_)
    dh = each(lambda v: dot(w2t[...], v.astype(BF16)).astype(BF16).astype(F32), dz2)
    dz1 = each(lambda d, v, s: d * (s * (1.0 + v * (1.0 - s))), dh, z1, sig1)
    dxv = each(lambda v: dot(wpt[...], v.astype(BF16)).astype(BF16).astype(F32), dz1)
    u = each(lambda v, s: jnp.sum(wout * (v * s), 0, keepdims=True), z2, sig2)
    for h, e in enumerate(lots):
        energy_ref[:, e] = env_[h] * u[h]
    gbuf[...] = jnp.zeros_like(gbuf)
    for h, e in enumerate(lots):
        nx, ny, nz, inv = nx_[h], ny_[h], nz_[h], inv_[h]
        acc = [jnp.zeros((8, EDGES // LOTS), F32) for _ in range(8)]
        for k in range(CH // 8):
            for l, ms in ((1, (1, 2, 3)), (2, (4, 5, 6, 7, 8))):
                at = slice(l * CH + 8 * k, l * CH + 8 * k + 8)
                dq = dxv[h][2 * CH + at.start : 2 * CH + at.stop, :]
                di, dj = dq * sj[at, e], dq * si[at, e]
                for m in ms:
                    acc[m - 1] = acc[m - 1] + di * rows_of(gi, m, k, e) + dj * rows_of(gj, m, k, e)
        h1, h2, h3, h4, h5, h6, h7, h8 = (jnp.sum(a, 0, keepdims=True) for a in acc)
        ax = root3 * h1 + root15 * (ny * h4 + nz * h7 + nx * h8)
        ay = root3 * h2 + root15 * (nx * h4 + nz * h5 - ny * h8)
        az = root3 * h3 + root15 * (ny * h5 + nx * h7) + (3.0 * root5) * nz * h6
        dr = jnp.sum(dxv[h][6 * CH - RB : 6 * CH, :] * slope_[h], 0, keepdims=True)
        dr = dr - (ax * nx + ay * ny + az * nz) * inv
        denv = live_[h] * u[h] * (2.0 * gap_[h]) * (-1.0 / (RADIUS * RADIUS))
        scale = dr * inv + 2.0 * denv
        for k, a in enumerate((ax, ay, az)):
            gbuf[k : k + 1, e] = a * inv + d_[k][h] * scale

    grad = gbuf[...]
    g_hi = grad.astype(BF16).astype(F32)
    both = jnp.concatenate([g_hi, grad - g_hi], 0).astype(BF16)

    def lanes(a, k):
        return a[:, k * ATOMS : (k + 1) * ATOMS]

    back = [remote(pout.at[k], pslot.at[k], psend, precv, home[k]) for k in range(NSLOT)]
    part_p = dot(both, ohpt[...])
    part_p = part_p[0:8] + part_p[8:16]
    pout[8] = lanes(part_p, 0)
    pout[9] = lanes(part_p, 2)
    back[8].start()
    back[9].start()
    part_c = dot(both, ohct[...])
    part_c = -(part_c[0:8] + part_c[8:16])
    for slot, k in enumerate((0, 2, 3, 4, 5, 6, 7, 8)):
        pout[slot] = lanes(part_c, k)
        back[slot].start()
    force = lanes(part_p, 1) + lanes(part_c, 1)
    meta_sent.wait_send()
    feat_sent.wait_send()

    @pl.when(first == 1)
    def _():
        sib_meta.wait_send()
        sib_feat.wait_send()

    back_all.wait_recv()
    for k in range(NSLOT):
        force = force + pslot[k]
    for k in range(3):
        force_ref[k] = force[k : k + 1, :]
    back_all.wait_send()


def finish(force_ref, energy_ref, force_out, energy_out, sems):
    copies = fetch([(force_ref, force_out), (energy_ref, energy_out)], sems)
    for c in copies:
        c.wait()


def shards(positions, features, species, emb_table, edges, edge_count, w_first, w_second, w_out):
    vmem = pl.BlockSpec(memory_space=pltpu.VMEM)
    hbm = pl.BlockSpec(memory_space=pl.ANY)
    dma = pltpu.SemaphoreType.DMA
    pos = jnp.transpose(positions.reshape(1, 3, ATOMS), (1, 0, 2))
    feat = features.reshape(ROWS, ATOMS)
    spec = species.reshape(1, ATOMS)
    small = [pltpu.VMEM((3, 1, ATOMS), F32), pltpu.VMEM((1, ATOMS), jnp.int32)]
    forces, energy = pl.pallas_call(
        kernel,
        name="edge_forces",
        out_shape=(pltpu.VMEM((3, 1, ATOMS), F32), pltpu.VMEM((1, EDGES), F32)),
        in_specs=[hbm] * 9,
        out_specs=(vmem, vmem),
        scratch_shapes=[
            small[0],
            pltpu.VMEM((ROWS, ATOMS), BF16),
            small[1],
            pltpu.VMEM((2, EDGES), jnp.int32),
            pltpu.SMEM((1, 1), jnp.int32),
            pltpu.VMEM((6, CH), BF16),
            pltpu.VMEM((RB + 5 * CH, LAT), BF16),
            pltpu.VMEM((CH, LAT), BF16),
            pltpu.VMEM((1, CH), BF16),
            pltpu.VMEM((ROWS, ATOMS), BF16),
            pltpu.VMEM((16, ATOMS), BF16),
            pltpu.VMEM((NSLOT, ROWS, ATOMS), BF16),
            pltpu.VMEM((16, ATOMS), BF16),
            pltpu.VMEM((NSLOT, 16, ATOMS), BF16),
            pltpu.VMEM((3 * ATOMS, EDGES), BF16),
            pltpu.VMEM((9 * ATOMS, EDGES), BF16),
            pltpu.VMEM((EDGES, 3 * ATOMS), BF16),
            pltpu.VMEM((EDGES, 9 * ATOMS), BF16),
            pltpu.VMEM((ROWS, EDGES), F32),
            pltpu.VMEM((ROWS, EDGES), F32),
            pltpu.VMEM((3 * CH, EDGES), F32),
            pltpu.VMEM((3 * CH, EDGES), F32),
            pltpu.VMEM((8, 8, EDGES), F32),
            pltpu.VMEM((6 * CH, EDGES), BF16),
            pltpu.VMEM((6 * CH, LAT), F32),
            pltpu.VMEM((LAT, 6 * CH), BF16),
            pltpu.VMEM((6 * CH, LAT), BF16),
            pltpu.VMEM((LAT, CH), BF16),
            pltpu.VMEM((LAT, LAT), F32),
            pltpu.VMEM((8, EDGES), F32),
            pltpu.VMEM((16, ATOMS), F32),
            pltpu.VMEM((NSLOT, 8, ATOMS), F32),
            pltpu.VMEM((NSLOT, 8, ATOMS), F32),
            dma((9,)),
            pltpu.SemaphoreType.REGULAR,
            pltpu.SemaphoreType.REGULAR,
            dma,
            dma((4,)),
            dma,
            dma((8 + ROWS // PART,)),
            dma((2,)),
            dma((2,)),
            dma,
            dma,
        ],
        compiler_params=pltpu.CompilerParams(collective_id=0, has_side_effects=True),
    )(
        pos,
        feat,
        spec,
        edges.reshape(2, EDGES),
        edge_count.reshape(1, 1),
        emb_table,
        w_first.T,
        w_second,
        w_out.reshape(1, CH),
    )
    forces, energy = pl.pallas_call(
        finish,
        name="finish",
        out_shape=(jax.ShapeDtypeStruct((3, 1, ATOMS), F32), jax.ShapeDtypeStruct((1, EDGES), F32)),
        in_specs=[vmem, vmem],
        out_specs=(hbm, hbm),
        scratch_shapes=[dma((2,))],
    )(
        pltpu.with_memory_space_constraint(forces, pltpu.VMEM),
        pltpu.with_memory_space_constraint(energy, pltpu.VMEM),
    )
    return (
        jnp.transpose(forces, (1, 0, 2)).reshape(1, 1, 1, 3, ATOMS),
        energy.reshape(1, 1, 1, EDGES),
    )


def solution(mesh):
    placed = (
        P("plate", "tower", "gz", None, None),
        P("plate", "tower", "gz", None, None),
        P("plate", "tower", "gz", None),
        P(),
        P("plate", "tower", "gz", None, None),
        P("plate", "tower", "gz"),
        P(),
        P(),
        P(),
    )
    return jax.shard_map(
        shards,
        mesh=mesh,
        in_specs=placed,
        out_specs=(P("plate", "tower", "gz", None, None), P("plate", "tower", "gz", None)),
        check_vma=False,
    )
```
